32 devices in a mesh: beam: 2 (over x), tm: 16 (over z, y, core).
Axes of the slice: x: 2, y: 2, z: 4, core: 2. Of those that a mesh axis runs over, the one named last changes fastest.
Arguments:
- voltage: bfloat16 [2, 2, 2097152], P(None, None, ('beam', 'tm')), parts along dimension 2, may hold values from -11 to 11
- delays: int32 [64, 2048], replicated, may hold values from 0 to 96, as said below
- chan_mask: int32 [4096], P('beam'), parts along dimension 0, may hold values 0 or 1
Outputs:
- zscore: float32 [64, 1024], P(None, ('beam', 'tm')), parts along dimension 1
- trial_stats: float32 [3, 128], P(None, 'beam'), parts along dimension 1
The draws below stay inside these ranges and needn't reach their ends.
There are 2 independent parts, one for each index of `beam`. The reference program is written for one: setup_inputs(seed, part) draws one part's arguments, and reference() takes and returns one part's arrays. A program takes and returns all parts, laid end to end along the dimension named above; an argument that names none is the same for every part. Nothing has to cross between parts.
Inputs may be any that keep to these rules, and one draw needn't show every extreme that they name: For each trial the delays never rise from one channel to the next; the last channel's delays are 0, and the first channel's delay of some trial is 96.
All inputs are finite; a program needn't handle non-finite values.
Results may differ from the reference program's by a relative error of at most 0.002.
Values may be sent and summed in bfloat16 or wider, within the bound.
A program may use at most 64 MiB of HBM per device.

```python
import jax
import jax.numpy as jnp
from jax import lax

NCHAN = 2048
TAPS = 16
NDM = 64
SAMPLES = 1048576
MAXD = 96


def draw_voltage(key, part):
    noise_key = jax.random.fold_in(jax.random.fold_in(key, 11), 0)
    position = jnp.arange(SAMPLES, dtype=jnp.float32) / SAMPLES
    envelope = jnp.exp(0.5 * jnp.log(3.5) * position)
    values = jnp.clip(jax.random.normal(noise_key, (2, 2, SAMPLES), jnp.float32) * envelope, -11.0, 11.0)
    return values.astype(jnp.bfloat16)


def draw_delays(key, part):
    size_key, pick_key = jax.random.split(jax.random.fold_in(key, 23))
    reaches = jax.random.randint(size_key, (NDM,), 0, MAXD + 1)
    chosen = jax.random.randint(pick_key, (), 0, NDM)
    reaches = jnp.where(jnp.arange(NDM, dtype=jnp.int32) == chosen, MAXD, reaches)
    channel = jnp.arange(NCHAN, dtype=jnp.int32)
    scale_unit = max(1, (NCHAN - 1) * 3 * NCHAN // 4096)
    chan_curve = (NCHAN - 1 - channel) * (3 * NCHAN - channel) // scale_unit
    top_value = (NCHAN - 1) * 3 * NCHAN // scale_unit
    return (reaches[:, None] * chan_curve[None, :] // top_value).astype(jnp.int32)


def plant(array, rng, least, high):
    shape = array.shape
    place = [jax.random.randint(jax.random.fold_in(rng, axis), (), 0, shape[axis]) for axis in range(len(shape))]
    array = array.at[tuple(place)].set(least)
    longest = shape.index(max(shape))
    place[longest] = (place[longest] + 1) % shape[longest]
    return array.at[tuple(place)].set(high)


def setup_inputs(seed: int = 0, part: int = 0) -> dict:
    key_of = jax.random.split(jax.random.key(seed), 4)
    part_splits = jax.random.split(jax.random.fold_in(key_of[3], part), 4)
    return {
        "voltage": draw_voltage(jax.random.fold_in(jax.random.fold_in(key_of[3], part), 71), part),
        "delays": draw_delays(jax.random.fold_in(key_of[3], 71), part),
        "chan_mask": plant((jax.random.randint(part_splits[2], (NCHAN,), 0, 8) < 7).astype(jnp.int32), jax.random.fold_in(part_splits[2], 1), 0, 1),
    }


def prototype(tap_count, chan_count):
    length = tap_count * chan_count
    position = jnp.arange(length, dtype=jnp.float32)
    centred = (position - (length - 1) / 2.0) / chan_count
    window = 0.54 - 0.46 * jnp.cos(2.0 * jnp.pi * position / (length - 1))
    shaped = jnp.sinc(centred) * window
    shaped = shaped * jnp.sqrt(chan_count / jnp.sum(shaped * shaped))
    return shaped.reshape(tap_count, chan_count)

def dedisperse(padded, delays, out_width, block_rows):
    chan_count = padded.shape[0]
    offsets = jnp.arange(out_width, dtype=jnp.int32)

    def pick_row(row_values, row_delays):
        return row_values[row_delays[:, None] + offsets[None, :]]

    def add_block(block_index, running):
        first_row = (block_index * block_rows).astype(jnp.int32)
        rows_here = lax.dynamic_slice_in_dim(padded, first_row, block_rows, 0)
        delay_here = lax.dynamic_slice_in_dim(delays, first_row, block_rows, 1)
        picked = jax.vmap(pick_row)(rows_here, delay_here.T)
        return running + lax.optimization_barrier(jnp.sum(picked.astype(jnp.float32), axis=0))
    zero_sums = jnp.zeros((delays.shape[0], out_width), jnp.float32)
    return lax.fori_loop(0, chan_count // block_rows, add_block, zero_sums)

def reference(voltage, delays, chan_mask):
    frame_count = voltage.shape[2] // NCHAN
    framed = voltage.astype(jnp.float32).reshape(2, 2, frame_count, NCHAN)
    history = jnp.zeros((2, 2, TAPS - 1, NCHAN), jnp.float32)
    extended = jnp.concatenate([history, framed], axis=2)
    coeffs = prototype(TAPS, NCHAN)
    weighted = jnp.zeros((2, 2, frame_count, NCHAN), jnp.float32)
    for tap_index in range(TAPS):
        weighted = weighted + coeffs[tap_index] * extended[:, :, tap_index:tap_index + frame_count]
    spectra = jnp.fft.fft(lax.complex(weighted[:, 0], weighted[:, 1]), axis=-1) / jnp.sqrt(jnp.float32(NCHAN))
    energy = lax.optimization_barrier(jnp.sum(jnp.real(spectra) ** 2 + jnp.imag(spectra) ** 2, axis=0))
    detected = energy.T.astype(jnp.bfloat16)
    masked = detected * chan_mask.astype(jnp.bfloat16)[:, None]
    padded = jnp.concatenate([masked, jnp.zeros((NCHAN, MAXD), jnp.bfloat16)], axis=1)
    series = dedisperse(padded, delays, frame_count, 16)
    average = lax.optimization_barrier(jnp.sum(series, axis=1)) / frame_count
    peak_value = lax.optimization_barrier(jnp.max(series, axis=1))
    centred = series - average[:, None]
    variance = lax.optimization_barrier(jnp.sum(centred * centred, axis=1)) / frame_count
    deviation = jnp.sqrt(variance + 1e-05)
    zscore = centred / deviation[:, None]
    live_count = jnp.maximum(jnp.sum(chan_mask).astype(jnp.float32), 1.0)
    trial_stats = jnp.stack([average / live_count, deviation / live_count, (peak_value - average) / deviation])
    return (zscore, trial_stats)
```

```python
import functools
import math

import jax
import jax.numpy as jnp
import numpy as np
from jax import lax
from jax.experimental import pallas as pl
from jax.experimental.pallas import tpu as pltpu
from jax.sharding import PartitionSpec as P

NCHAN = 2048
TAPS = 16
DSPAN = 3
LANES = 128
RADIX = NCHAN // LANES
STEP = 9
GRANT = 16 * 1024 * 1024
MESH = pl.DeviceIdType.MESH


def prototype():
    length = TAPS * NCHAN
    position = np.arange(length, dtype=np.float64)
    window = 0.54 - 0.46 * np.cos(2.0 * np.pi * position / (length - 1))
    shaped = np.sinc((position - (length - 1) / 2.0) / NCHAN) * window
    shaped = shaped * np.sqrt(NCHAN / np.sum(shaped * shaped))
    taps = shaped.reshape(TAPS, RADIX, 1, LANES)
    taps = np.broadcast_to(taps, (TAPS, RADIX, 2, LANES))
    return taps.reshape(TAPS, 2 * RADIX, LANES).astype(np.float32)


def twiddles():
    angle = -2.0 * np.pi * np.outer(np.arange(RADIX), np.arange(LANES)) / NCHAN
    return np.stack([np.cos(angle), np.sin(angle)]).astype(np.float32)


def transform_table():
    angle = -2.0 * np.pi * (np.outer(np.arange(LANES), np.arange(LANES)) % LANES) / LANES
    scale = 1.0 / math.sqrt(NCHAN)
    cos, sin = np.cos(angle) * scale, np.sin(angle) * scale
    full = np.block([[cos, sin], [-sin, cos]]).astype(np.float32)
    high = full.astype(jnp.bfloat16)
    low = (full - high.astype(np.float32)).astype(jnp.bfloat16)
    return np.stack([high, low])


def butterflies(items):
    count = len(items)
    if count == 1:
        return items
    even = butterflies(items[0::2])
    odd = butterflies(items[1::2])
    half = count // 2
    out = [None] * count
    for k in range(half):
        re, im = odd[k]
        if k == 0:
            tr, ti = re, im
        elif 4 * k == count:
            tr, ti = im, -re
        elif 8 * k == count:
            r = math.sqrt(0.5)
            tr, ti = (re + im) * r, (im - re) * r
        elif 8 * k == 3 * count:
            r = math.sqrt(0.5)
            tr, ti = (im - re) * r, (re + im) * (-r)
        else:
            c, s = math.cos(2 * math.pi * k / count), -math.sin(2 * math.pi * k / count)
            tr, ti = re * c - im * s, re * s + im * c
        er, ei = even[k]
        out[k] = (er + tr, ei + ti)
        out[k + half] = (er - tr, ei - ti)
    return out


def channelize_kernel(count, frames, volt_hbm, taps_hbm, twid_hbm, table_hbm, delay_hbm, mask_hbm, out_ref,
                      relative_ref, meta_ref, mask_out, volt_ref, taps_ref, twid_ref, table_ref, delay_ref, mask_ref,
                      halo, ext, weighted, sections, energy, power, load_sem, send_sem, recv_sem):
    me = lax.axis_index("tm")
    past = TAPS - 1
    lines = 2 * RADIX
    half = frames // 2
    quarter = frames // 4
    cut = min(quarter, past - 1)
    spans = ((cut, past - cut), (0, cut))
    barrier = pltpu.get_barrier_semaphore()
    pairs = ((volt_hbm, volt_ref), (taps_hbm, taps_ref), (twid_hbm, twid_ref), (table_hbm, table_ref),
             (delay_hbm, delay_ref), (mask_hbm, mask_ref))
    loads = [pltpu.make_async_copy(a, b, load_sem.at[i]) for i, (a, b) in enumerate(pairs)]
    for load in loads:
        load.start()

    def pass_on(i):
        begin, size = spans[i]
        return pltpu.make_async_remote_copy(
            src_ref=volt_ref.at[:, pl.ds(frames - past + begin, size)],
            dst_ref=halo.at[:, pl.ds(begin, size)],
            send_sem=send_sem.at[i],
            recv_sem=recv_sem.at[i],
            device_id={"tm": me + 1},
            device_id_type=MESH,
        )

    @pl.when(me > 0)
    def _():
        pl.semaphore_signal(barrier, inc=1, device_id={"tm": me - 1}, device_id_type=MESH)

    loads[0].wait()

    @pl.when(me < count - 1)
    def _():
        pl.semaphore_wait(barrier, 1)
        pass_on(0).start()
        pass_on(1).start()

    for p in range(2):
        ext[p, past:past + frames] = volt_ref[p].astype(jnp.float32)

    def fir(begin, end):
        for part in range(lines // 8):
            rows = pl.ds(8 * part, 8)
            taps = [taps_ref[j, rows, :] for j in range(TAPS)]

            def one(f, carry):
                for p in range(2):
                    terms = [taps[j] * ext[p, f + j, rows, :] for j in range(TAPS)]
                    while len(terms) > 1:
                        terms = [a + b for a, b in zip(terms[0::2], terms[1::2])]
                    start = pl.multiple_of((p * frames + f) * lines, 8) + 8 * part
                    weighted[pl.ds(start, 8), :] = terms[0]
                return carry

            lax.fori_loop(begin, end, one, 0, unroll=4)

    def transform(begin, size):
        group = 8
        rows_half = 2 * size
        for g in range(rows_half // group):
            p, f = divmod(g * group, size)
            first = (p * frames + begin + f) * lines
            items = []
            for m in range(RADIX):
                re = weighted[pl.ds(first + 2 * m, group, stride=lines), :]
                im = weighted[pl.ds(first + 2 * m + 1, group, stride=lines), :]
                items.append((re, im))
            for k1, (re, im) in enumerate(butterflies(items)):
                if k1:
                    c, s = twid_ref[0, k1:k1 + 1, :], twid_ref[1, k1:k1 + 1, :]
                    re, im = re * c - im * s, re * s + im * c
                place = k1 * rows_half + g * group
                sections[place:place + group, :LANES] = re
                sections[place:place + group, LANES:] = im
        both = sections[0:RADIX * rows_half, :]
        high = both.astype(jnp.bfloat16)
        low = (both - high.astype(jnp.float32)).astype(jnp.bfloat16)
        dot = functools.partial(jnp.dot, preferred_element_type=jnp.float32)
        spec = dot(high, table_ref[0]) + (dot(high, table_ref[1]) + dot(low, table_ref[0]))
        spec = spec * spec
        both_pols = (spec[:, :LANES] + spec[:, LANES:]).reshape(RADIX, 2, size, LANES)
        energy[:, begin:begin + size, :] = both_pols[:, 0] + both_pols[:, 1]

    loads[1].wait()
    fir(half, frames)
    loads[2].wait()
    loads[3].wait()
    transform(half, frames - half)
    loads[4].wait()
    loads[5].wait()
    mask_out[...] = mask_ref[...]
    trials = delay_ref.shape[0]
    blocks = NCHAN // LANES
    lane = lax.broadcasted_iota(jnp.int32, (trials, LANES), 1)
    meta = jnp.zeros((trials, LANES), jnp.int32)
    most = jnp.zeros((trials, 1), jnp.int32)
    for b in range(blocks):
        block = delay_ref[:, b * LANES:(b + 1) * LANES]
        base = jnp.take_along_axis(block, jnp.full((trials, LANES), LANES - 1, jnp.int32), axis=1, mode="promise_in_bounds")
        away = block - base
        most = jnp.maximum(most, away[:, 0:1])
        meta = jnp.where(lane == b, base, meta)
        away = jnp.where(mask_ref[b:b + 1, :] > 0, away, -1)
        relative_ref[:, b * LANES:(b + 1) * LANES] = away.astype(jnp.float32).astype(jnp.bfloat16)
    meta_ref[...] = jnp.where(lane == blocks, most, meta)

    for i, (begin, end) in enumerate(((quarter, half), (0, quarter))):
        first, size = spans[i]

        @pl.when(me > 0)
        def _():
            pass_on(i).wait_recv()
            for p in range(2):
                ext[p, first:first + size] = halo[p, first:first + size].astype(jnp.float32)

        @pl.when(me == 0)
        def _():
            for p in range(2):
                ext[p, first:first + size] = jnp.zeros((size, lines, LANES), jnp.float32)

        fir(begin, end)
        transform(begin, end - begin)

    for k1 in range(RADIX):
        padded = jnp.concatenate([jnp.zeros((LANES - frames, LANES), jnp.float32), energy[k1]], axis=0)
        power[pl.ds(k1, LANES, stride=RADIX), :] = padded.T
    out_ref[...] = power[...].astype(jnp.bfloat16)

    @pl.when(me < count - 1)
    def _():
        pass_on(0).wait_send()
        pass_on(1).wait_send()


def dedisperse_kernel(frames, relative, meta_ref, power_ref, out_ref, acc):
    trials = relative.shape[0]
    blocks = NCHAN // LANES
    most = meta_ref[:, blocks:blocks + 1]
    zeros = jnp.zeros((LANES, LANES), jnp.bfloat16)

    def sweep(first, pair):
        upper = power_ref[2 * pair * LANES:(2 * pair + 1) * LANES, :]
        lower = power_ref[(2 * pair + 1) * LANES:(2 * pair + 2) * LANES, :]
        values = jnp.concatenate(
            [jnp.concatenate([upper, zeros], axis=1), jnp.concatenate([zeros, lower], axis=1)], axis=0
        )
        away = relative[:, 2 * pair * LANES:(2 * pair + 2) * LANES]
        picks = []
        for r in range(STEP):
            target = jnp.asarray(first + r, jnp.float32).astype(jnp.bfloat16)
            picks.append(jnp.where(away == target, jnp.ones_like(away), jnp.zeros_like(away)))
        sums = jnp.dot(jnp.concatenate(picks, axis=0), values, preferred_element_type=jnp.float32)
        out = []
        for side in range(2):
            part = sums[:, side * LANES:(side + 1) * LANES]
            run = part[:trials]
            for r in range(1, STEP):
                run = run + pltpu.roll(part[r * trials:(r + 1) * trials], LANES - r, 1)
            out.append(run)
        return out

    for pair in range(blocks // 2):
        for side, run in enumerate(sweep(0, pair)):
            acc[2 * pair + side] = run

    def more(i, carry):
        first = i * STEP
        turn = lax.rem(2 * LANES - first, LANES)
        for pair in range(blocks // 2):
            for side, run in enumerate(sweep(first, pair)):
                acc[2 * pair + side] += pltpu.roll(run, turn, 1)
        return carry

    lax.fori_loop(1, lax.div(jnp.max(most), STEP) + 1, more, 0)
    lane = lax.broadcasted_iota(jnp.int32, (trials, LANES), 1)
    total = jnp.zeros((trials, LANES), jnp.float32)
    for b in range(blocks):
        place = (lane + meta_ref[:, b:b + 1]) & (LANES - 1)
        total = total + jnp.take_along_axis(acc[b], place, axis=1, mode="promise_in_bounds")
    turned = jnp.concatenate([total, jnp.zeros((LANES - trials, LANES), jnp.float32)], axis=0).T
    half = frames // 2
    for s in range(LANES // frames):
        top = turned[s * frames:s * frames + half]
        low = turned[s * frames + half:(s + 1) * frames]
        out_ref[s * half:(s + 1) * half, :] = top + pltpu.roll(low, trials, 1)


def combine_kernel(count, frames, part_ref, mask_ref, z_ref, stats_ref, landed, mine, gathered, near_send, near_recv,
                   far_send, far_recv):
    me = lax.axis_index("tm")
    half = frames // 2
    trials = LANES // 2
    barrier = pltpu.get_barrier_semaphore()
    for k in range(1, count):
        pl.semaphore_signal(barrier, inc=1, device_id={"tm": lax.rem(me + k, count)}, device_id_type=MESH)
    pl.semaphore_wait(barrier, count - 1)

    def near(k):
        return pltpu.make_async_remote_copy(
            src_ref=part_ref.at[pl.ds((DSPAN - k) * half, half)],
            dst_ref=landed.at[k - 1],
            send_sem=near_send.at[k - 1],
            recv_sem=near_recv.at[k - 1],
            device_id={"tm": me - k},
            device_id_type=MESH,
        )

    for k in range(1, DSPAN + 1):
        @pl.when(me >= k)
        def _():
            near(k).start()

    series = part_ref[DSPAN * half:(DSPAN + 1) * half, :]
    for k in range(1, DSPAN + 1):
        @pl.when(me + k >= count)
        def _():
            landed[k - 1] = jnp.zeros((half, LANES), jnp.float32)

        @pl.when(me + k < count)
        def _():
            near(k).wait_recv()
    for k in range(1, DSPAN + 1):
        series = series + landed[k - 1]

    lane = lax.broadcasted_iota(jnp.int32, (1, LANES), 1)

    def fold(value, op):
        return op(value, pltpu.roll(value, trials, 1))

    def low_half(value):
        return jnp.where(lane < trials, value, pltpu.roll(value, trials, 1))

    def high_half(value):
        return jnp.where(lane < trials, pltpu.roll(value, trials, 1), value)

    mean = fold(jnp.sum(series, axis=0, keepdims=True), jnp.add) * (1.0 / frames)
    away = series - mean
    spread = fold(jnp.sum(away * away, axis=0, keepdims=True), jnp.add)
    peak = fold(jnp.max(series, axis=0, keepdims=True), jnp.maximum)
    mine[...] = jnp.concatenate([jnp.where(lane < trials, mean, spread), peak], axis=0)

    def far(k):
        return pltpu.make_async_remote_copy(
            src_ref=mine,
            dst_ref=gathered.at[k - 1],
            send_sem=far_send.at[k - 1],
            recv_sem=far_recv.at[k - 1],
            device_id={"tm": lax.rem(me + k, count)},
            device_id_type=MESH,
        )

    for k in range(1, count):
        far(k).start()
    live = jnp.maximum(jnp.sum(mask_ref[...].astype(jnp.float32)), 1.0)
    for k in range(1, count):
        far(k).wait_recv()
    sums = gathered[:, 0, :]
    tops = gathered[:, 1, :]
    average = (mean + low_half(jnp.sum(sums, axis=0, keepdims=True))) * (1.0 / count)
    offset = sums - average
    squares = spread + high_half(jnp.sum(sums, axis=0, keepdims=True))
    between = (mean - average) * (mean - average) + low_half(jnp.sum(offset * offset, axis=0, keepdims=True))
    variance = (squares + frames * between) * (1.0 / (frames * count))
    top = jnp.maximum(peak, jnp.max(tops, axis=0, keepdims=True))
    deviation = jnp.sqrt(variance + 1e-05)
    z = (series - average) / deviation
    z_ref[0:half, :] = z[:, :trials]
    z_ref[half:frames, :] = pltpu.roll(z, trials, 1)[:, :trials]
    stats_ref[...] = jnp.concatenate(
        [average / live, deviation / live, (top - average) / deviation], axis=0
    )[:, :trials]
    for k in range(1, DSPAN + 1):
        @pl.when(me >= k)
        def _():
            near(k).wait_send()
    for k in range(1, count):
        far(k).wait_send()


def finish_kernel(z_ref, stats_ref, z_out, stats_out, sem):
    first = pltpu.make_async_copy(z_ref, z_out, sem.at[0])
    second = pltpu.make_async_copy(stats_ref, stats_out, sem.at[1])
    first.start()
    second.start()
    first.wait()
    second.wait()


def per_device(voltage, delays, chan_mask):
    frames = voltage.shape[2] // NCHAN
    trials = delays.shape[0]
    count = lax.axis_size("tm")
    vmem = pl.BlockSpec(memory_space=pltpu.VMEM)
    lines = 2 * RADIX
    framed = voltage.reshape(2, 2, frames * RADIX, LANES).transpose(0, 2, 1, 3).reshape(2, frames, lines, LANES)
    mask_table = chan_mask.reshape(RADIX, LANES)
    power, relative, meta, mask_table = pl.pallas_call(
        functools.partial(channelize_kernel, count, frames),
        out_shape=(
            jax.ShapeDtypeStruct((NCHAN, LANES), jnp.bfloat16),
            jax.ShapeDtypeStruct((trials, NCHAN), jnp.bfloat16),
            jax.ShapeDtypeStruct((trials, LANES), jnp.int32),
            jax.ShapeDtypeStruct((RADIX, LANES), jnp.int32),
        ),
        in_specs=[pl.BlockSpec(memory_space=pltpu.HBM)] * 6,
        out_specs=(vmem,) * 4,
        scratch_shapes=[
            pltpu.VMEM((2, frames, lines, LANES), jnp.bfloat16),
            pltpu.VMEM((TAPS, lines, LANES), jnp.float32),
            pltpu.VMEM((2, RADIX, LANES), jnp.float32),
            pltpu.VMEM((2, 2 * LANES, 2 * LANES), jnp.bfloat16),
            pltpu.VMEM((trials, NCHAN), jnp.int32),
            pltpu.VMEM((RADIX, LANES), jnp.int32),
            pltpu.VMEM((2, TAPS - 1, lines, LANES), jnp.bfloat16),
            pltpu.VMEM((2, frames + TAPS - 1, lines, LANES), jnp.float32),
            pltpu.VMEM((2 * frames * lines, LANES), jnp.float32),
            pltpu.VMEM((RADIX * frames, 2 * LANES), jnp.float32),
            pltpu.VMEM((RADIX, frames, LANES), jnp.float32),
            pltpu.VMEM((NCHAN, LANES), jnp.float32),
            pltpu.SemaphoreType.DMA((6,)),
            pltpu.SemaphoreType.DMA((2,)),
            pltpu.SemaphoreType.DMA((2,)),
        ],
        compiler_params=pltpu.CompilerParams(collective_id=1, vmem_limit_bytes=GRANT, has_side_effects=True),
        name="channelize",
    )(*[pltpu.with_memory_space_constraint(v, pltpu.HBM) for v in (framed, jnp.asarray(prototype()), jnp.asarray(twiddles()), jnp.asarray(transform_table()), delays, mask_table)])
    partial = pl.pallas_call(
        functools.partial(dedisperse_kernel, frames),
        out_shape=jax.ShapeDtypeStruct((2 * frames, LANES), jnp.float32),
        in_specs=[vmem] * 3,
        out_specs=vmem,
        scratch_shapes=[
            pltpu.VMEM((NCHAN // LANES, trials, LANES), jnp.float32),
        ],
        compiler_params=pltpu.CompilerParams(vmem_limit_bytes=GRANT),
        name="dedisperse",
    )(relative, meta, power)
    zscore, trial_stats = pl.pallas_call(
        functools.partial(combine_kernel, count, frames),
        out_shape=(
            jax.ShapeDtypeStruct((frames, trials), jnp.float32),
            jax.ShapeDtypeStruct((3, trials), jnp.float32),
        ),
        in_specs=[vmem] * 2,
        out_specs=(vmem, vmem),
        scratch_shapes=[
            pltpu.VMEM((DSPAN, frames // 2, LANES), jnp.float32),
            pltpu.VMEM((2, LANES), jnp.float32),
            pltpu.VMEM((count - 1, 2, LANES), jnp.float32),
            pltpu.SemaphoreType.DMA((DSPAN,)),
            pltpu.SemaphoreType.DMA((DSPAN,)),
            pltpu.SemaphoreType.DMA((count - 1,)),
            pltpu.SemaphoreType.DMA((count - 1,)),
        ],
        compiler_params=pltpu.CompilerParams(collective_id=0, vmem_limit_bytes=GRANT, has_side_effects=True),
        name="combine",
    )(partial, mask_table)
    zscore, trial_stats = pl.pallas_call(
        finish_kernel,
        out_shape=(
            jax.ShapeDtypeStruct((frames, trials), jnp.float32),
            jax.ShapeDtypeStruct((3, trials), jnp.float32),
        ),
        in_specs=[vmem] * 2,
        out_specs=(pl.BlockSpec(memory_space=pltpu.HBM),) * 2,
        scratch_shapes=[pltpu.SemaphoreType.DMA((2,))],
        compiler_params=pltpu.CompilerParams(vmem_limit_bytes=GRANT),
        name="finish",
    )(zscore, trial_stats)
    return (zscore.T, trial_stats)


def solution(mesh):
    in_specs = (P(None, None, ("beam", "tm")), P(), P("beam"))
    out_specs = (P(None, ("beam", "tm")), P(None, "beam"))
    return jax.shard_map(
        per_device, mesh=mesh, in_specs=in_specs, out_specs=out_specs, check_vma=False
    )
```

```python
import functools
import math

import jax
import jax.numpy as jnp
import numpy as np
from jax import lax
from jax.experimental import pallas as pl
from jax.experimental.pallas import tpu as pltpu
from jax.sharding import PartitionSpec as P

NCHAN = 2048
TAPS = 16
LANES = 128
RADIX = NCHAN // LANES
MAXD = 96
EDGE = 8
HALF = MAXD // 2
GRANT = 32 * 1024 * 1024
MESH = pl.DeviceIdType.MESH


def prototype():
    length = TAPS * NCHAN
    position = np.arange(length, dtype=np.float64)
    window = 0.54 - 0.46 * np.cos(2.0 * np.pi * position / (length - 1))
    shaped = np.sinc((position - (length - 1) / 2.0) / NCHAN) * window
    shaped = shaped * np.sqrt(NCHAN / np.sum(shaped * shaped))
    taps = shaped.reshape(TAPS, RADIX, 1, LANES)
    taps = np.broadcast_to(taps, (TAPS, RADIX, 2, LANES))
    return taps.reshape(TAPS, 2 * RADIX, LANES).astype(np.float32)


def twiddles():
    angle = -2.0 * np.pi * np.outer(np.arange(RADIX), np.arange(LANES)) / NCHAN
    return np.stack([np.cos(angle), np.sin(angle)]).astype(np.float32)


def transform_table():
    angle = -2.0 * np.pi * (np.outer(np.arange(LANES), np.arange(LANES)) % LANES) / LANES
    scale = 1.0 / math.sqrt(NCHAN)
    cos, sin = np.cos(angle) * scale, np.sin(angle) * scale
    full = np.block([[cos, sin], [-sin, cos]]).astype(np.float32)
    high = full.astype(jnp.bfloat16)
    low = (full - high.astype(np.float32)).astype(jnp.bfloat16)
    return np.stack([high, low])


def butterflies(items):
    count = len(items)
    if count == 1:
        return items
    even = butterflies(items[0::2])
    odd = butterflies(items[1::2])
    half = count // 2
    out = [None] * count
    for k in range(half):
        re, im = odd[k]
        if k == 0:
            tr, ti = re, im
        elif 4 * k == count:
            tr, ti = im, -re
        elif 8 * k == count:
            r = math.sqrt(0.5)
            tr, ti = (re + im) * r, (im - re) * r
        elif 8 * k == 3 * count:
            r = math.sqrt(0.5)
            tr, ti = (im - re) * r, (re + im) * (-r)
        else:
            c, s = math.cos(2 * math.pi * k / count), -math.sin(2 * math.pi * k / count)
            tr, ti = re * c - im * s, re * s + im * c
        er, ei = even[k]
        out[k] = (er + tr, ei + ti)
        out[k + half] = (er - tr, ei - ti)
    return out


def wait_some(sem, amount):
    @pl.when(amount > 0)
    def _():
        pl.semaphore_wait(sem, amount)


def beam_kernel(count, frames, trials, volt_hbm, taps_hbm, twid_hbm, table_hbm, delay_hbm, mask_hbm, z_ref, stats_ref,
                volt_ref, taps_ref, twid_ref, table_ref, delay_ref, mask_ref, before, after, ext, weighted, sections,
                spread_out, early, late_delay, counts, picks, acc, part, landed, risen, mine, gathered,
                load_sem, halo_send, halo_recv, near_send, near_recv, far_send, far_recv, know):
    me = lax.axis_index("tm")
    past = TAPS - 1
    lead = past - EDGE
    lines = 2 * RADIX
    own = EDGE + lead
    blocks = LANES // RADIX
    wide = NCHAN // blocks
    reach = MAXD // frames
    steps = HALF + 2
    barrier = pltpu.get_barrier_semaphore()

    def here(k):
        return (me + k >= 0) & (me + k < count)

    def tell(sem, k):
        @pl.when(here(k))
        def _():
            pl.semaphore_signal(sem, inc=1, device_id={"tm": me + k}, device_id_type=MESH)

    def number(distances):
        return sum(jnp.where(here(k), 1, 0) for k in distances)

    close = [k for d in range(1, reach + 1) for k in (-d, d)]
    for k in close:
        tell(barrier, k)
    pairs = ((volt_hbm, volt_ref), (taps_hbm, taps_ref), (delay_hbm, delay_ref), (twid_hbm, twid_ref),
             (table_hbm, table_ref), (mask_hbm, mask_ref))
    loads = [pltpu.make_async_copy(a, b, load_sem.at[i]) for i, (a, b) in enumerate(pairs)]
    for load in loads:
        load.start()

    def forward():
        return pltpu.make_async_remote_copy(
            src_ref=volt_ref.at[:, pl.ds(frames - lead, lead)], dst_ref=before,
            send_sem=halo_send.at[0], recv_sem=halo_recv.at[0], device_id={"tm": me + 1}, device_id_type=MESH,
        )

    def backward():
        return pltpu.make_async_remote_copy(
            src_ref=volt_ref.at[:, pl.ds(0, EDGE)], dst_ref=after,
            send_sem=halo_send.at[1], recv_sem=halo_recv.at[1], device_id={"tm": me - 1}, device_id_type=MESH,
        )

    loads[0].wait()
    wait_some(barrier, number(close))

    @pl.when(me < count - 1)
    def _():
        forward().start()

    @pl.when(me > 0)
    def _():
        backward().start()

    rounds = []
    known = reach
    while known < count - 1:
        rounds.append(known)
        known *= 2

    def open_round(i):
        if i < len(rounds):
            for k in (-rounds[i], rounds[i]):
                tell(know.at[i], k)

    def close_round(i):
        if i < len(rounds):
            wait_some(know.at[i], number((-rounds[i], rounds[i])))

    open_round(0)
    for p in range(2):
        ext[p, own:own + frames] = volt_ref[p].astype(jnp.float32)
    for load in loads[1:]:
        load.wait()

    row = lax.broadcasted_iota(jnp.int32, (blocks, LANES), 1)
    even = mask_ref[pl.ds(0, blocks, stride=2), :]
    odd = mask_ref[pl.ds(1, blocks, stride=2), :]
    usable = []
    for h in range(2):
        place = (row & 7) * RADIX + 8 * h + row // RADIX
        low = jnp.take_along_axis(even, place, axis=1, mode="promise_in_bounds")
        high = jnp.take_along_axis(odd, place, axis=1, mode="promise_in_bounds")
        usable.append(jnp.where((row & 8) == 0, low, high).astype(jnp.float32))

    def fir(begin, size):
        for part_index in range(lines // 8):
            rows = pl.ds(8 * part_index, 8)
            taps = [taps_ref[j, rows, :] for j in range(TAPS)]

            def one(f, carry):
                for p in range(2):
                    terms = [taps[j] * ext[p, begin + EDGE + f + j, rows, :] for j in range(TAPS)]
                    while len(terms) > 1:
                        terms = [a + b for a, b in zip(terms[0::2], terms[1::2])]
                    start = pl.multiple_of((p * size + f) * lines, 8) + 8 * part_index
                    weighted[pl.ds(start, 8), :] = terms[0]
                return carry

            lax.fori_loop(0, size, one, 0, unroll=4)

    def transform(size, out, begin, scale):
        group = 8
        rows_half = 2 * size
        for g in range(rows_half // group):
            p, f = divmod(g * group, size)
            first = (p * size + f) * lines
            items = []
            for m in range(RADIX):
                re = weighted[pl.ds(first + 2 * m, group, stride=lines), :]
                im = weighted[pl.ds(first + 2 * m + 1, group, stride=lines), :]
                items.append((re, im))
            for k1, (re, im) in enumerate(butterflies(items)):
                if k1:
                    c, s = twid_ref[0, k1:k1 + 1, :], twid_ref[1, k1:k1 + 1, :]
                    re, im = re * c - im * s, re * s + im * c
                place = k1 * rows_half + g * group
                sections[place:place + group, :LANES] = re
                sections[place:place + group, LANES:] = im
        both = sections[0:RADIX * rows_half, :]
        high = both.astype(jnp.bfloat16)
        low = (both - high.astype(jnp.float32)).astype(jnp.bfloat16)
        dot = functools.partial(jnp.dot, preferred_element_type=jnp.float32)
        spec = dot(high, table_ref[0]) + (dot(high, table_ref[1]) + dot(low, table_ref[0]))
        spec = spec * spec
        both_pols = (spec[:, :LANES] + spec[:, LANES:]).reshape(RADIX, 2, size, LANES)
        energy = both_pols[:, 0] + both_pols[:, 1]
        chunk = lax.broadcasted_iota(jnp.int32, (size, LANES), 1) // RADIX
        for h in range(2):
            parts = [energy[8 * h + i] for i in range(8)]
            for bit in (4, 2, 1):
                kept = (chunk & bit) == 0
                for i in range(8):
                    if i & bit == 0:
                        low_part, high_part = parts[i], parts[i | bit]
                        parts[i] = jnp.where(kept, low_part, pltpu.roll(high_part, bit * RADIX, 1))
                        parts[i | bit] = jnp.where(kept, pltpu.roll(low_part, LANES - bit * RADIX, 1), high_part)
            for b in range(blocks):
                out[b, pl.ds(begin, size), h * LANES:(h + 1) * LANES] = parts[b] * (usable[h][b:b + 1] * scale)

    fir(EDGE, frames // 2)
    transform(frames // 2, spread_out, EDGE, 1.0)
    close_round(0)
    open_round(1)

    for b in range(NCHAN // LANES):
        block = delay_ref[:, b * LANES:(b + 1) * LANES].astype(jnp.float32)
        late_delay[b * LANES:(b + 1) * LANES, :] = jnp.concatenate([block, block], axis=0).T.astype(jnp.bfloat16)
    lane = lax.broadcasted_iota(jnp.int32, (16, LANES), 1)
    second = jnp.where(lane < trials, 0.0, float(HALF))
    at_once = 10

    def tally(g, carry):
        base = second + (g * at_once).astype(jnp.float32)
        levels = [(base + float(i)).astype(jnp.bfloat16) for i in range(at_once)]

        def some(k, sums):
            seen = late_delay[pl.ds(pl.multiple_of(k * 16, 16), 16), :]
            one = jnp.ones_like(seen)
            zero = jnp.zeros_like(seen)
            return tuple(t + jnp.where(seen >= level, one, zero) for t, level in zip(sums, levels))

        sums = lax.fori_loop(
            0, NCHAN // 16, some, tuple(jnp.zeros((16, LANES), jnp.bfloat16) for _ in range(at_once)), unroll=4
        )
        for i in range(at_once):
            counts[pl.ds(g * at_once + i, 1), :] = jnp.sum(sums[i].astype(jnp.float32), axis=0, keepdims=True)
        return carry

    lax.fori_loop(0, steps // at_once, tally, 0)
    close_round(1)
    open_round(2)
    order = lax.broadcasted_iota(jnp.int32, (wide, LANES), 0)
    order = ((order & (RADIX - 1)) * RADIX + order // RADIX).astype(jnp.float32).astype(jnp.bfloat16)

    def choose(i, carry):
        for side in range(2):
            total = counts[pl.ds(2 * i + side, 1), :].astype(jnp.int32)
            within = jnp.broadcast_to((total & (wide - 1)).astype(jnp.float32), (16, LANES)).astype(jnp.bfloat16)
            for g in range(wide // 16):
                mark = order[16 * g:16 * g + 16] < within
                picks[i, 16 * g:16 * g + 16, side * LANES:(side + 1) * LANES] = jnp.where(
                    mark, jnp.ones_like(within), jnp.zeros_like(within))
        return carry

    lax.fori_loop(0, steps // 2, choose, 0)
    acc[...] = jnp.zeros_like(acc)

    def dedisperse(source, size, offset):
        values = jnp.concatenate([source[b] for b in range(blocks)], axis=0).astype(jnp.bfloat16)
        dot = functools.partial(jnp.dot, preferred_element_type=jnp.float32)
        sums = dot(values, jnp.ones((wide, LANES), jnp.bfloat16))
        column = lax.broadcasted_iota(jnp.int32, (size, LANES), 1)
        prefix = jnp.zeros((size, LANES), jnp.float32)
        for b in range(blocks):
            prefix = prefix + jnp.where(column > b, sums[b * size:(b + 1) * size], 0.0)
        last = None
        for i in range(steps // 2):
            found = dot(values, picks[i])
            for side in range(2):
                j = 2 * i + side
                which = jnp.broadcast_to(counts[j:j + 1, :].astype(jnp.int32) // wide, (size, LANES))
                inner = jnp.zeros((size, LANES), jnp.float32)
                for b in range(blocks):
                    inner = jnp.where(which == b, found[b * size:(b + 1) * size, side * LANES:(side + 1) * LANES], inner)
                now = inner + jnp.take_along_axis(prefix, which, axis=1, mode="promise_in_bounds")
                if j:
                    change = last - now
                    if j - 1 == HALF:
                        change = jnp.where(column < trials, 0.0, change)
                    a, m = divmod(j - 1, 8)
                    place = HALF + EDGE + offset - 8 * a
                    acc[m, place:place + size] += change
                last = now

    @pl.when(me == 0)
    def _():
        for p in range(2):
            ext[p, 0:own] = jnp.zeros((own, lines, LANES), jnp.float32)
        fir(-EDGE, EDGE)
        transform(EDGE, early, 0, 1.0)
        dedisperse(early, EDGE, -EDGE)

    for i in range(2):
        from_before = lax.rem(me + i, 2) == 1
        begin = pl.multiple_of(jnp.where(from_before, 0, frames - EDGE), EDGE)

        @pl.when(from_before & (me > 0))
        def _():
            forward().wait_recv()
            for p in range(2):
                ext[p, EDGE:own] = before[p].astype(jnp.float32)

        @pl.when(jnp.logical_not(from_before) & (me < count - 1))
        def _():
            backward().wait_recv()
            for p in range(2):
                ext[p, own + frames:own + frames + EDGE] = after[p].astype(jnp.float32)

        @pl.when(jnp.logical_not(from_before) & (me == count - 1))
        def _():
            for p in range(2):
                ext[p, own + frames:own + frames + EDGE] = jnp.zeros((EDGE, lines, LANES), jnp.float32)

        fir(begin, EDGE)
        ended = jnp.logical_not(from_before) & (me == count - 1)
        transform(EDGE, spread_out, begin, jnp.where(ended, 0.0, 1.0))

    dedisperse(spread_out, frames, 0)
    height = HALF + frames + EDGE
    total = acc[0, 0:height]
    for m in range(1, 8):
        total = total + acc[m, m:m + height]
    side = lax.broadcasted_iota(jnp.int32, (8, LANES), 1) < trials
    empty = jnp.zeros((8, LANES), jnp.float32)

    def joined(r):
        first = total[r - HALF:r - HALF + 8] if HALF <= r < HALF + height else empty
        other = total[r:r + 8] if r < height else empty
        mixed = jnp.where(side, first, other)
        return mixed + pltpu.roll(mixed, trials, 1)

    half = frames // 2
    for q in range(reach + 1):
        for r in range(0, half, 8):
            top = joined(q * frames + r)
            low = joined(q * frames + half + r)
            part[q * half + r:q * half + r + 8, :] = jnp.where(side, top, low)
    rise = (reach + 1) * frames
    part[(reach + 1) * half:(reach + 1) * half + EDGE, :] = jnp.where(side, joined(rise), 0.0)

    def near(k):
        return pltpu.make_async_remote_copy(
            src_ref=part.at[pl.ds((reach - k) * half, half)], dst_ref=landed.at[k - 1],
            send_sem=near_send.at[k - 1], recv_sem=near_recv.at[k - 1],
            device_id={"tm": me - k}, device_id_type=MESH,
        )

    def up():
        return pltpu.make_async_remote_copy(
            src_ref=part.at[pl.ds((reach + 1) * half, EDGE)], dst_ref=risen,
            send_sem=near_send.at[reach], recv_sem=near_recv.at[reach],
            device_id={"tm": me + 1}, device_id_type=MESH,
        )

    for k in range(reach, 0, -1):
        @pl.when(me >= k)
        def _():
            near(k).start()

    @pl.when(me < count - 1)
    def _():
        up().start()

    for i in range(2, len(rounds)):
        close_round(i)
        open_round(i + 1)

    @pl.when(me == 0)
    def _():
        risen[...] = jnp.zeros_like(risen)

    @pl.when(me > 0)
    def _():
        up().wait_recv()

    for k in range(1, reach + 1):
        @pl.when(me + k >= count)
        def _():
            landed[k - 1] = jnp.zeros((half, LANES), jnp.float32)

        @pl.when(me + k < count)
        def _():
            near(k).wait_recv()

    series = part[reach * half:(reach + 1) * half, :]
    for k in range(1, reach + 1):
        series = series + landed[k - 1]
    series = series + jnp.concatenate([risen[...], jnp.zeros((half - EDGE, LANES), jnp.float32)], axis=0)
    lane = lax.broadcasted_iota(jnp.int32, (1, LANES), 1)

    def fold(value, op):
        return op(value, pltpu.roll(value, trials, 1))

    def low_half(value):
        return jnp.where(lane < trials, value, pltpu.roll(value, trials, 1))

    def high_half(value):
        return jnp.where(lane < trials, pltpu.roll(value, trials, 1), value)

    mean = fold(jnp.sum(series, axis=0, keepdims=True), jnp.add) * (1.0 / frames)
    away = series - mean
    spread = fold(jnp.sum(away * away, axis=0, keepdims=True), jnp.add)
    peak = fold(jnp.max(series, axis=0, keepdims=True), jnp.maximum)
    mine[...] = jnp.concatenate([jnp.where(lane < trials, mean, spread), peak], axis=0)

    def far(k):
        return pltpu.make_async_remote_copy(
            src_ref=mine, dst_ref=gathered.at[k - 1],
            send_sem=far_send.at[k - 1], recv_sem=far_recv.at[k - 1],
            device_id={"tm": lax.rem(me + k, count)}, device_id_type=MESH,
        )

    for k in range(1, count):
        far(k).start()
    live = jnp.maximum(jnp.sum(mask_ref[...].astype(jnp.float32)), 1.0)
    for k in range(1, count):
        far(k).wait_recv()
    sums = gathered[:, 0, :]
    tops = gathered[:, 1, :]
    average = (mean + low_half(jnp.sum(sums, axis=0, keepdims=True))) * (1.0 / count)
    offset = sums - average
    squares = spread + high_half(jnp.sum(sums, axis=0, keepdims=True))
    between = (mean - average) * (mean - average) + low_half(jnp.sum(offset * offset, axis=0, keepdims=True))
    variance = (squares + frames * between) * (1.0 / (frames * count))
    top = jnp.maximum(peak, jnp.max(tops, axis=0, keepdims=True))
    deviation = jnp.sqrt(variance + 1e-05)
    z = (series - average) / deviation
    z_ref[0:half, :] = z[:, :trials]
    z_ref[half:frames, :] = pltpu.roll(z, trials, 1)[:, :trials]
    stats_ref[...] = jnp.concatenate(
        [average / live, deviation / live, (top - average) / deviation], axis=0
    )[:, :trials]

    @pl.when(me < count - 1)
    def _():
        forward().wait_send()
        up().wait_send()

    @pl.when(me > 0)
    def _():
        backward().wait_send()

    for k in range(1, reach + 1):
        @pl.when(me >= k)
        def _():
            near(k).wait_send()
    for k in range(1, count):
        far(k).wait_send()


def finish_kernel(z_ref, stats_ref, z_out, stats_out, sem):
    first = pltpu.make_async_copy(z_ref, z_out, sem.at[0])
    second = pltpu.make_async_copy(stats_ref, stats_out, sem.at[1])
    first.start()
    second.start()
    first.wait()
    second.wait()


def per_device(voltage, delays, chan_mask):
    frames = voltage.shape[2] // NCHAN
    trials = delays.shape[0]
    count = lax.axis_size("tm")
    lines = 2 * RADIX
    half = frames // 2
    blocks = LANES // RADIX
    wide = NCHAN // blocks
    reach = MAXD // frames
    steps = HALF + 2
    past = TAPS - 1
    vmem = pl.BlockSpec(memory_space=pltpu.VMEM)
    hbm = pl.BlockSpec(memory_space=pltpu.HBM)
    framed = voltage.reshape(2, 2, frames * RADIX, LANES).transpose(0, 2, 1, 3).reshape(2, frames, lines, LANES)
    operands = (framed, jnp.asarray(prototype()), jnp.asarray(twiddles()), jnp.asarray(transform_table()), delays,
                chan_mask.reshape(RADIX, LANES))
    dma = pltpu.SemaphoreType.DMA
    outputs = (
        jax.ShapeDtypeStruct((frames, trials), jnp.float32),
        jax.ShapeDtypeStruct((3, trials), jnp.float32),
    )
    results = pl.pallas_call(
        functools.partial(beam_kernel, count, frames, trials),
        out_shape=outputs,
        in_specs=[hbm] * 6,
        out_specs=(vmem,) * 2,
        scratch_shapes=[
            pltpu.VMEM((2, frames, lines, LANES), jnp.bfloat16),
            pltpu.VMEM((TAPS, lines, LANES), jnp.float32),
            pltpu.VMEM((2, RADIX, LANES), jnp.float32),
            pltpu.VMEM((2, 2 * LANES, 2 * LANES), jnp.bfloat16),
            pltpu.VMEM((trials, NCHAN), jnp.int32),
            pltpu.VMEM((RADIX, LANES), jnp.int32),
            pltpu.VMEM((2, past - EDGE, lines, LANES), jnp.bfloat16),
            pltpu.VMEM((2, EDGE, lines, LANES), jnp.bfloat16),
            pltpu.VMEM((2, frames + past + EDGE, lines, LANES), jnp.float32),
            pltpu.VMEM((frames * lines, LANES), jnp.float32),
            pltpu.VMEM((RADIX * frames, 2 * LANES), jnp.float32),
            pltpu.VMEM((blocks, frames, 2 * LANES), jnp.float32),
            pltpu.VMEM((blocks, EDGE, 2 * LANES), jnp.float32),
            pltpu.VMEM((NCHAN, LANES), jnp.bfloat16),
            pltpu.VMEM((steps + 6, LANES), jnp.float32),
            pltpu.VMEM((steps // 2, wide, 2 * LANES), jnp.bfloat16),
            pltpu.VMEM((8, HALF + frames + 2 * EDGE, LANES), jnp.float32),
            pltpu.VMEM(((reach + 1) * half + EDGE, LANES), jnp.float32),
            pltpu.VMEM((reach, half, LANES), jnp.float32),
            pltpu.VMEM((EDGE, LANES), jnp.float32),
            pltpu.VMEM((2, LANES), jnp.float32),
            pltpu.VMEM((count - 1, 2, LANES), jnp.float32),
            dma((6,)),
            dma((2,)),
            dma((2,)),
            dma((reach + 1,)),
            dma((reach + 1,)),
            dma((count - 1,)),
            dma((count - 1,)),
            pltpu.SemaphoreType.REGULAR((8,)),
        ],
        compiler_params=pltpu.CompilerParams(collective_id=1, vmem_limit_bytes=GRANT, has_side_effects=True),
        name="beam",
    )(*[pltpu.with_memory_space_constraint(v, pltpu.HBM) for v in operands])
    zscore, trial_stats = pl.pallas_call(
        finish_kernel,
        out_shape=outputs,
        in_specs=[vmem] * 2,
        out_specs=(hbm,) * 2,
        scratch_shapes=[dma((2,))],
        compiler_params=pltpu.CompilerParams(vmem_limit_bytes=GRANT),
        name="finish",
    )(*results)
    return (zscore.T, trial_stats)


def solution(mesh):
    in_specs = (P(None, None, ("beam", "tm")), P(), P("beam"))
    out_specs = (P(None, ("beam", "tm")), P(None, "beam"))
    return jax.shard_map(
        per_device, mesh=mesh, in_specs=in_specs, out_specs=out_specs, check_vma=False
    )
```

```python
import functools
import math

import jax
import jax.numpy as jnp
import numpy as np
from jax import lax
from jax.experimental import pallas as pl
from jax.experimental.pallas import tpu as pltpu
from jax.sharding import PartitionSpec as P

NCHAN = 2048
TAPS = 16
LANES = 128
RADIX = NCHAN // LANES
MAXD = 96
EDGE = 8
HALF = MAXD // 2
PITCH = 40
GRANT = 32 * 1024 * 1024
MESH = pl.DeviceIdType.MESH


def prototype():
    length = TAPS * NCHAN
    position = np.arange(length, dtype=np.float64)
    window = 0.54 - 0.46 * np.cos(2.0 * np.pi * position / (length - 1))
    shaped = np.sinc((position - (length - 1) / 2.0) / NCHAN) * window
    shaped = shaped * np.sqrt(NCHAN / np.sum(shaped * shaped))
    taps = shaped.reshape(TAPS, RADIX, 1, LANES)
    taps = np.broadcast_to(taps, (TAPS, RADIX, 2, LANES))
    return taps.reshape(TAPS, 2 * RADIX, LANES).astype(np.float32)


def twiddles():
    angle = -2.0 * np.pi * np.outer(np.arange(RADIX), np.arange(LANES)) / NCHAN
    return np.stack([np.cos(angle), np.sin(angle)]).astype(np.float32)


def transform_table():
    angle = -2.0 * np.pi * (np.outer(np.arange(LANES), np.arange(LANES)) % LANES) / LANES
    scale = 1.0 / math.sqrt(NCHAN)
    cos, sin = np.cos(angle) * scale, np.sin(angle) * scale
    full = np.block([[cos, sin], [-sin, cos]]).astype(np.float32)
    high = full.astype(jnp.bfloat16)
    low = (full - high.astype(np.float32)).astype(jnp.bfloat16)
    return np.stack([high, low])


def butterflies(items):
    count = len(items)
    if count == 1:
        return items
    even = butterflies(items[0::2])
    odd = butterflies(items[1::2])
    half = count // 2
    out = [None] * count
    for k in range(half):
        re, im = odd[k]
        if k == 0:
            tr, ti = re, im
        elif 4 * k == count:
            tr, ti = im, -re
        elif 8 * k == count:
            r = math.sqrt(0.5)
            tr, ti = (re + im) * r, (im - re) * r
        elif 8 * k == 3 * count:
            r = math.sqrt(0.5)
            tr, ti = (im - re) * r, (re + im) * (-r)
        else:
            c, s = math.cos(2 * math.pi * k / count), -math.sin(2 * math.pi * k / count)
            tr, ti = re * c - im * s, re * s + im * c
        er, ei = even[k]
        out[k] = (er + tr, ei + ti)
        out[k + half] = (er - tr, ei - ti)
    return out


def wait_some(sem, amount):
    @pl.when(amount > 0)
    def _():
        pl.semaphore_wait(sem, amount)


def beam_kernel(count, frames, trials, volt_hbm, taps_hbm, twid_hbm, table_hbm, delay_hbm, mask_hbm, z_ref, stats_ref,
                volt_ref, taps_ref, twid_ref, table_ref, delay_ref, mask_ref, before, after, ext, weighted, sections,
                spread_out, early, blockno, within, picks, acc, part, landed, risen, mine, gathered,
                load_sem, halo_send, halo_recv, near_send, near_recv, far_send, far_recv, know):
    me = lax.axis_index("tm")
    past = TAPS - 1
    lead = past - EDGE
    lines = 2 * RADIX
    own = EDGE + lead
    blocks = LANES // RADIX
    wide = NCHAN // blocks
    reach = MAXD // frames
    steps = HALF + 2
    barrier = pltpu.get_barrier_semaphore()

    def here(k):
        return (me + k >= 0) & (me + k < count)

    def tell(sem, k):
        @pl.when(here(k))
        def _():
            pl.semaphore_signal(sem, inc=1, device_id={"tm": me + k}, device_id_type=MESH)

    def number(distances):
        return sum(jnp.where(here(k), 1, 0) for k in distances)

    close = [k for d in range(1, reach + 1) for k in (-d, d)]
    for k in close:
        tell(barrier, k)
    pairs = ((volt_hbm, volt_ref), (taps_hbm, taps_ref.at[:, pl.ds(0, lines)]), (delay_hbm, delay_ref), (twid_hbm, twid_ref),
             (table_hbm, table_ref), (mask_hbm, mask_ref))
    loads = [pltpu.make_async_copy(a, b, load_sem.at[i]) for i, (a, b) in enumerate(pairs)]
    for load in loads:
        load.start()

    def forward():
        return pltpu.make_async_remote_copy(
            src_ref=volt_ref.at[:, pl.ds(frames - lead, lead)], dst_ref=before,
            send_sem=halo_send.at[0], recv_sem=halo_recv.at[0], device_id={"tm": me + 1}, device_id_type=MESH,
        )

    def backward():
        return pltpu.make_async_remote_copy(
            src_ref=volt_ref.at[:, pl.ds(0, EDGE)], dst_ref=after,
            send_sem=halo_send.at[1], recv_sem=halo_recv.at[1], device_id={"tm": me - 1}, device_id_type=MESH,
        )

    loads[0].wait()
    wait_some(barrier, number(close))

    @pl.when(me < count - 1)
    def _():
        forward().start()

    @pl.when(me > 0)
    def _():
        backward().start()

    rounds = []
    known = reach
    while known < count - 1:
        rounds.append(known)
        known *= 2

    def open_round(i):
        if i < len(rounds):
            for k in (-rounds[i], rounds[i]):
                tell(know.at[i], k)

    def close_round(i):
        if i < len(rounds):
            wait_some(know.at[i], number((-rounds[i], rounds[i])))

    open_round(0)
    for p in range(2):
        ext[p, own:own + frames, 0:lines] = volt_ref[p].astype(jnp.float32)
    for load in loads[1:]:
        load.wait()

    row = lax.broadcasted_iota(jnp.int32, (blocks, LANES), 1)
    even = mask_ref[pl.ds(0, blocks, stride=2), :]
    odd = mask_ref[pl.ds(1, blocks, stride=2), :]
    usable = []
    for h in range(2):
        place = (row & 7) * RADIX + 8 * h + (row >> 4)
        low = jnp.take_along_axis(even, place, axis=1, mode="promise_in_bounds")
        high = jnp.take_along_axis(odd, place, axis=1, mode="promise_in_bounds")
        usable.append(jnp.where((row & 8) == 0, low, high).astype(jnp.float32))

    def fir(begin, size):
        for part_index in range(lines // 8):
            rows = pl.ds(8 * part_index, 8)
            taps = [taps_ref[j, rows, :] for j in range(TAPS)]

            def some(g, carry):
                for p in range(2):
                    sums = [None] * 4
                    for i in range(TAPS + 3):
                        sample = ext[p, begin + EDGE + 4 * g + i, rows, :]
                        for f in range(4):
                            if 0 <= i - f < TAPS:
                                term = taps[i - f] * sample
                                sums[f] = term if sums[f] is None else sums[f] + term
                    for f in range(4):
                        start = pl.multiple_of((p * size + 4 * g + f) * PITCH, 8) + 8 * part_index
                        weighted[pl.ds(start, 8), :] = sums[f]
                return carry

            lax.fori_loop(0, size // 4, some, 0)

    def transform(size, out, begin, scale):
        group = 8
        rows_half = 2 * size
        for g in range(rows_half // group):
            p, f = divmod(g * group, size)
            first = (p * size + f) * PITCH
            items = []
            for m in range(RADIX):
                re = weighted[pl.ds(first + 2 * m, group, stride=PITCH), :]
                im = weighted[pl.ds(first + 2 * m + 1, group, stride=PITCH), :]
                items.append((re, im))
            for k1, (re, im) in enumerate(butterflies(items)):
                if k1:
                    c, s = twid_ref[0, k1:k1 + 1, :], twid_ref[1, k1:k1 + 1, :]
                    re, im = re * c - im * s, re * s + im * c
                place = k1 * rows_half + g * group
                sections[place:place + group, :LANES] = re
                sections[place:place + group, LANES:] = im
        both = sections[0:RADIX * rows_half, :]
        high = both.astype(jnp.bfloat16)
        low = (both - high.astype(jnp.float32)).astype(jnp.bfloat16)
        dot = functools.partial(jnp.dot, preferred_element_type=jnp.float32)
        spec = dot(high, table_ref[0]) + (dot(high, table_ref[1]) + dot(low, table_ref[0]))
        spec = spec * spec
        both_pols = (spec[:, :LANES] + spec[:, LANES:]).reshape(RADIX, 2, size, LANES)
        energy = both_pols[:, 0] + both_pols[:, 1]
        chunk = lax.broadcasted_iota(jnp.int32, (size, LANES), 1) >> 4
        for h in range(2):
            parts = [energy[8 * h + i] for i in range(8)]
            for bit in (4, 2, 1):
                kept = (chunk & bit) == 0
                for i in range(8):
                    if i & bit == 0:
                        low_part, high_part = parts[i], parts[i | bit]
                        parts[i] = jnp.where(kept, low_part, pltpu.roll(high_part, bit * RADIX, 1))
                        parts[i | bit] = jnp.where(kept, pltpu.roll(low_part, LANES - bit * RADIX, 1), high_part)
            for b in range(blocks):
                out[b, pl.ds(begin, size), h * LANES:(h + 1) * LANES] = parts[b] * (usable[h][b:b + 1] * scale)

    fir(EDGE, frames // 2)
    transform(frames // 2, spread_out, EDGE, 1.0)
    close_round(0)
    open_round(1)

    level = lax.broadcasted_iota(jnp.int32, (trials, LANES), 1)

    def look(table, place):
        return jnp.take_along_axis(table, place, axis=1, mode="promise_in_bounds")

    tables = NCHAN // LANES
    seldom = jnp.zeros((trials, LANES), jnp.int32)
    each = (level & (LANES // tables - 1)) * tables + (tables - 1)
    for b in range(tables):
        seen = look(delay_ref[:, b * LANES:(b + 1) * LANES], each)
        seldom = jnp.where((level >> 3) == b, seen, seldom)
    coarse = jnp.zeros((trials, LANES), jnp.int32)
    for step in (64, 32, 16, 8, 4, 2, 1):
        seen = look(seldom, coarse + (step - 1))
        coarse = jnp.where(seen >= level, coarse + step, coarse)
    which = coarse >> 3
    start = (coarse & 7) * tables
    fine = jnp.zeros((trials, LANES), jnp.int32)
    for step in (8, 4, 2, 1):
        place = start + fine + (step - 1)
        seen = jnp.full((trials, LANES), -1, jnp.int32)
        for b in range(tables):
            seen = jnp.where(which == b, look(delay_ref[:, b * LANES:(b + 1) * LANES], place), seen)
        fine = jnp.where(seen >= level, fine + step, fine)
    total = jnp.where(level == 0, NCHAN, coarse * tables + fine).astype(jnp.float32)
    turned = jnp.concatenate([total, jnp.zeros((LANES - trials, LANES), jnp.float32)], axis=0).T
    rows_kept = blockno.shape[0]
    near_side = lax.broadcasted_iota(jnp.int32, (rows_kept, LANES), 1) < trials
    total = jnp.where(
        near_side, turned[0:rows_kept], pltpu.roll(turned[HALF:HALF + rows_kept], trials, 1)
    ).astype(jnp.int32)
    blockno[...] = total >> 8
    within[...] = (total & (wide - 1)).astype(jnp.float32)
    close_round(1)
    open_round(2)
    order = lax.broadcasted_iota(jnp.int32, (wide, LANES), 0)
    order = ((order & (RADIX - 1)) * RADIX + (order >> 4)).astype(jnp.float32)

    def choose(i, carry):
        for side in range(2):
            end = jnp.broadcast_to(within[pl.ds(2 * i + side, 1), :], (wide, LANES))
            picks[i, :, side * LANES:(side + 1) * LANES] = jnp.where(order < end, 1.0, 0.0).astype(jnp.bfloat16)
        return carry

    lax.fori_loop(0, steps // 2, choose, 0)
    acc[...] = jnp.zeros_like(acc)

    def dedisperse(source, size, offset):
        values = jnp.concatenate([source[b] for b in range(blocks)], axis=0).astype(jnp.bfloat16)
        dot = functools.partial(jnp.dot, preferred_element_type=jnp.float32)
        sums = dot(values, jnp.ones((wide, LANES), jnp.bfloat16))
        column = lax.broadcasted_iota(jnp.int32, (size, LANES), 1)
        prefix = jnp.zeros((size, LANES), jnp.float32)
        for b in range(blocks):
            prefix = prefix + jnp.where(column > b, sums[b * size:(b + 1) * size], 0.0)
        last = None
        for i in range(steps // 2):
            found = dot(values, picks[i])
            for side in range(2):
                j = 2 * i + side
                which = jnp.broadcast_to(blockno[j:j + 1, :], (size, LANES))
                inner = jnp.zeros((size, LANES), jnp.float32)
                for b in range(blocks):
                    inner = jnp.where(which == b, found[b * size:(b + 1) * size, side * LANES:(side + 1) * LANES], inner)
                now = inner + jnp.take_along_axis(prefix, which, axis=1, mode="promise_in_bounds")
                if j:
                    change = last - now
                    if j - 1 == HALF:
                        change = jnp.where(column < trials, 0.0, change)
                    a, m = divmod(j - 1, 8)
                    place = HALF + EDGE + offset - 8 * a
                    acc[m, place:place + size] += change
                last = now

    @pl.when(me == 0)
    def _():
        for p in range(2):
            ext[p, 0:own, 0:lines] = jnp.zeros((own, lines, LANES), jnp.float32)
        fir(-EDGE, EDGE)
        transform(EDGE, early, 0, 1.0)
        dedisperse(early, EDGE, -EDGE)

    for i in range(2):
        from_before = lax.rem(me + i, 2) == 1
        begin = pl.multiple_of(jnp.where(from_before, 0, frames - EDGE), EDGE)

        @pl.when(from_before & (me > 0))
        def _():
            forward().wait_recv()
            for p in range(2):
                ext[p, EDGE:own, 0:lines] = before[p].astype(jnp.float32)

        @pl.when(jnp.logical_not(from_before) & (me < count - 1))
        def _():
            backward().wait_recv()
            for p in range(2):
                ext[p, own + frames:own + frames + EDGE, 0:lines] = after[p].astype(jnp.float32)

        @pl.when(jnp.logical_not(from_before) & (me == count - 1))
        def _():
            for p in range(2):
                ext[p, own + frames:own + frames + EDGE, 0:lines] = jnp.zeros((EDGE, lines, LANES), jnp.float32)

        fir(begin, EDGE)
        ended = jnp.logical_not(from_before) & (me == count - 1)
        transform(EDGE, spread_out, begin, jnp.where(ended, 0.0, 1.0))

    dedisperse(spread_out, frames, 0)
    height = HALF + frames + EDGE
    total = acc[0, 0:height]
    for m in range(1, 8):
        total = total + acc[m, m:m + height]
    side = lax.broadcasted_iota(jnp.int32, (8, LANES), 1) < trials
    empty = jnp.zeros((8, LANES), jnp.float32)

    def joined(r):
        first = total[r - HALF:r - HALF + 8] if HALF <= r < HALF + height else empty
        other = total[r:r + 8] if r < height else empty
        mixed = jnp.where(side, first, other)
        return mixed + pltpu.roll(mixed, trials, 1)

    half = frames // 2
    for q in range(reach + 1):
        for r in range(0, half, 8):
            top = joined(q * frames + r)
            low = joined(q * frames + half + r)
            part[q * half + r:q * half + r + 8, :] = jnp.where(side, top, low)
    rise = (reach + 1) * frames
    part[(reach + 1) * half:(reach + 1) * half + EDGE, :] = jnp.where(side, joined(rise), 0.0)

    def near(k):
        return pltpu.make_async_remote_copy(
            src_ref=part.at[pl.ds((reach - k) * half, half)], dst_ref=landed.at[k - 1],
            send_sem=near_send.at[k - 1], recv_sem=near_recv.at[k - 1],
            device_id={"tm": me - k}, device_id_type=MESH,
        )

    def up():
        return pltpu.make_async_remote_copy(
            src_ref=part.at[pl.ds((reach + 1) * half, EDGE)], dst_ref=risen,
            send_sem=near_send.at[reach], recv_sem=near_recv.at[reach],
            device_id={"tm": me + 1}, device_id_type=MESH,
        )

    for k in range(reach, 0, -1):
        @pl.when(me >= k)
        def _():
            near(k).start()

    @pl.when(me < count - 1)
    def _():
        up().start()

    for i in range(2, len(rounds)):
        close_round(i)
        open_round(i + 1)

    @pl.when(me == 0)
    def _():
        risen[...] = jnp.zeros_like(risen)

    @pl.when(me > 0)
    def _():
        up().wait_recv()

    for k in range(1, reach + 1):
        @pl.when(me + k >= count)
        def _():
            landed[k - 1] = jnp.zeros((half, LANES), jnp.float32)

        @pl.when(me + k < count)
        def _():
            near(k).wait_recv()

    series = part[reach * half:(reach + 1) * half, :]
    for k in range(1, reach + 1):
        series = series + landed[k - 1]
    series = series + jnp.concatenate([risen[...], jnp.zeros((half - EDGE, LANES), jnp.float32)], axis=0)
    lane = lax.broadcasted_iota(jnp.int32, (1, LANES), 1)

    def fold(value, op):
        return op(value, pltpu.roll(value, trials, 1))

    def low_half(value):
        return jnp.where(lane < trials, value, pltpu.roll(value, trials, 1))

    def high_half(value):
        return jnp.where(lane < trials, pltpu.roll(value, trials, 1), value)

    mean = fold(jnp.sum(series, axis=0, keepdims=True), jnp.add) * (1.0 / frames)
    away = series - mean
    spread = fold(jnp.sum(away * away, axis=0, keepdims=True), jnp.add)
    peak = fold(jnp.max(series, axis=0, keepdims=True), jnp.maximum)
    mine[...] = jnp.concatenate([jnp.where(lane < trials, mean, spread), peak], axis=0)

    def far(k):
        return pltpu.make_async_remote_copy(
            src_ref=mine, dst_ref=gathered.at[k - 1],
            send_sem=far_send.at[k - 1], recv_sem=far_recv.at[k - 1],
            device_id={"tm": lax.rem(me + k, count)}, device_id_type=MESH,
        )

    for k in range(1, count):
        far(k).start()
    live = jnp.maximum(jnp.sum(mask_ref[...].astype(jnp.float32)), 1.0)
    for k in range(1, count):
        far(k).wait_recv()
    sums = gathered[:, 0, :]
    tops = gathered[:, 1, :]
    average = (mean + low_half(jnp.sum(sums, axis=0, keepdims=True))) * (1.0 / count)
    offset = sums - average
    squares = spread + high_half(jnp.sum(sums, axis=0, keepdims=True))
    between = (mean - average) * (mean - average) + low_half(jnp.sum(offset * offset, axis=0, keepdims=True))
    variance = (squares + frames * between) * (1.0 / (frames * count))
    top = jnp.maximum(peak, jnp.max(tops, axis=0, keepdims=True))
    deviation = jnp.sqrt(variance + 1e-05)
    z = (series - average) / deviation
    z_ref[0:half, :] = z[:, :trials]
    z_ref[half:frames, :] = pltpu.roll(z, trials, 1)[:, :trials]
    stats_ref[...] = jnp.concatenate(
        [average / live, deviation / live, (top - average) / deviation], axis=0
    )[:, :trials]

    @pl.when(me < count - 1)
    def _():
        forward().wait_send()
        up().wait_send()

    @pl.when(me > 0)
    def _():
        backward().wait_send()

    for k in range(1, reach + 1):
        @pl.when(me >= k)
        def _():
            near(k).wait_send()
    for k in range(1, count):
        far(k).wait_send()


def finish_kernel(z_ref, stats_ref, z_out, stats_out, sem):
    first = pltpu.make_async_copy(z_ref, z_out, sem.at[0])
    second = pltpu.make_async_copy(stats_ref, stats_out, sem.at[1])
    first.start()
    second.start()
    first.wait()
    second.wait()


def per_device(voltage, delays, chan_mask):
    frames = voltage.shape[2] // NCHAN
    trials = delays.shape[0]
    count = lax.axis_size("tm")
    lines = 2 * RADIX
    half = frames // 2
    blocks = LANES // RADIX
    wide = NCHAN // blocks
    reach = MAXD // frames
    steps = HALF + 2
    past = TAPS - 1
    vmem = pl.BlockSpec(memory_space=pltpu.VMEM)
    hbm = pl.BlockSpec(memory_space=pltpu.HBM)
    framed = voltage.reshape(2, 2, frames * RADIX, LANES).transpose(0, 2, 1, 3).reshape(2, frames, lines, LANES)
    operands = (framed, jnp.asarray(prototype()), jnp.asarray(twiddles()), jnp.asarray(transform_table()), delays,
                chan_mask.reshape(RADIX, LANES))
    dma = pltpu.SemaphoreType.DMA
    outputs = (
        jax.ShapeDtypeStruct((frames, trials), jnp.float32),
        jax.ShapeDtypeStruct((3, trials), jnp.float32),
    )
    results = pl.pallas_call(
        functools.partial(beam_kernel, count, frames, trials),
        out_shape=outputs,
        in_specs=[hbm] * 6,
        out_specs=(vmem,) * 2,
        scratch_shapes=[
            pltpu.VMEM((2, frames, lines, LANES), jnp.bfloat16),
            pltpu.VMEM((TAPS, PITCH, LANES), jnp.float32),
            pltpu.VMEM((2, RADIX, LANES), jnp.float32),
            pltpu.VMEM((2, 2 * LANES, 2 * LANES), jnp.bfloat16),
            pltpu.VMEM((trials, NCHAN), jnp.int32),
            pltpu.VMEM((RADIX, LANES), jnp.int32),
            pltpu.VMEM((2, past - EDGE, lines, LANES), jnp.bfloat16),
            pltpu.VMEM((2, EDGE, lines, LANES), jnp.bfloat16),
            pltpu.VMEM((2, frames + past + EDGE, PITCH, LANES), jnp.float32),
            pltpu.VMEM((frames * PITCH, LANES), jnp.float32),
            pltpu.VMEM((RADIX * frames, 2 * LANES), jnp.float32),
            pltpu.VMEM((blocks, frames, 2 * LANES), jnp.float32),
            pltpu.VMEM((blocks, EDGE, 2 * LANES), jnp.float32),
            pltpu.VMEM((steps + 6, LANES), jnp.int32),
            pltpu.VMEM((steps + 6, LANES), jnp.float32),
            pltpu.VMEM((steps // 2, wide, 2 * LANES), jnp.bfloat16),
            pltpu.VMEM((8, HALF + frames + 2 * EDGE, LANES), jnp.float32),
            pltpu.VMEM(((reach + 1) * half + EDGE, LANES), jnp.float32),
            pltpu.VMEM((reach, half, LANES), jnp.float32),
            pltpu.VMEM((EDGE, LANES), jnp.float32),
            pltpu.VMEM((2, LANES), jnp.float32),
            pltpu.VMEM((count - 1, 2, LANES), jnp.float32),
            dma((6,)),
            dma((2,)),
            dma((2,)),
            dma((reach + 1,)),
            dma((reach + 1,)),
            dma((count - 1,)),
            dma((count - 1,)),
            pltpu.SemaphoreType.REGULAR((8,)),
        ],
        compiler_params=pltpu.CompilerParams(collective_id=1, vmem_limit_bytes=GRANT, has_side_effects=True),
        name="beam",
    )(*[pltpu.with_memory_space_constraint(v, pltpu.HBM) for v in operands])
    zscore, trial_stats = pl.pallas_call(
        finish_kernel,
        out_shape=outputs,
        in_specs=[vmem] * 2,
        out_specs=(hbm,) * 2,
        scratch_shapes=[dma((2,))],
        compiler_params=pltpu.CompilerParams(vmem_limit_bytes=GRANT),
        name="finish",
    )(*results)
    return (zscore.T, trial_stats)


def solution(mesh):
    in_specs = (P(None, None, ("beam", "tm")), P(), P("beam"))
    out_specs = (P(None, ("beam", "tm")), P(None, "beam"))
    return jax.shard_map(
        per_device, mesh=mesh, in_specs=in_specs, out_specs=out_specs, check_vma=False
    )
```

```python
import functools
import math

import jax
import jax.numpy as jnp
import numpy as np
from jax import lax
from jax.experimental import pallas as pl
from jax.experimental.pallas import tpu as pltpu
from jax.sharding import PartitionSpec as P

NCHAN = 2048
TAPS = 16
LANES = 128
RADIX = NCHAN // LANES
MAXD = 96
EDGE = 8
HALF = MAXD // 2
PITCH = 40
GRANT = 32 * 1024 * 1024
MESH = pl.DeviceIdType.MESH


def prototype():
    length = TAPS * NCHAN
    position = np.arange(length, dtype=np.float64)
    window = 0.54 - 0.46 * np.cos(2.0 * np.pi * position / (length - 1))
    shaped = np.sinc((position - (length - 1) / 2.0) / NCHAN) * window
    shaped = shaped * np.sqrt(NCHAN / np.sum(shaped * shaped))
    taps = shaped.reshape(TAPS, RADIX, 1, LANES)
    taps = np.broadcast_to(taps, (TAPS, RADIX, 2, LANES))
    return taps.reshape(TAPS, 2 * RADIX, LANES).astype(np.float32)


def twiddles():
    angle = -2.0 * np.pi * np.outer(np.arange(RADIX), np.arange(LANES)) / NCHAN
    return np.stack([np.cos(angle), np.sin(angle)]).astype(np.float32)


def transform_table():
    angle = -2.0 * np.pi * (np.outer(np.arange(LANES), np.arange(LANES)) % LANES) / LANES
    scale = 1.0 / math.sqrt(NCHAN)
    cos, sin = np.cos(angle) * scale, np.sin(angle) * scale
    full = np.block([[cos, sin], [-sin, cos]]).astype(np.float32)
    high = full.astype(jnp.bfloat16)
    low = (full - high.astype(np.float32)).astype(jnp.bfloat16)
    return np.stack([high, low])


def butterflies(items):
    count = len(items)
    if count == 1:
        return items
    even = butterflies(items[0::2])
    odd = butterflies(items[1::2])
    half = count // 2
    out = [None] * count
    for k in range(half):
        re, im = odd[k]
        if k == 0:
            tr, ti = re, im
        elif 4 * k == count:
            tr, ti = im, -re
        elif 8 * k == count:
            r = math.sqrt(0.5)
            tr, ti = (re + im) * r, (im - re) * r
        elif 8 * k == 3 * count:
            r = math.sqrt(0.5)
            tr, ti = (im - re) * r, (re + im) * (-r)
        else:
            c, s = math.cos(2 * math.pi * k / count), -math.sin(2 * math.pi * k / count)
            tr, ti = re * c - im * s, re * s + im * c
        er, ei = even[k]
        out[k] = (er + tr, ei + ti)
        out[k + half] = (er - tr, ei - ti)
    return out


def wait_some(sem, amount):
    @pl.when(amount > 0)
    def _():
        pl.semaphore_wait(sem, amount)


def beam_kernel(count, frames, trials, volt_hbm, taps_hbm, twid_hbm, table_hbm, delay_hbm, mask_hbm, z_ref, stats_ref,
                volt_ref, taps_ref, twid_ref, table_ref, delay_ref, mask_ref, before, after, ext, weighted, sections,
                spread_out, early, blockno, within, acc, part, landed, risen, mine, gathered,
                load_sem, halo_send, halo_recv, near_send, near_recv, far_send, far_recv, know):
    me = lax.axis_index("tm")
    past = TAPS - 1
    lead = past - EDGE
    lines = 2 * RADIX
    own = EDGE + lead
    blocks = LANES // RADIX
    wide = NCHAN // blocks
    reach = MAXD // frames
    steps = HALF + 2
    barrier = pltpu.get_barrier_semaphore()

    def here(k):
        return (me + k >= 0) & (me + k < count)

    def tell(sem, k):
        @pl.when(here(k))
        def _():
            pl.semaphore_signal(sem, inc=1, device_id={"tm": me + k}, device_id_type=MESH)

    def number(distances):
        return sum(jnp.where(here(k), 1, 0) for k in distances)

    close = [k for d in range(1, reach + 1) for k in (-d, d)]
    for k in close:
        tell(barrier, k)
    pairs = ((volt_hbm, volt_ref), (taps_hbm, taps_ref.at[:, pl.ds(0, lines)]), (delay_hbm, delay_ref), (twid_hbm, twid_ref),
             (table_hbm, table_ref), (mask_hbm, mask_ref))
    loads = [pltpu.make_async_copy(a, b, load_sem.at[i]) for i, (a, b) in enumerate(pairs)]
    for load in loads:
        load.start()

    def forward():
        return pltpu.make_async_remote_copy(
            src_ref=volt_ref.at[:, pl.ds(frames - lead, lead)], dst_ref=before,
            send_sem=halo_send.at[0], recv_sem=halo_recv.at[0], device_id={"tm": me + 1}, device_id_type=MESH,
        )

    def backward():
        return pltpu.make_async_remote_copy(
            src_ref=volt_ref.at[:, pl.ds(0, EDGE)], dst_ref=after,
            send_sem=halo_send.at[1], recv_sem=halo_recv.at[1], device_id={"tm": me - 1}, device_id_type=MESH,
        )

    loads[0].wait()
    for p in range(2):
        ext[p, own:own + frames, 0:lines] = volt_ref[p].astype(jnp.float32)
    wait_some(barrier, number(close))

    @pl.when(me < count - 1)
    def _():
        forward().start()

    @pl.when(me > 0)
    def _():
        backward().start()

    rounds = []
    known = reach
    while known < count - 1:
        rounds.append(known)
        known *= 2

    def open_round(i):
        if i < len(rounds):
            for k in (-rounds[i], rounds[i]):
                tell(know.at[i], k)

    def close_round(i):
        if i < len(rounds):
            wait_some(know.at[i], number((-rounds[i], rounds[i])))

    open_round(0)
    for load in loads[1:]:
        load.wait()

    row = lax.broadcasted_iota(jnp.int32, (blocks, LANES), 1)
    even = mask_ref[pl.ds(0, blocks, stride=2), :]
    odd = mask_ref[pl.ds(1, blocks, stride=2), :]
    usable = []
    for h in range(2):
        place = (row & 7) * RADIX + 8 * h + (row >> 4)
        low = jnp.take_along_axis(even, place, axis=1, mode="promise_in_bounds")
        high = jnp.take_along_axis(odd, place, axis=1, mode="promise_in_bounds")
        usable.append(jnp.where((row & 8) == 0, low, high).astype(jnp.float32))

    def fir(begin, size):
        for part_index in range(lines // 8):
            rows = pl.ds(8 * part_index, 8)
            taps = [taps_ref[j, rows, :] for j in range(TAPS)]

            def some(g, carry):
                for p in range(2):
                    sums = [None] * 4
                    for i in range(TAPS + 3):
                        sample = ext[p, begin + EDGE + 4 * g + i, rows, :]
                        for f in range(4):
                            if 0 <= i - f < TAPS:
                                term = taps[i - f] * sample
                                sums[f] = term if sums[f] is None else sums[f] + term
                    for f in range(4):
                        start = pl.multiple_of((p * size + 4 * g + f) * PITCH, 8) + 8 * part_index
                        weighted[pl.ds(start, 8), :] = sums[f]
                return carry

            lax.fori_loop(0, size // 4, some, 0)

    def transform(size, out, begin, scale):
        group = 8
        rows_half = 2 * size
        for g in range(rows_half // group):
            p, f = divmod(g * group, size)
            first = (p * size + f) * PITCH
            items = []
            for m in range(RADIX):
                re = weighted[pl.ds(first + 2 * m, group, stride=PITCH), :]
                im = weighted[pl.ds(first + 2 * m + 1, group, stride=PITCH), :]
                items.append((re, im))
            for k1, (re, im) in enumerate(butterflies(items)):
                if k1:
                    c, s = twid_ref[0, k1:k1 + 1, :], twid_ref[1, k1:k1 + 1, :]
                    re, im = re * c - im * s, re * s + im * c
                place = k1 * rows_half + g * group
                sections[place:place + group, :LANES] = re
                sections[place:place + group, LANES:] = im
        both = sections[0:RADIX * rows_half, :]
        high = both.astype(jnp.bfloat16)
        low = (both - high.astype(jnp.float32)).astype(jnp.bfloat16)
        dot = functools.partial(jnp.dot, preferred_element_type=jnp.float32)
        spec = dot(high, table_ref[0]) + (dot(high, table_ref[1]) + dot(low, table_ref[0]))
        spec = spec * spec
        both_pols = (spec[:, :LANES] + spec[:, LANES:]).reshape(RADIX, 2, size, LANES)
        energy = both_pols[:, 0] + both_pols[:, 1]
        chunk = lax.broadcasted_iota(jnp.int32, (size, LANES), 1) >> 4
        for h in range(2):
            parts = [energy[8 * h + i] for i in range(8)]
            for bit in (4, 2, 1):
                kept = (chunk & bit) == 0
                for i in range(8):
                    if i & bit == 0:
                        low_part, high_part = parts[i], parts[i | bit]
                        parts[i] = jnp.where(kept, low_part, pltpu.roll(high_part, bit * RADIX, 1))
                        parts[i | bit] = jnp.where(kept, pltpu.roll(low_part, LANES - bit * RADIX, 1), high_part)
            for b in range(blocks):
                out[b, pl.ds(begin, size), h * LANES:(h + 1) * LANES] = parts[b] * (usable[h][b:b + 1] * scale)

    fir(EDGE, frames // 2)
    transform(frames // 2, spread_out, EDGE, 1.0)
    close_round(0)
    open_round(1)

    level = lax.broadcasted_iota(jnp.int32, (8, LANES), 1)

    def look(table, place):
        return jnp.take_along_axis(table, place, axis=1, mode="promise_in_bounds")

    tables = NCHAN // LANES
    groups = range(trials // 8)
    each = (level & (LANES // tables - 1)) * tables + (tables - 1)

    def table(g, b):
        return delay_ref[8 * g:8 * g + 8, b * LANES:(b + 1) * LANES]

    seldom = []
    for g in groups:
        kept = jnp.zeros((8, LANES), jnp.int32)
        for b in range(tables):
            kept = jnp.where((level >> 3) == b, look(table(g, b), each), kept)
        seldom.append(kept)
    coarse = [jnp.zeros((8, LANES), jnp.int32) for g in groups]
    for step in (64, 32, 16, 8, 4, 2, 1):
        for g in groups:
            seen = look(seldom[g], coarse[g] + (step - 1))
            coarse[g] = jnp.where(seen >= level, coarse[g] + step, coarse[g])
    fine = [jnp.zeros((8, LANES), jnp.int32) for g in groups]
    for step in (8, 4, 2, 1):
        for g in groups:
            place = (coarse[g] & 7) * tables + fine[g] + (step - 1)
            which = coarse[g] >> 3
            seen = jnp.full((8, LANES), -1, jnp.int32)
            for b in range(tables):
                seen = jnp.where(which == b, look(table(g, b), place), seen)
            fine[g] = jnp.where(seen >= level, fine[g] + step, fine[g])
    total = jnp.concatenate(
        [jnp.where(level == 0, NCHAN, coarse[g] * tables + fine[g]).astype(jnp.float32) for g in groups], axis=0)
    turned = jnp.concatenate([total, jnp.zeros((LANES - trials, LANES), jnp.float32)], axis=0).T
    rows_kept = blockno.shape[0]
    near_side = lax.broadcasted_iota(jnp.int32, (rows_kept, LANES), 1) < trials
    total = jnp.where(
        near_side, turned[0:rows_kept], pltpu.roll(turned[HALF:HALF + rows_kept], trials, 1)
    ).astype(jnp.int32)
    blockno[...] = total >> 8
    within[...] = (total & (wide - 1)).astype(jnp.float32)
    close_round(1)
    open_round(2)
    order = lax.broadcasted_iota(jnp.int32, (wide, LANES), 0)
    order = ((order & (RADIX - 1)) * RADIX + (order >> 4)).astype(jnp.float32)

    order = order.astype(jnp.bfloat16)

    def pick(j):
        end = jnp.broadcast_to(within[j:j + 1, :], (wide, LANES)).astype(jnp.bfloat16)
        return jnp.minimum(jnp.maximum(end - order, jnp.zeros_like(end)), jnp.ones_like(end))

    acc[...] = jnp.zeros_like(acc)

    def dedisperse(source, size, offset):
        values = jnp.concatenate([source[b] for b in range(blocks)], axis=0).astype(jnp.bfloat16)
        dot = functools.partial(jnp.dot, preferred_element_type=jnp.float32)
        sums = dot(values, jnp.ones((wide, LANES), jnp.bfloat16))
        column = lax.broadcasted_iota(jnp.int32, (size, LANES), 1)
        prefix = jnp.zeros((size, LANES), jnp.float32)
        for b in range(blocks):
            prefix = prefix + jnp.where(column > b, sums[b * size:(b + 1) * size], 0.0)
        last = None
        for i in range(steps // 2):
            found = dot(values, jnp.concatenate([pick(2 * i), pick(2 * i + 1)], axis=1))
            for side in range(2):
                j = 2 * i + side
                which = jnp.broadcast_to(blockno[j:j + 1, :], (size, LANES))
                inner = jnp.zeros((size, LANES), jnp.float32)
                for b in range(blocks):
                    inner = jnp.where(which == b, found[b * size:(b + 1) * size, side * LANES:(side + 1) * LANES], inner)
                now = inner + jnp.take_along_axis(prefix, which, axis=1, mode="promise_in_bounds")
                if j:
                    change = last - now
                    if j - 1 == HALF:
                        change = jnp.where(column < trials, 0.0, change)
                    a, m = divmod(j - 1, 8)
                    place = HALF + EDGE + offset - 8 * a
                    acc[m, place:place + size] += change
                last = now

    @pl.when(me == 0)
    def _():
        for p in range(2):
            ext[p, 0:own, 0:lines] = jnp.zeros((own, lines, LANES), jnp.float32)
        fir(-EDGE, EDGE)
        transform(EDGE, early, 0, 1.0)
        dedisperse(early, EDGE, -EDGE)

    for i in range(2):
        from_before = lax.rem(me + i, 2) == 1
        begin = pl.multiple_of(jnp.where(from_before, 0, frames - EDGE), EDGE)

        @pl.when(from_before & (me > 0))
        def _():
            forward().wait_recv()
            for p in range(2):
                ext[p, EDGE:own, 0:lines] = before[p].astype(jnp.float32)

        @pl.when(jnp.logical_not(from_before) & (me < count - 1))
        def _():
            backward().wait_recv()
            for p in range(2):
                ext[p, own + frames:own + frames + EDGE, 0:lines] = after[p].astype(jnp.float32)

        @pl.when(jnp.logical_not(from_before) & (me == count - 1))
        def _():
            for p in range(2):
                ext[p, own + frames:own + frames + EDGE, 0:lines] = jnp.zeros((EDGE, lines, LANES), jnp.float32)

        fir(begin, EDGE)
        ended = jnp.logical_not(from_before) & (me == count - 1)
        transform(EDGE, spread_out, begin, jnp.where(ended, 0.0, 1.0))

    dedisperse(spread_out, frames, 0)
    height = HALF + frames + EDGE
    total = acc[0, 0:height]
    for m in range(1, 8):
        total = total + acc[m, m:m + height]
    side = lax.broadcasted_iota(jnp.int32, (8, LANES), 1) < trials
    empty = jnp.zeros((8, LANES), jnp.float32)

    def joined(r):
        first = total[r - HALF:r - HALF + 8] if HALF <= r < HALF + height else empty
        other = total[r:r + 8] if r < height else empty
        mixed = jnp.where(side, first, other)
        return mixed + pltpu.roll(mixed, trials, 1)

    half = frames // 2
    for q in range(reach + 1):
        for r in range(0, half, 8):
            top = joined(q * frames + r)
            low = joined(q * frames + half + r)
            part[q * half + r:q * half + r + 8, :] = jnp.where(side, top, low)
    rise = (reach + 1) * frames
    part[(reach + 1) * half:(reach + 1) * half + EDGE, :] = jnp.where(side, joined(rise), 0.0)

    def near(k):
        return pltpu.make_async_remote_copy(
            src_ref=part.at[pl.ds((reach - k) * half, half)], dst_ref=landed.at[k - 1],
            send_sem=near_send.at[k - 1], recv_sem=near_recv.at[k - 1],
            device_id={"tm": me - k}, device_id_type=MESH,
        )

    def up():
        return pltpu.make_async_remote_copy(
            src_ref=part.at[pl.ds((reach + 1) * half, EDGE)], dst_ref=risen,
            send_sem=near_send.at[reach], recv_sem=near_recv.at[reach],
            device_id={"tm": me + 1}, device_id_type=MESH,
        )

    for k in range(reach, 0, -1):
        @pl.when(me >= k)
        def _():
            near(k).start()

    @pl.when(me < count - 1)
    def _():
        up().start()

    for i in range(2, len(rounds)):
        close_round(i)
        open_round(i + 1)

    @pl.when(me == 0)
    def _():
        risen[...] = jnp.zeros_like(risen)

    @pl.when(me > 0)
    def _():
        up().wait_recv()

    for k in range(1, reach + 1):
        @pl.when(me + k >= count)
        def _():
            landed[k - 1] = jnp.zeros((half, LANES), jnp.float32)

        @pl.when(me + k < count)
        def _():
            near(k).wait_recv()

    series = part[reach * half:(reach + 1) * half, :]
    for k in range(1, reach + 1):
        series = series + landed[k - 1]
    series = series + jnp.concatenate([risen[...], jnp.zeros((half - EDGE, LANES), jnp.float32)], axis=0)
    lane = lax.broadcasted_iota(jnp.int32, (1, LANES), 1)

    def fold(value, op):
        return op(value, pltpu.roll(value, trials, 1))

    def low_half(value):
        return jnp.where(lane < trials, value, pltpu.roll(value, trials, 1))

    def high_half(value):
        return jnp.where(lane < trials, pltpu.roll(value, trials, 1), value)

    mean = fold(jnp.sum(series, axis=0, keepdims=True), jnp.add) * (1.0 / frames)
    away = series - mean
    spread = fold(jnp.sum(away * away, axis=0, keepdims=True), jnp.add)
    peak = fold(jnp.max(series, axis=0, keepdims=True), jnp.maximum)
    mine[...] = jnp.concatenate([jnp.where(lane < trials, mean, spread), peak], axis=0)

    def far(k):
        return pltpu.make_async_remote_copy(
            src_ref=mine, dst_ref=gathered.at[k - 1],
            send_sem=far_send.at[k - 1], recv_sem=far_recv.at[k - 1],
            device_id={"tm": lax.rem(me + k, count)}, device_id_type=MESH,
        )

    for k in range(1, count):
        far(k).start()
    live = jnp.maximum(jnp.sum(mask_ref[...].astype(jnp.float32)), 1.0)
    for k in range(1, count):
        far(k).wait_recv()
    sums = gathered[:, 0, :]
    tops = gathered[:, 1, :]
    average = (mean + low_half(jnp.sum(sums, axis=0, keepdims=True))) * (1.0 / count)
    offset = sums - average
    squares = spread + high_half(jnp.sum(sums, axis=0, keepdims=True))
    between = (mean - average) * (mean - average) + low_half(jnp.sum(offset * offset, axis=0, keepdims=True))
    variance = (squares + frames * between) * (1.0 / (frames * count))
    top = jnp.maximum(peak, jnp.max(tops, axis=0, keepdims=True))
    deviation = jnp.sqrt(variance + 1e-05)
    z = (series - average) / deviation
    z_ref[0:half, :] = z[:, :trials]
    z_ref[half:frames, :] = pltpu.roll(z, trials, 1)[:, :trials]
    stats_ref[...] = jnp.concatenate(
        [average / live, deviation / live, (top - average) / deviation], axis=0
    )[:, :trials]

    @pl.when(me < count - 1)
    def _():
        forward().wait_send()
        up().wait_send()

    @pl.when(me > 0)
    def _():
        backward().wait_send()

    for k in range(1, reach + 1):
        @pl.when(me >= k)
        def _():
            near(k).wait_send()
    for k in range(1, count):
        far(k).wait_send()


def finish_kernel(z_ref, stats_ref, z_out, stats_out, sem):
    first = pltpu.make_async_copy(z_ref, z_out, sem.at[0])
    second = pltpu.make_async_copy(stats_ref, stats_out, sem.at[1])
    first.start()
    second.start()
    first.wait()
    second.wait()


def per_device(voltage, delays, chan_mask):
    frames = voltage.shape[2] // NCHAN
    trials = delays.shape[0]
    count = lax.axis_size("tm")
    lines = 2 * RADIX
    half = frames // 2
    blocks = LANES // RADIX
    wide = NCHAN // blocks
    reach = MAXD // frames
    steps = HALF + 2
    past = TAPS - 1
    vmem = pl.BlockSpec(memory_space=pltpu.VMEM)
    hbm = pl.BlockSpec(memory_space=pltpu.HBM)
    framed = voltage.reshape(2, 2, frames * RADIX, LANES).transpose(0, 2, 1, 3).reshape(2, frames, lines, LANES)
    operands = (framed, jnp.asarray(prototype()), jnp.asarray(twiddles()), jnp.asarray(transform_table()), delays,
                chan_mask.reshape(RADIX, LANES))
    dma = pltpu.SemaphoreType.DMA
    outputs = (
        jax.ShapeDtypeStruct((frames, trials), jnp.float32),
        jax.ShapeDtypeStruct((3, trials), jnp.float32),
    )
    results = pl.pallas_call(
        functools.partial(beam_kernel, count, frames, trials),
        out_shape=outputs,
        in_specs=[hbm] * 6,
        out_specs=(vmem,) * 2,
        scratch_shapes=[
            pltpu.VMEM((2, frames, lines, LANES), jnp.bfloat16),
            pltpu.VMEM((TAPS, PITCH, LANES), jnp.float32),
            pltpu.VMEM((2, RADIX, LANES), jnp.float32),
            pltpu.VMEM((2, 2 * LANES, 2 * LANES), jnp.bfloat16),
            pltpu.VMEM((trials, NCHAN), jnp.int32),
            pltpu.VMEM((RADIX, LANES), jnp.int32),
            pltpu.VMEM((2, past - EDGE, lines, LANES), jnp.bfloat16),
            pltpu.VMEM((2, EDGE, lines, LANES), jnp.bfloat16),
            pltpu.VMEM((2, frames + past + EDGE, PITCH, LANES), jnp.float32),
            pltpu.VMEM((frames * PITCH, LANES), jnp.float32),
            pltpu.VMEM((RADIX * frames, 2 * LANES), jnp.float32),
            pltpu.VMEM((blocks, frames, 2 * LANES), jnp.float32),
            pltpu.VMEM((blocks, EDGE, 2 * LANES), jnp.float32),
            pltpu.VMEM((steps + 6, LANES), jnp.int32),
            pltpu.VMEM((steps + 6, LANES), jnp.float32),
            pltpu.VMEM((8, HALF + frames + 2 * EDGE, LANES), jnp.float32),
            pltpu.VMEM(((reach + 1) * half + EDGE, LANES), jnp.float32),
            pltpu.VMEM((reach, half, LANES), jnp.float32),
            pltpu.VMEM((EDGE, LANES), jnp.float32),
            pltpu.VMEM((2, LANES), jnp.float32),
            pltpu.VMEM((count - 1, 2, LANES), jnp.float32),
            dma((6,)),
            dma((2,)),
            dma((2,)),
            dma((reach + 1,)),
            dma((reach + 1,)),
            dma((count - 1,)),
            dma((count - 1,)),
            pltpu.SemaphoreType.REGULAR((8,)),
        ],
        compiler_params=pltpu.CompilerParams(collective_id=1, vmem_limit_bytes=GRANT, has_side_effects=True),
        name="beam",
    )(*[pltpu.with_memory_space_constraint(v, pltpu.HBM) for v in operands])
    zscore, trial_stats = pl.pallas_call(
        finish_kernel,
        out_shape=outputs,
        in_specs=[vmem] * 2,
        out_specs=(hbm,) * 2,
        scratch_shapes=[dma((2,))],
        compiler_params=pltpu.CompilerParams(vmem_limit_bytes=GRANT),
        name="finish",
    )(*results)
    return (zscore.T, trial_stats)


def solution(mesh):
    in_specs = (P(None, None, ("beam", "tm")), P(), P("beam"))
    out_specs = (P(None, ("beam", "tm")), P(None, "beam"))
    return jax.shard_map(
        per_device, mesh=mesh, in_specs=in_specs, out_specs=out_specs, check_vma=False
    )
```

```python
import functools
import math

import jax
import jax.numpy as jnp
import numpy as np
from jax import lax
from jax.experimental import pallas as pl
from jax.experimental.pallas import tpu as pltpu
from jax.sharding import PartitionSpec as P

NCHAN = 2048
TAPS = 16
LANES = 128
RADIX = NCHAN // LANES
MAXD = 96
EDGE = 8
HALF = MAXD // 2
PITCH = 40
GRANT = 32 * 1024 * 1024
MESH = pl.DeviceIdType.MESH


def prototype():
    length = TAPS * NCHAN
    position = np.arange(length, dtype=np.float64)
    window = 0.54 - 0.46 * np.cos(2.0 * np.pi * position / (length - 1))
    shaped = np.sinc((position - (length - 1) / 2.0) / NCHAN) * window
    shaped = shaped * np.sqrt(NCHAN / np.sum(shaped * shaped))
    taps = shaped.reshape(TAPS, RADIX, 1, LANES)
    taps = np.broadcast_to(taps, (TAPS, RADIX, 2, LANES))
    return taps.reshape(TAPS, 2 * RADIX, LANES).astype(np.float32)


def twiddles():
    angle = -2.0 * np.pi * np.outer(np.arange(RADIX), np.arange(LANES)) / NCHAN
    return np.stack([np.cos(angle), np.sin(angle)]).astype(np.float32)


def transform_table():
    angle = -2.0 * np.pi * (np.outer(np.arange(LANES), np.arange(LANES)) % LANES) / LANES
    scale = 1.0 / math.sqrt(NCHAN)
    cos, sin = np.cos(angle) * scale, np.sin(angle) * scale
    full = np.block([[cos, sin], [-sin, cos]]).astype(np.float32)
    high = full.astype(jnp.bfloat16)
    low = (full - high.astype(np.float32)).astype(jnp.bfloat16)
    return np.stack([high, low])


def butterflies(items):
    count = len(items)
    if count == 1:
        return items
    even = butterflies(items[0::2])
    odd = butterflies(items[1::2])
    half = count // 2
    out = [None] * count
    for k in range(half):
        re, im = odd[k]
        if k == 0:
            tr, ti = re, im
        elif 4 * k == count:
            tr, ti = im, -re
        elif 8 * k == count:
            r = math.sqrt(0.5)
            tr, ti = (re + im) * r, (im - re) * r
        elif 8 * k == 3 * count:
            r = math.sqrt(0.5)
            tr, ti = (im - re) * r, (re + im) * (-r)
        else:
            c, s = math.cos(2 * math.pi * k / count), -math.sin(2 * math.pi * k / count)
            tr, ti = re * c - im * s, re * s + im * c
        er, ei = even[k]
        out[k] = (er + tr, ei + ti)
        out[k + half] = (er - tr, ei - ti)
    return out


def wait_some(sem, amount):
    @pl.when(amount > 0)
    def _():
        pl.semaphore_wait(sem, amount)


def beam_kernel(count, frames, trials, volt_hbm, taps_hbm, twid_hbm, table_hbm, delay_hbm, mask_hbm, z_ref, stats_ref,
                volt_ref, taps_ref, twid_ref, table_ref, delay_ref, mask_ref, before, after, ext, weighted, sections,
                spread_out, early, tally, blockno, within, acc, part, landed, risen, mine, gathered,
                load_sem, halo_send, halo_recv, near_send, near_recv, far_send, far_recv, swap_sem, know):
    me = lax.axis_index("tm")
    past = TAPS - 1
    lead = past - EDGE
    lines = 2 * RADIX
    own = EDGE + lead
    blocks = LANES // RADIX
    wide = NCHAN // blocks
    reach = MAXD // frames
    steps = HALF + 2
    share = trials // 2
    core = lax.rem(me, 2)
    first = pl.multiple_of(core * share, share)
    barrier = pltpu.get_barrier_semaphore()

    def here(k):
        return (me + k >= 0) & (me + k < count)

    def tell(sem, k):
        @pl.when(here(k))
        def _():
            pl.semaphore_signal(sem, inc=1, device_id={"tm": me + k}, device_id_type=MESH)

    def number(distances):
        return sum(jnp.where(here(k), 1, 0) for k in distances)

    close = (-1, 1)
    for k in close:
        tell(barrier, k)
    pairs = ((volt_hbm, volt_ref), (taps_hbm, taps_ref.at[:, pl.ds(0, lines)]), (delay_hbm.at[pl.ds(first, share)], delay_ref), (twid_hbm, twid_ref),
             (table_hbm, table_ref), (mask_hbm, mask_ref))
    loads = [pltpu.make_async_copy(a, b, load_sem.at[i]) for i, (a, b) in enumerate(pairs)]
    for load in loads:
        load.start()

    def forward():
        return pltpu.make_async_remote_copy(
            src_ref=volt_ref.at[:, pl.ds(frames - lead, lead)], dst_ref=before,
            send_sem=halo_send.at[0], recv_sem=halo_recv.at[0], device_id={"tm": me + 1}, device_id_type=MESH,
        )

    def backward():
        return pltpu.make_async_remote_copy(
            src_ref=volt_ref.at[:, pl.ds(0, EDGE)], dst_ref=after,
            send_sem=halo_send.at[1], recv_sem=halo_recv.at[1], device_id={"tm": me - 1}, device_id_type=MESH,
        )

    loads[0].wait()
    for p in range(2):
        ext[p, own:own + frames, 0:lines] = volt_ref[p].astype(jnp.float32)
    wait_some(barrier, number(close))

    @pl.when((core == 1) & (me < count - 1))
    def _():
        forward().start()

    @pl.when(me > 0)
    def _():
        backward().start()

    @pl.when((core == 0) & (me < count - 1))
    def _():
        forward().start()

    rounds = []
    known = 1
    while known < count - 1:
        rounds.append(known)
        known *= 2

    def open_round(i):
        if i < len(rounds):
            for k in (-rounds[i], rounds[i]):
                tell(know.at[i], k)

    def close_round(i):
        if i < len(rounds):
            wait_some(know.at[i], number((-rounds[i], rounds[i])))

    open_round(0)
    for load in loads[1:]:
        load.wait()

    row = lax.broadcasted_iota(jnp.int32, (blocks, LANES), 1)
    even = mask_ref[pl.ds(0, blocks, stride=2), :]
    odd = mask_ref[pl.ds(1, blocks, stride=2), :]
    usable = []
    for h in range(2):
        place = (row & 7) * RADIX + 8 * h + (row >> 4)
        low = jnp.take_along_axis(even, place, axis=1, mode="promise_in_bounds")
        high = jnp.take_along_axis(odd, place, axis=1, mode="promise_in_bounds")
        usable.append(jnp.where((row & 8) == 0, low, high).astype(jnp.float32))

    def fir(begin, size):
        for part_index in range(lines // 8):
            rows = pl.ds(8 * part_index, 8)
            taps = [taps_ref[j, rows, :] for j in range(TAPS)]

            def some(g, carry):
                for p in range(2):
                    sums = [None] * 4
                    for i in range(TAPS + 3):
                        sample = ext[p, begin + EDGE + 4 * g + i, rows, :]
                        for f in range(4):
                            if 0 <= i - f < TAPS:
                                term = taps[i - f] * sample
                                sums[f] = term if sums[f] is None else sums[f] + term
                    for f in range(4):
                        start = pl.multiple_of((p * size + 4 * g + f) * PITCH, 8) + 8 * part_index
                        weighted[pl.ds(start, 8), :] = sums[f]
                return carry

            lax.fori_loop(0, size // 4, some, 0)

    def transform(size, out, begin, scale):
        group = 8
        rows_half = 2 * size
        for g in range(rows_half // group):
            p, f = divmod(g * group, size)
            first = (p * size + f) * PITCH
            items = []
            for m in range(RADIX):
                re = weighted[pl.ds(first + 2 * m, group, stride=PITCH), :]
                im = weighted[pl.ds(first + 2 * m + 1, group, stride=PITCH), :]
                items.append((re, im))
            for k1, (re, im) in enumerate(butterflies(items)):
                if k1:
                    c, s = twid_ref[0, k1:k1 + 1, :], twid_ref[1, k1:k1 + 1, :]
                    re, im = re * c - im * s, re * s + im * c
                place = k1 * rows_half + g * group
                sections[place:place + group, :LANES] = re
                sections[place:place + group, LANES:] = im
        both = sections[0:RADIX * rows_half, :]
        high = both.astype(jnp.bfloat16)
        low = (both - high.astype(jnp.float32)).astype(jnp.bfloat16)
        dot = functools.partial(jnp.dot, preferred_element_type=jnp.float32)
        spec = dot(high, table_ref[0]) + (dot(high, table_ref[1]) + dot(low, table_ref[0]))
        spec = spec * spec
        both_pols = (spec[:, :LANES] + spec[:, LANES:]).reshape(RADIX, 2, size, LANES)
        energy = both_pols[:, 0] + both_pols[:, 1]
        chunk = lax.broadcasted_iota(jnp.int32, (size, LANES), 1) >> 4
        for h in range(2):
            parts = [energy[8 * h + i] for i in range(8)]
            for bit in (4, 2, 1):
                kept = (chunk & bit) == 0
                for i in range(8):
                    if i & bit == 0:
                        low_part, high_part = parts[i], parts[i | bit]
                        parts[i] = jnp.where(kept, low_part, pltpu.roll(high_part, bit * RADIX, 1))
                        parts[i | bit] = jnp.where(kept, pltpu.roll(low_part, LANES - bit * RADIX, 1), high_part)
            for b in range(blocks):
                out[b, pl.ds(begin, size), h * LANES:(h + 1) * LANES] = parts[b] * (usable[h][b:b + 1] * scale)

    level = lax.broadcasted_iota(jnp.int32, (8, LANES), 1)

    def look(table, place):
        return jnp.take_along_axis(table, place, axis=1, mode="promise_in_bounds")

    tables = NCHAN // LANES
    groups = range(share // 8)
    each = (level & (LANES // tables - 1)) * tables + (tables - 1)

    def table(g, b):
        return delay_ref[8 * g:8 * g + 8, b * LANES:(b + 1) * LANES]

    seldom = []
    for g in groups:
        kept = jnp.zeros((8, LANES), jnp.int32)
        for b in range(tables):
            kept = jnp.where((level >> 3) == b, look(table(g, b), each), kept)
        seldom.append(kept)
    coarse = [jnp.zeros((8, LANES), jnp.int32) for g in groups]
    for step in (64, 32, 16, 8, 4, 2, 1):
        for g in groups:
            seen = look(seldom[g], coarse[g] + (step - 1))
            coarse[g] = jnp.where(seen >= level, coarse[g] + step, coarse[g])
    fine = [jnp.zeros((8, LANES), jnp.int32) for g in groups]
    for step in (8, 4, 2, 1):
        for g in groups:
            place = (coarse[g] & 7) * tables + fine[g] + (step - 1)
            which = coarse[g] >> 3
            seen = jnp.full((8, LANES), -1, jnp.int32)
            for b in range(tables):
                seen = jnp.where(which == b, look(table(g, b), place), seen)
            fine[g] = jnp.where(seen >= level, fine[g] + step, fine[g])
    tally[pl.ds(first, share), :] = jnp.concatenate(
        [jnp.where(level == 0, NCHAN, coarse[g] * tables + fine[g]).astype(jnp.float32) for g in groups], axis=0)

    def swap():
        rows = pl.ds(first, share)
        return pltpu.make_async_remote_copy(
            src_ref=tally.at[rows], dst_ref=tally.at[rows],
            send_sem=swap_sem.at[0], recv_sem=swap_sem.at[1],
            device_id={"tm": me + 1 - 2 * core}, device_id_type=MESH,
        )

    swap().start()
    close_round(0)
    open_round(1)
    fir(EDGE, frames // 2)
    transform(frames // 2, spread_out, EDGE, 1.0)
    close_round(1)
    open_round(2)

    swap().wait_recv()
    total = tally[...]
    turned = jnp.concatenate([total, jnp.zeros((LANES - trials, LANES), jnp.float32)], axis=0).T
    rows_kept = blockno.shape[0]
    near_side = lax.broadcasted_iota(jnp.int32, (rows_kept, LANES), 1) < trials
    total = jnp.where(
        near_side, turned[0:rows_kept], pltpu.roll(turned[HALF:HALF + rows_kept], trials, 1)
    ).astype(jnp.int32)
    blockno[...] = total >> 8
    within[...] = (total & (wide - 1)).astype(jnp.float32)
    order = lax.broadcasted_iota(jnp.int32, (wide, LANES), 0)
    order = ((order & (RADIX - 1)) * RADIX + (order >> 4)).astype(jnp.float32)

    order = order.astype(jnp.bfloat16)

    def pick(j):
        end = jnp.broadcast_to(within[j:j + 1, :], (wide, LANES)).astype(jnp.bfloat16)
        return jnp.minimum(jnp.maximum(end - order, jnp.zeros_like(end)), jnp.ones_like(end))

    acc[...] = jnp.zeros_like(acc)

    def dedisperse(source, size, offset):
        values = jnp.concatenate([source[b] for b in range(blocks)], axis=0).astype(jnp.bfloat16)
        dot = functools.partial(jnp.dot, preferred_element_type=jnp.float32)
        sums = dot(values, jnp.ones((wide, LANES), jnp.bfloat16))
        column = lax.broadcasted_iota(jnp.int32, (size, LANES), 1)
        prefix = jnp.zeros((size, LANES), jnp.float32)
        for b in range(blocks):
            prefix = prefix + jnp.where(column > b, sums[b * size:(b + 1) * size], 0.0)
        last = None
        for i in range(steps // 2):
            found = dot(values, jnp.concatenate([pick(2 * i), pick(2 * i + 1)], axis=1))
            for side in range(2):
                j = 2 * i + side
                which = jnp.broadcast_to(blockno[j:j + 1, :], (size, LANES))
                inner = jnp.zeros((size, LANES), jnp.float32)
                for b in range(blocks):
                    inner = jnp.where(which == b, found[b * size:(b + 1) * size, side * LANES:(side + 1) * LANES], inner)
                now = inner + jnp.take_along_axis(prefix, which, axis=1, mode="promise_in_bounds")
                if j:
                    change = last - now
                    if j - 1 == HALF:
                        change = jnp.where(column < trials, 0.0, change)
                    a, m = divmod(j - 1, 8)
                    place = HALF + EDGE + offset - 8 * a
                    acc[m, place:place + size] += change
                last = now

    @pl.when(me == 0)
    def _():
        for p in range(2):
            ext[p, 0:own, 0:lines] = jnp.zeros((own, lines, LANES), jnp.float32)
        fir(-EDGE, EDGE)
        transform(EDGE, early, 0, 1.0)
        dedisperse(early, EDGE, -EDGE)

    for i in range(2):
        from_before = lax.rem(me + i, 2) == 1
        begin = pl.multiple_of(jnp.where(from_before, 0, frames - EDGE), EDGE)

        @pl.when(from_before & (me > 0))
        def _():
            forward().wait_recv()
            for p in range(2):
                ext[p, EDGE:own, 0:lines] = before[p].astype(jnp.float32)

        @pl.when(jnp.logical_not(from_before) & (me < count - 1))
        def _():
            backward().wait_recv()
            for p in range(2):
                ext[p, own + frames:own + frames + EDGE, 0:lines] = after[p].astype(jnp.float32)

        @pl.when(jnp.logical_not(from_before) & (me == count - 1))
        def _():
            for p in range(2):
                ext[p, own + frames:own + frames + EDGE, 0:lines] = jnp.zeros((EDGE, lines, LANES), jnp.float32)

        fir(begin, EDGE)
        ended = jnp.logical_not(from_before) & (me == count - 1)
        transform(EDGE, spread_out, begin, jnp.where(ended, 0.0, 1.0))

    close_round(2)
    open_round(3)
    dedisperse(spread_out, frames, 0)
    height = HALF + frames + EDGE
    total = acc[0, 0:height]
    for m in range(1, 8):
        total = total + acc[m, m:m + height]
    side = lax.broadcasted_iota(jnp.int32, (8, LANES), 1) < trials
    empty = jnp.zeros((8, LANES), jnp.float32)

    def joined(r):
        first = total[r - HALF:r - HALF + 8] if HALF <= r < HALF + height else empty
        other = total[r:r + 8] if r < height else empty
        mixed = jnp.where(side, first, other)
        return mixed + pltpu.roll(mixed, trials, 1)

    half = frames // 2
    for q in range(reach + 1):
        for r in range(0, half, 8):
            top = joined(q * frames + r)
            low = joined(q * frames + half + r)
            part[q * half + r:q * half + r + 8, :] = jnp.where(side, top, low)
    rise = (reach + 1) * frames
    part[(reach + 1) * half:(reach + 1) * half + EDGE, :] = jnp.where(side, joined(rise), 0.0)

    def near(k):
        return pltpu.make_async_remote_copy(
            src_ref=part.at[pl.ds((reach - k) * half, half)], dst_ref=landed.at[k - 1],
            send_sem=near_send.at[k - 1], recv_sem=near_recv.at[k - 1],
            device_id={"tm": me - k}, device_id_type=MESH,
        )

    def up():
        return pltpu.make_async_remote_copy(
            src_ref=part.at[pl.ds((reach + 1) * half, EDGE)], dst_ref=risen,
            send_sem=near_send.at[reach], recv_sem=near_recv.at[reach],
            device_id={"tm": me + 1}, device_id_type=MESH,
        )

    for k in range(reach, 0, -1):
        @pl.when(me >= k)
        def _():
            near(k).start()

    @pl.when(me < count - 1)
    def _():
        up().start()

    @pl.when(me == 0)
    def _():
        risen[...] = jnp.zeros_like(risen)

    @pl.when(me > 0)
    def _():
        up().wait_recv()

    for k in range(1, reach + 1):
        @pl.when(me + k >= count)
        def _():
            landed[k - 1] = jnp.zeros((half, LANES), jnp.float32)

        @pl.when(me + k < count)
        def _():
            near(k).wait_recv()

    series = part[reach * half:(reach + 1) * half, :]
    for k in range(1, reach + 1):
        series = series + landed[k - 1]
    series = series + jnp.concatenate([risen[...], jnp.zeros((half - EDGE, LANES), jnp.float32)], axis=0)
    turned = pltpu.roll(series, trials, 1)

    def fold(value, op):
        return op(value, pltpu.roll(value, trials, 1))

    piece = jnp.sum(series, axis=0, keepdims=True) * (1.0 / half)
    away = series - piece
    opposite = pltpu.roll(piece, trials, 1)
    mean = (piece + opposite) * 0.5
    gap = piece - opposite
    spread = fold(jnp.sum(away * away, axis=0, keepdims=True), jnp.add) + (0.5 * half) * (gap * gap)
    peak = fold(jnp.max(series, axis=0, keepdims=True), jnp.maximum)
    mine[...] = jnp.concatenate([mean, spread, peak, peak], axis=0)

    def flipped(k):
        place = me
        for bit in range(count.bit_length()):
            if k >> bit & 1:
                place = place + (1 << bit) * (1 - 2 * lax.rem(lax.div(me, 1 << bit), 2))
        return place

    def far(k):
        return pltpu.make_async_remote_copy(
            src_ref=mine, dst_ref=gathered.at[k - 1],
            send_sem=far_send.at[k - 1], recv_sem=far_recv.at[k - 1],
            device_id={"tm": flipped(k)}, device_id_type=MESH,
        )

    for i in range(3, len(rounds)):
        close_round(i)
        open_round(i + 1)
    for k in range(count - 1, 0, -1):
        far(k).start()
    live = jnp.maximum(jnp.sum(mask_ref[...].astype(jnp.float32)), 1.0)
    for k in range(1, count):
        far(k).wait_recv()
    means, spreads, peaks = gathered[:, 0, :], gathered[:, 1, :], gathered[:, 2, :]
    average = (mean + jnp.sum(means, axis=0, keepdims=True)) * (1.0 / count)
    offset = means - average
    squares = spread + jnp.sum(spreads, axis=0, keepdims=True)
    between = (mean - average) * (mean - average) + jnp.sum(offset * offset, axis=0, keepdims=True)
    variance = (squares + frames * between) * (1.0 / (frames * count))
    top = jnp.maximum(peak, jnp.max(peaks, axis=0, keepdims=True))
    deviation = jnp.sqrt(variance + 1e-05)
    z_ref[0:half, :] = ((series - average) / deviation)[:, :trials]
    z_ref[half:frames, :] = ((turned - average) / deviation)[:, :trials]
    stats_ref[...] = jnp.concatenate(
        [average / live, deviation / live, (top - average) / deviation], axis=0
    )[:, :trials]

    @pl.when(me < count - 1)
    def _():
        forward().wait_send()
        up().wait_send()

    @pl.when(me > 0)
    def _():
        backward().wait_send()

    swap().wait_send()
    for k in range(1, reach + 1):
        @pl.when(me >= k)
        def _():
            near(k).wait_send()
    for k in range(1, count):
        far(k).wait_send()


def finish_kernel(z_ref, stats_ref, z_out, stats_out, sem):
    first = pltpu.make_async_copy(z_ref, z_out, sem.at[0])
    second = pltpu.make_async_copy(stats_ref, stats_out, sem.at[1])
    first.start()
    second.start()
    first.wait()
    second.wait()


def per_device(voltage, delays, chan_mask):
    frames = voltage.shape[2] // NCHAN
    trials = delays.shape[0]
    count = lax.axis_size("tm")
    lines = 2 * RADIX
    half = frames // 2
    blocks = LANES // RADIX
    wide = NCHAN // blocks
    reach = MAXD // frames
    steps = HALF + 2
    past = TAPS - 1
    vmem = pl.BlockSpec(memory_space=pltpu.VMEM)
    hbm = pl.BlockSpec(memory_space=pltpu.HBM)
    framed = voltage.reshape(2, 2, frames * RADIX, LANES).transpose(0, 2, 1, 3).reshape(2, frames, lines, LANES)
    operands = (framed, jnp.asarray(prototype()), jnp.asarray(twiddles()), jnp.asarray(transform_table()), delays,
                chan_mask.reshape(RADIX, LANES))
    dma = pltpu.SemaphoreType.DMA
    outputs = (
        jax.ShapeDtypeStruct((frames, trials), jnp.float32),
        jax.ShapeDtypeStruct((3, trials), jnp.float32),
    )
    results = pl.pallas_call(
        functools.partial(beam_kernel, count, frames, trials),
        out_shape=outputs,
        in_specs=[hbm] * 6,
        out_specs=(vmem,) * 2,
        scratch_shapes=[
            pltpu.VMEM((2, frames, lines, LANES), jnp.bfloat16),
            pltpu.VMEM((TAPS, PITCH, LANES), jnp.float32),
            pltpu.VMEM((2, RADIX, LANES), jnp.float32),
            pltpu.VMEM((2, 2 * LANES, 2 * LANES), jnp.bfloat16),
            pltpu.VMEM((trials // 2, NCHAN), jnp.int32),
            pltpu.VMEM((RADIX, LANES), jnp.int32),
            pltpu.VMEM((2, past - EDGE, lines, LANES), jnp.bfloat16),
            pltpu.VMEM((2, EDGE, lines, LANES), jnp.bfloat16),
            pltpu.VMEM((2, frames + past + EDGE, PITCH, LANES), jnp.float32),
            pltpu.VMEM((frames * PITCH, LANES), jnp.float32),
            pltpu.VMEM((RADIX * frames, 2 * LANES), jnp.float32),
            pltpu.VMEM((blocks, frames, 2 * LANES), jnp.float32),
            pltpu.VMEM((blocks, EDGE, 2 * LANES), jnp.float32),
            pltpu.VMEM((trials, LANES), jnp.float32),
            pltpu.VMEM((steps + 6, LANES), jnp.int32),
            pltpu.VMEM((steps + 6, LANES), jnp.float32),
            pltpu.VMEM((8, HALF + frames + 2 * EDGE, LANES), jnp.float32),
            pltpu.VMEM(((reach + 1) * half + EDGE, LANES), jnp.float32),
            pltpu.VMEM((reach, half, LANES), jnp.float32),
            pltpu.VMEM((EDGE, LANES), jnp.float32),
            pltpu.VMEM((4, LANES), jnp.float32),
            pltpu.VMEM((count - 1, 4, LANES), jnp.float32),
            dma((6,)),
            dma((2,)),
            dma((2,)),
            dma((reach + 1,)),
            dma((reach + 1,)),
            dma((count - 1,)),
            dma((count - 1,)),
            dma((2,)),
            pltpu.SemaphoreType.REGULAR((8,)),
        ],
        compiler_params=pltpu.CompilerParams(collective_id=1, vmem_limit_bytes=GRANT, has_side_effects=True),
        name="beam",
    )(*[pltpu.with_memory_space_constraint(v, pltpu.HBM) for v in operands])
    zscore, trial_stats = pl.pallas_call(
        finish_kernel,
        out_shape=outputs,
        in_specs=[vmem] * 2,
        out_specs=(hbm,) * 2,
        scratch_shapes=[dma((2,))],
        compiler_params=pltpu.CompilerParams(vmem_limit_bytes=GRANT),
        name="finish",
    )(*results)
    return (zscore.T, trial_stats)


def solution(mesh):
    in_specs = (P(None, None, ("beam", "tm")), P(), P("beam"))
    out_specs = (P(None, ("beam", "tm")), P(None, "beam"))
    return jax.shard_map(
        per_device, mesh=mesh, in_specs=in_specs, out_specs=out_specs, check_vma=False
    )
```

```python
import functools
import math

import jax
import jax.numpy as jnp
import numpy as np
from jax import lax
from jax.experimental import pallas as pl
from jax.experimental.pallas import tpu as pltpu
from jax.sharding import PartitionSpec as P

NCHAN = 2048
TAPS = 16
LANES = 128
RADIX = NCHAN // LANES
MAXD = 96
EDGE = 8
HALF = MAXD // 2
PITCH = 40
GRANT = 32 * 1024 * 1024
MESH = pl.DeviceIdType.MESH


def prototype():
    length = TAPS * NCHAN
    position = np.arange(length, dtype=np.float64)
    window = 0.54 - 0.46 * np.cos(2.0 * np.pi * position / (length - 1))
    shaped = np.sinc((position - (length - 1) / 2.0) / NCHAN) * window
    shaped = shaped * np.sqrt(NCHAN / np.sum(shaped * shaped))
    taps = shaped.reshape(TAPS, RADIX, 1, LANES)
    taps = np.broadcast_to(taps, (TAPS, RADIX, 2, LANES))
    return taps.reshape(TAPS, 2 * RADIX, LANES).astype(np.float32)


def twiddles():
    angle = -2.0 * np.pi * np.outer(np.arange(RADIX), np.arange(LANES)) / NCHAN
    return np.stack([np.cos(angle), np.sin(angle)]).astype(np.float32)


def transform_table():
    angle = -2.0 * np.pi * (np.outer(np.arange(LANES), np.arange(LANES)) % LANES) / LANES
    scale = 1.0 / math.sqrt(NCHAN)
    cos, sin = np.cos(angle) * scale, np.sin(angle) * scale
    full = np.block([[cos, sin], [-sin, cos]]).astype(np.float32)
    high = full.astype(jnp.bfloat16)
    low = (full - high.astype(np.float32)).astype(jnp.bfloat16)
    return np.stack([high, low])


def butterflies(items):
    count = len(items)
    if count == 1:
        return items
    even = butterflies(items[0::2])
    odd = butterflies(items[1::2])
    half = count // 2
    out = [None] * count
    for k in range(half):
        re, im = odd[k]
        if k == 0:
            tr, ti = re, im
        elif 4 * k == count:
            tr, ti = im, -re
        elif 8 * k == count:
            r = math.sqrt(0.5)
            tr, ti = (re + im) * r, (im - re) * r
        elif 8 * k == 3 * count:
            r = math.sqrt(0.5)
            tr, ti = (im - re) * r, (re + im) * (-r)
        else:
            c, s = math.cos(2 * math.pi * k / count), -math.sin(2 * math.pi * k / count)
            tr, ti = re * c - im * s, re * s + im * c
        er, ei = even[k]
        out[k] = (er + tr, ei + ti)
        out[k + half] = (er - tr, ei - ti)
    return out


def wait_some(sem, amount):
    @pl.when(amount > 0)
    def _():
        pl.semaphore_wait(sem, amount)


def beam_kernel(count, frames, trials, volt_hbm, taps_hbm, twid_hbm, table_hbm, delay_hbm, mask_hbm, z_ref, stats_ref,
                volt_ref, taps_ref, twid_ref, table_ref, delay_ref, mask_ref, before, after, ext, weighted, sections,
                spread_out, early, tally, blockno, within, acc, part, landed, risen, mine, gathered,
                load_sem, halo_send, halo_recv, near_send, near_recv, far_send, far_recv, swap_sem, know):
    me = lax.axis_index("tm")
    past = TAPS - 1
    lead = past - EDGE
    lines = 2 * RADIX
    own = EDGE + lead
    blocks = LANES // RADIX
    wide = NCHAN // blocks
    reach = MAXD // frames
    steps = HALF + 2
    share = trials // 2
    core = lax.rem(me, 2)
    first = pl.multiple_of(core * share, share)
    barrier = pltpu.get_barrier_semaphore()

    def here(k):
        return (me + k >= 0) & (me + k < count)

    def tell(sem, k):
        @pl.when(here(k))
        def _():
            pl.semaphore_signal(sem, inc=1, device_id={"tm": me + k}, device_id_type=MESH)

    def number(distances):
        return sum(jnp.where(here(k), 1, 0) for k in distances)

    close = (-2, -1, 1, 2)
    for k in close:
        tell(barrier, k)
    pairs = ((volt_hbm, volt_ref), (taps_hbm, taps_ref.at[:, pl.ds(0, lines)]), (delay_hbm.at[pl.ds(first, share)], delay_ref), (twid_hbm, twid_ref),
             (table_hbm, table_ref), (mask_hbm, mask_ref))
    loads = [pltpu.make_async_copy(a, b, load_sem.at[i]) for i, (a, b) in enumerate(pairs)]
    for load in loads:
        load.start()

    def forward():
        return pltpu.make_async_remote_copy(
            src_ref=volt_ref.at[:, pl.ds(frames - lead, lead)], dst_ref=before,
            send_sem=halo_send.at[0], recv_sem=halo_recv.at[0], device_id={"tm": me + 1}, device_id_type=MESH,
        )

    def backward():
        return pltpu.make_async_remote_copy(
            src_ref=volt_ref.at[:, pl.ds(0, EDGE)], dst_ref=after,
            send_sem=halo_send.at[1], recv_sem=halo_recv.at[1], device_id={"tm": me - 1}, device_id_type=MESH,
        )

    loads[0].wait()
    for p in range(2):
        ext[p, own:own + frames, 0:lines] = volt_ref[p].astype(jnp.float32)
    wait_some(barrier, number(close))

    @pl.when((core == 1) & (me < count - 1))
    def _():
        forward().start()

    @pl.when(me > 0)
    def _():
        backward().start()

    @pl.when((core == 0) & (me < count - 1))
    def _():
        forward().start()

    rounds = []
    known = 2
    while known < count - 1:
        rounds.append(known)
        known *= 2

    def open_round(i):
        if i < len(rounds):
            for k in (-rounds[i], rounds[i]):
                tell(know.at[i], k)

    def close_round(i):
        if i < len(rounds):
            wait_some(know.at[i], number((-rounds[i], rounds[i])))

    open_round(0)
    for load in loads[1:]:
        load.wait()

    row = lax.broadcasted_iota(jnp.int32, (blocks, LANES), 1)
    even = mask_ref[pl.ds(0, blocks, stride=2), :]
    odd = mask_ref[pl.ds(1, blocks, stride=2), :]
    usable = []
    for h in range(2):
        place = (row & 7) * RADIX + 8 * h + (row >> 4)
        low = jnp.take_along_axis(even, place, axis=1, mode="promise_in_bounds")
        high = jnp.take_along_axis(odd, place, axis=1, mode="promise_in_bounds")
        usable.append(jnp.where((row & 8) == 0, low, high).astype(jnp.float32))

    def fir(begin, size, base, whole):
        for part_index in range(lines // 8):
            rows = pl.ds(8 * part_index, 8)
            taps = [taps_ref[j, rows, :] for j in range(TAPS)]

            def some(g, carry):
                for p in range(2):
                    sums = [None] * 4
                    for i in range(TAPS + 3):
                        sample = ext[p, begin + EDGE + 4 * g + i, rows, :]
                        for f in range(4):
                            if 0 <= i - f < TAPS:
                                term = taps[i - f] * sample
                                sums[f] = term if sums[f] is None else sums[f] + term
                    for f in range(4):
                        start = pl.multiple_of((p * whole + base + 4 * g + f) * PITCH, 8) + 8 * part_index
                        weighted[pl.ds(start, 8), :] = sums[f]
                return carry

            lax.fori_loop(0, size // 4, some, 0)

    def transform(size, out, begin, scale):
        group = 8
        rows_half = 2 * size
        for g in range(rows_half // group):
            p, f = divmod(g * group, size)
            first = (p * size + f) * PITCH
            items = []
            for m in range(RADIX):
                re = weighted[pl.ds(first + 2 * m, group, stride=PITCH), :]
                im = weighted[pl.ds(first + 2 * m + 1, group, stride=PITCH), :]
                items.append((re, im))
            for k1, (re, im) in enumerate(butterflies(items)):
                if k1:
                    c, s = twid_ref[0, k1:k1 + 1, :], twid_ref[1, k1:k1 + 1, :]
                    re, im = re * c - im * s, re * s + im * c
                place = k1 * rows_half + g * group
                sections[place:place + group, :LANES] = re
                sections[place:place + group, LANES:] = im
        both = sections[0:RADIX * rows_half, :]
        high = both.astype(jnp.bfloat16)
        low = (both - high.astype(jnp.float32)).astype(jnp.bfloat16)
        dot = functools.partial(jnp.dot, preferred_element_type=jnp.float32)
        spec = dot(high, table_ref[0]) + (dot(high, table_ref[1]) + dot(low, table_ref[0]))
        spec = spec * spec
        both_pols = (spec[:, :LANES] + spec[:, LANES:]).reshape(RADIX, 2, size, LANES)
        energy = both_pols[:, 0] + both_pols[:, 1]
        chunk = lax.broadcasted_iota(jnp.int32, (size, LANES), 1) >> 4
        for h in range(2):
            parts = [energy[8 * h + i] for i in range(8)]
            for bit in (4, 2, 1):
                kept = (chunk & bit) == 0
                for i in range(8):
                    if i & bit == 0:
                        low_part, high_part = parts[i], parts[i | bit]
                        parts[i] = jnp.where(kept, low_part, pltpu.roll(high_part, bit * RADIX, 1))
                        parts[i | bit] = jnp.where(kept, pltpu.roll(low_part, LANES - bit * RADIX, 1), high_part)
            for b in range(blocks):
                out[b, pl.ds(begin, size), h * LANES:(h + 1) * LANES] = parts[b] * (usable[h][b:b + 1] * scale)

    def swap():
        rows = pl.ds(first, share)
        return pltpu.make_async_remote_copy(
            src_ref=tally.at[rows], dst_ref=tally.at[rows],
            send_sem=swap_sem.at[0], recv_sem=swap_sem.at[1],
            device_id={"tm": me + 1 - 2 * core}, device_id_type=MESH,
        )

    def admit(from_before):
        @pl.when(from_before & (me > 0))
        def _():
            forward().wait_recv()
            for p in range(2):
                ext[p, EDGE:own, 0:lines] = before[p].astype(jnp.float32)

        @pl.when(jnp.logical_not(from_before) & (me < count - 1))
        def _():
            backward().wait_recv()
            for p in range(2):
                ext[p, own + frames:own + frames + EDGE, 0:lines] = after[p].astype(jnp.float32)

    @pl.when(me == 0)
    def _():
        for p in range(2):
            ext[p, 0:own, 0:lines] = jnp.zeros((own, lines, LANES), jnp.float32)

    @pl.when(me == count - 1)
    def _():
        for p in range(2):
            ext[p, own + frames:own + frames + EDGE, 0:lines] = jnp.zeros((EDGE, lines, LANES), jnp.float32)

    inner = frames - 2 * EDGE
    fir(EDGE, inner, core * EDGE, frames - EDGE)
    admit(core == 1)
    fir((1 - core) * (frames - EDGE), EDGE, (1 - core) * inner, frames - EDGE)
    begin = pl.multiple_of(EDGE - core * EDGE, EDGE)
    level = lax.broadcasted_iota(jnp.int32, (8, LANES), 1)

    def look(table, place):
        return jnp.take_along_axis(table, place, axis=1, mode="promise_in_bounds")

    tables = NCHAN // LANES
    groups = range(share // 8)
    each = (level & (LANES // tables - 1)) * tables + (tables - 1)

    def table(g, b):
        return delay_ref[8 * g:8 * g + 8, b * LANES:(b + 1) * LANES]

    seldom = []
    for g in groups:
        kept = jnp.zeros((8, LANES), jnp.int32)
        for b in range(tables):
            kept = jnp.where((level >> 3) == b, look(table(g, b), each), kept)
        seldom.append(kept)
    coarse = [jnp.zeros((8, LANES), jnp.int32) for g in groups]
    for step in (64, 32, 16, 8, 4, 2, 1):
        for g in groups:
            seen = look(seldom[g], coarse[g] + (step - 1))
            coarse[g] = jnp.where(seen >= level, coarse[g] + step, coarse[g])
    fine = [jnp.zeros((8, LANES), jnp.int32) for g in groups]
    for step in (8, 4, 2, 1):
        for g in groups:
            place = (coarse[g] & 7) * tables + fine[g] + (step - 1)
            which = coarse[g] >> 3
            seen = jnp.full((8, LANES), -1, jnp.int32)
            for b in range(tables):
                seen = jnp.where(which == b, look(table(g, b), place), seen)
            fine[g] = jnp.where(seen >= level, fine[g] + step, fine[g])
    tally[pl.ds(first, share), :] = jnp.concatenate(
        [jnp.where(level == 0, NCHAN, coarse[g] * tables + fine[g]).astype(jnp.float32) for g in groups], axis=0)

    transform(frames - EDGE, spread_out, begin, 1.0)
    swap().start()
    close_round(0)
    open_round(1)
    acc[...] = jnp.zeros_like(acc)

    admit(core == 0)
    begin = pl.multiple_of(core * (frames - EDGE), EDGE)
    fir(begin, EDGE, 0, EDGE)
    transform(EDGE, spread_out, begin, jnp.where(me == count - 1, 0.0, 1.0))
    swap().wait_recv()
    total = tally[...]
    turned = jnp.concatenate([total, jnp.zeros((LANES - trials, LANES), jnp.float32)], axis=0).T
    rows_kept = blockno.shape[0]
    near_side = lax.broadcasted_iota(jnp.int32, (rows_kept, LANES), 1) < trials
    total = jnp.where(
        near_side, turned[0:rows_kept], pltpu.roll(turned[HALF:HALF + rows_kept], trials, 1)
    ).astype(jnp.int32)
    blockno[...] = total >> 8
    within[...] = (total & (wide - 1)).astype(jnp.float32)
    order = lax.broadcasted_iota(jnp.int32, (wide, LANES), 0)
    order = ((order & (RADIX - 1)) * RADIX + (order >> 4)).astype(jnp.float32)

    order = order.astype(jnp.bfloat16)

    def pick(j):
        end = jnp.broadcast_to(within[j:j + 1, :], (wide, LANES)).astype(jnp.bfloat16)
        return jnp.minimum(jnp.maximum(end - order, jnp.zeros_like(end)), jnp.ones_like(end))

    def dedisperse(source, size, offset):
        values = jnp.concatenate([source[b] for b in range(blocks)], axis=0).astype(jnp.bfloat16)
        dot = functools.partial(jnp.dot, preferred_element_type=jnp.float32)
        sums = dot(values, jnp.ones((wide, LANES), jnp.bfloat16))
        column = lax.broadcasted_iota(jnp.int32, (size, LANES), 1)
        prefix = jnp.zeros((size, LANES), jnp.float32)
        for b in range(blocks):
            prefix = prefix + jnp.where(column > b, sums[b * size:(b + 1) * size], 0.0)
        last = None
        for i in range(steps // 2):
            found = dot(values, jnp.concatenate([pick(2 * i), pick(2 * i + 1)], axis=1))
            for side in range(2):
                j = 2 * i + side
                which = jnp.broadcast_to(blockno[j:j + 1, :], (size, LANES))
                inner = jnp.zeros((size, LANES), jnp.float32)
                for b in range(blocks):
                    inner = jnp.where(which == b, found[b * size:(b + 1) * size, side * LANES:(side + 1) * LANES], inner)
                now = inner + jnp.take_along_axis(prefix, which, axis=1, mode="promise_in_bounds")
                if j:
                    change = last - now
                    if j - 1 == HALF:
                        change = jnp.where(column < trials, 0.0, change)
                    a, m = divmod(j - 1, 8)
                    place = HALF + EDGE + offset - 8 * a
                    acc[m, place:place + size] += change
                last = now

    @pl.when(me == 0)
    def _():
        fir(-EDGE, EDGE, 0, EDGE)
        transform(EDGE, early, 0, 1.0)
        dedisperse(early, EDGE, -EDGE)

    dedisperse(spread_out, frames, 0)
    height = HALF + frames + EDGE
    total = acc[0, 0:height]
    for m in range(1, 8):
        total = total + acc[m, m:m + height]
    side = lax.broadcasted_iota(jnp.int32, (8, LANES), 1) < trials
    empty = jnp.zeros((8, LANES), jnp.float32)

    def joined(r):
        first = total[r - HALF:r - HALF + 8] if HALF <= r < HALF + height else empty
        other = total[r:r + 8] if r < height else empty
        mixed = jnp.where(side, first, other)
        return mixed + pltpu.roll(mixed, trials, 1)

    half = frames // 2
    for q in range(reach + 1):
        for r in range(0, half, 8):
            top = joined(q * frames + r)
            low = joined(q * frames + half + r)
            part[q * half + r:q * half + r + 8, :] = jnp.where(side, top, low)
    rise = (reach + 1) * frames
    part[(reach + 1) * half:(reach + 1) * half + EDGE, :] = jnp.where(side, joined(rise), 0.0)

    def near(k):
        return pltpu.make_async_remote_copy(
            src_ref=part.at[pl.ds((reach - k) * half, half)], dst_ref=landed.at[k - 1],
            send_sem=near_send.at[k - 1], recv_sem=near_recv.at[k - 1],
            device_id={"tm": me - k}, device_id_type=MESH,
        )

    def up():
        return pltpu.make_async_remote_copy(
            src_ref=part.at[pl.ds((reach + 1) * half, EDGE)], dst_ref=risen,
            send_sem=near_send.at[reach], recv_sem=near_recv.at[reach],
            device_id={"tm": me + 1}, device_id_type=MESH,
        )

    for k in range(reach, 0, -1):
        @pl.when(me >= k)
        def _():
            near(k).start()

    @pl.when(me < count - 1)
    def _():
        up().start()

    close_round(1)
    open_round(2)

    @pl.when(me == 0)
    def _():
        risen[...] = jnp.zeros_like(risen)

    @pl.when(me > 0)
    def _():
        up().wait_recv()

    for k in range(1, reach + 1):
        @pl.when(me + k >= count)
        def _():
            landed[k - 1] = jnp.zeros((half, LANES), jnp.float32)

        @pl.when(me + k < count)
        def _():
            near(k).wait_recv()

    series = part[reach * half:(reach + 1) * half, :]
    for k in range(1, reach + 1):
        series = series + landed[k - 1]
    series = series + jnp.concatenate([risen[...], jnp.zeros((half - EDGE, LANES), jnp.float32)], axis=0)
    turned = pltpu.roll(series, trials, 1)

    def fold(value, op):
        return op(value, pltpu.roll(value, trials, 1))

    piece = jnp.sum(series, axis=0, keepdims=True) * (1.0 / half)
    away = series - piece
    opposite = pltpu.roll(piece, trials, 1)
    mean = (piece + opposite) * 0.5
    gap = piece - opposite
    spread = fold(jnp.sum(away * away, axis=0, keepdims=True), jnp.add) + (0.5 * half) * (gap * gap)
    peak = fold(jnp.max(series, axis=0, keepdims=True), jnp.maximum)
    mine[...] = jnp.concatenate([mean, spread, peak, peak], axis=0)

    def flipped(k):
        place = me
        for bit in range(count.bit_length()):
            if k >> bit & 1:
                place = place + (1 << bit) * (1 - 2 * lax.rem(lax.div(me, 1 << bit), 2))
        return place

    def far(k):
        return pltpu.make_async_remote_copy(
            src_ref=mine, dst_ref=gathered.at[k - 1],
            send_sem=far_send.at[k - 1], recv_sem=far_recv.at[k - 1],
            device_id={"tm": flipped(k)}, device_id_type=MESH,
        )

    for i in range(2, len(rounds)):
        close_round(i)
        open_round(i + 1)
    for k in range(count - 1, 0, -1):
        far(k).start()
    live = jnp.maximum(jnp.sum(mask_ref[...].astype(jnp.float32)), 1.0)
    for k in range(1, count):
        far(k).wait_recv()
    means, spreads, peaks = gathered[:, 0, :], gathered[:, 1, :], gathered[:, 2, :]
    average = (mean + jnp.sum(means, axis=0, keepdims=True)) * (1.0 / count)
    offset = means - average
    squares = spread + jnp.sum(spreads, axis=0, keepdims=True)
    between = (mean - average) * (mean - average) + jnp.sum(offset * offset, axis=0, keepdims=True)
    variance = (squares + frames * between) * (1.0 / (frames * count))
    top = jnp.maximum(peak, jnp.max(peaks, axis=0, keepdims=True))
    deviation = jnp.sqrt(variance + 1e-05)
    z_ref[0:half, :] = ((series - average) / deviation)[:, :trials]
    z_ref[half:frames, :] = ((turned - average) / deviation)[:, :trials]
    stats_ref[...] = jnp.concatenate(
        [average / live, deviation / live, (top - average) / deviation], axis=0
    )[:, :trials]

    @pl.when(me < count - 1)
    def _():
        forward().wait_send()
        up().wait_send()

    @pl.when(me > 0)
    def _():
        backward().wait_send()

    swap().wait_send()
    for k in range(1, reach + 1):
        @pl.when(me >= k)
        def _():
            near(k).wait_send()
    for k in range(1, count):
        far(k).wait_send()


def finish_kernel(z_ref, stats_ref, z_out, stats_out, sem):
    first = pltpu.make_async_copy(z_ref, z_out, sem.at[0])
    second = pltpu.make_async_copy(stats_ref, stats_out, sem.at[1])
    first.start()
    second.start()
    first.wait()
    second.wait()


def per_device(voltage, delays, chan_mask):
    frames = voltage.shape[2] // NCHAN
    trials = delays.shape[0]
    count = lax.axis_size("tm")
    lines = 2 * RADIX
    half = frames // 2
    blocks = LANES // RADIX
    wide = NCHAN // blocks
    reach = MAXD // frames
    steps = HALF + 2
    past = TAPS - 1
    vmem = pl.BlockSpec(memory_space=pltpu.VMEM)
    hbm = pl.BlockSpec(memory_space=pltpu.HBM)
    framed = voltage.reshape(2, 2, frames * RADIX, LANES).transpose(0, 2, 1, 3).reshape(2, frames, lines, LANES)
    operands = (framed, jnp.asarray(prototype()), jnp.asarray(twiddles()), jnp.asarray(transform_table()), delays,
                chan_mask.reshape(RADIX, LANES))
    dma = pltpu.SemaphoreType.DMA
    outputs = (
        jax.ShapeDtypeStruct((frames, trials), jnp.float32),
        jax.ShapeDtypeStruct((3, trials), jnp.float32),
    )
    results = pl.pallas_call(
        functools.partial(beam_kernel, count, frames, trials),
        out_shape=outputs,
        in_specs=[hbm] * 6,
        out_specs=(vmem,) * 2,
        scratch_shapes=[
            pltpu.VMEM((2, frames, lines, LANES), jnp.bfloat16),
            pltpu.VMEM((TAPS, PITCH, LANES), jnp.float32),
            pltpu.VMEM((2, RADIX, LANES), jnp.float32),
            pltpu.VMEM((2, 2 * LANES, 2 * LANES), jnp.bfloat16),
            pltpu.VMEM((trials // 2, NCHAN), jnp.int32),
            pltpu.VMEM((RADIX, LANES), jnp.int32),
            pltpu.VMEM((2, past - EDGE, lines, LANES), jnp.bfloat16),
            pltpu.VMEM((2, EDGE, lines, LANES), jnp.bfloat16),
            pltpu.VMEM((2, frames + past + EDGE, PITCH, LANES), jnp.float32),
            pltpu.VMEM((2 * frames * PITCH, LANES), jnp.float32),
            pltpu.VMEM((2 * RADIX * frames, 2 * LANES), jnp.float32),
            pltpu.VMEM((blocks, frames, 2 * LANES), jnp.float32),
            pltpu.VMEM((blocks, EDGE, 2 * LANES), jnp.float32),
            pltpu.VMEM((trials, LANES), jnp.float32),
            pltpu.VMEM((steps + 6, LANES), jnp.int32),
            pltpu.VMEM((steps + 6, LANES), jnp.float32),
            pltpu.VMEM((8, HALF + frames + 2 * EDGE, LANES), jnp.float32),
            pltpu.VMEM(((reach + 1) * half + EDGE, LANES), jnp.float32),
            pltpu.VMEM((reach, half, LANES), jnp.float32),
            pltpu.VMEM((EDGE, LANES), jnp.float32),
            pltpu.VMEM((4, LANES), jnp.float32),
            pltpu.VMEM((count - 1, 4, LANES), jnp.float32),
            dma((6,)),
            dma((2,)),
            dma((2,)),
            dma((reach + 1,)),
            dma((reach + 1,)),
            dma((count - 1,)),
            dma((count - 1,)),
            dma((2,)),
            pltpu.SemaphoreType.REGULAR((8,)),
        ],
        compiler_params=pltpu.CompilerParams(collective_id=1, vmem_limit_bytes=GRANT, has_side_effects=True),
        name="beam",
    )(*[pltpu.with_memory_space_constraint(v, pltpu.HBM) for v in operands])
    zscore, trial_stats = pl.pallas_call(
        finish_kernel,
        out_shape=outputs,
        in_specs=[vmem] * 2,
        out_specs=(hbm,) * 2,
        scratch_shapes=[dma((2,))],
        compiler_params=pltpu.CompilerParams(vmem_limit_bytes=GRANT),
        name="finish",
    )(*results)
    return (zscore.T, trial_stats)


def solution(mesh):
    in_specs = (P(None, None, ("beam", "tm")), P(), P("beam"))
    out_specs = (P(None, ("beam", "tm")), P(None, "beam"))
    return jax.shard_map(
        per_device, mesh=mesh, in_specs=in_specs, out_specs=out_specs, check_vma=False
    )
```

```python
import functools
import math

import jax
import jax.numpy as jnp
import numpy as np
from jax import lax
from jax.experimental import pallas as pl
from jax.experimental.pallas import tpu as pltpu
from jax.sharding import PartitionSpec as P

NCHAN = 2048
TAPS = 16
LANES = 128
RADIX = NCHAN // LANES
MAXD = 96
EDGE = 8
HALF = MAXD // 2
PITCH = 40
GRANT = 32 * 1024 * 1024
MESH = pl.DeviceIdType.MESH


def prototype():
    length = TAPS * NCHAN
    position = np.arange(length, dtype=np.float64)
    window = 0.54 - 0.46 * np.cos(2.0 * np.pi * position / (length - 1))
    shaped = np.sinc((position - (length - 1) / 2.0) / NCHAN) * window
    shaped = shaped * np.sqrt(NCHAN / np.sum(shaped * shaped))
    taps = shaped.reshape(TAPS, RADIX, 1, LANES)
    taps = np.broadcast_to(taps, (TAPS, RADIX, 2, LANES))
    return taps.reshape(TAPS, 2 * RADIX, LANES).astype(np.float32)


def twiddles():
    angle = -2.0 * np.pi * np.outer(np.arange(RADIX), np.arange(LANES)) / NCHAN
    return np.stack([np.cos(angle), np.sin(angle)]).astype(np.float32)


def transform_table():
    angle = -2.0 * np.pi * (np.outer(np.arange(LANES), np.arange(LANES)) % LANES) / LANES
    scale = 1.0 / math.sqrt(NCHAN)
    cos, sin = np.cos(angle) * scale, np.sin(angle) * scale
    full = np.block([[cos, sin], [-sin, cos]]).astype(np.float32)
    high = full.astype(jnp.bfloat16)
    low = (full - high.astype(np.float32)).astype(jnp.bfloat16)
    return np.stack([high, low])


def butterflies(items):
    count = len(items)
    if count == 1:
        return items
    even = butterflies(items[0::2])
    odd = butterflies(items[1::2])
    half = count // 2
    out = [None] * count
    for k in range(half):
        re, im = odd[k]
        if k == 0:
            tr, ti = re, im
        elif 4 * k == count:
            tr, ti = im, -re
        elif 8 * k == count:
            r = math.sqrt(0.5)
            tr, ti = (re + im) * r, (im - re) * r
        elif 8 * k == 3 * count:
            r = math.sqrt(0.5)
            tr, ti = (im - re) * r, (re + im) * (-r)
        else:
            c, s = math.cos(2 * math.pi * k / count), -math.sin(2 * math.pi * k / count)
            tr, ti = re * c - im * s, re * s + im * c
        er, ei = even[k]
        out[k] = (er + tr, ei + ti)
        out[k + half] = (er - tr, ei - ti)
    return out


def wait_some(sem, amount):
    @pl.when(amount > 0)
    def _():
        pl.semaphore_wait(sem, amount)


def beam_kernel(count, frames, trials, volt_hbm, taps_hbm, twid_hbm, table_hbm, delay_hbm, mask_hbm, z_ref, stats_ref,
                volt_ref, taps_ref, twid_ref, table_ref, delay_ref, mask_ref, before, after, ext, weighted, held, sections,
                spread_out, early, tally, blockno, within, acc, part, landed, risen, mine, gathered,
                load_sem, halo_send, halo_recv, near_send, near_recv, far_send, far_recv, swap_sem, know):
    me = lax.axis_index("tm")
    past = TAPS - 1
    lead = past - EDGE
    lines = 2 * RADIX
    own = EDGE + lead
    blocks = LANES // RADIX
    wide = NCHAN // blocks
    reach = MAXD // frames
    steps = HALF + 2
    steps_of = [
        (1 << bit) * (1 - 2 * lax.rem(lax.div(me, 1 << bit), 2)) for bit in range((count - 1).bit_length())
    ]
    share = trials // 2
    core = lax.rem(me, 2)
    first = pl.multiple_of(core * share, share)
    barrier = pltpu.get_barrier_semaphore()

    def here(k):
        return (me + k >= 0) & (me + k < count)

    def tell(sem, k):
        @pl.when(here(k))
        def _():
            pl.semaphore_signal(sem, inc=1, device_id={"tm": me + k}, device_id_type=MESH)

    def number(distances):
        return sum(jnp.where(here(k), 1, 0) for k in distances)

    close = (-1, 1)
    for k in close:
        tell(barrier, k)
    pairs = ((volt_hbm, volt_ref), (taps_hbm, taps_ref.at[:, pl.ds(0, lines)]), (delay_hbm.at[pl.ds(first, share)], delay_ref), (twid_hbm, twid_ref),
             (table_hbm, table_ref), (mask_hbm, mask_ref))
    loads = [pltpu.make_async_copy(a, b, load_sem.at[i]) for i, (a, b) in enumerate(pairs)]
    for load in loads:
        load.start()

    def forward():
        return pltpu.make_async_remote_copy(
            src_ref=volt_ref.at[:, pl.ds(frames - lead, lead)], dst_ref=before,
            send_sem=halo_send.at[0], recv_sem=halo_recv.at[0], device_id={"tm": me + 1}, device_id_type=MESH,
        )

    def backward():
        return pltpu.make_async_remote_copy(
            src_ref=volt_ref.at[:, pl.ds(0, EDGE)], dst_ref=after,
            send_sem=halo_send.at[1], recv_sem=halo_recv.at[1], device_id={"tm": me - 1}, device_id_type=MESH,
        )

    @pl.when(core == 0)
    def _():
        for p in range(2):
            ext[p, 0:own, 0:lines] = jnp.zeros((own, lines, LANES), jnp.float32)

    @pl.when(core == 1)
    def _():
        for p in range(2):
            ext[p, own + frames:own + frames + EDGE, 0:lines] = jnp.zeros((EDGE, lines, LANES), jnp.float32)

    loads[0].wait()
    wait_some(barrier, number(close))

    @pl.when((core == 1) & (me < count - 1))
    def _():
        forward().start()

    @pl.when(me > 0)
    def _():
        backward().start()

    @pl.when((core == 0) & (me < count - 1))
    def _():
        forward().start()

    for p in range(2):
        ext[p, own:own + frames, 0:lines] = volt_ref[p].astype(jnp.float32)
    rounds = []
    known = 1
    while known < count - 1:
        rounds.append(known)
        known *= 2

    def open_round(i):
        if i < len(rounds):
            for k in (-rounds[i], rounds[i]):
                tell(know.at[i], k)

    def close_round(i):
        if i < len(rounds):
            wait_some(know.at[i], number((-rounds[i], rounds[i])))

    open_round(0)
    for load in loads[1:]:
        load.wait()

    row = lax.broadcasted_iota(jnp.int32, (blocks, LANES), 1)
    even = mask_ref[pl.ds(0, blocks, stride=2), :]
    odd = mask_ref[pl.ds(1, blocks, stride=2), :]
    usable = []
    for h in range(2):
        place = (row & 7) * RADIX + 8 * h + (row >> 4)
        low = jnp.take_along_axis(even, place, axis=1, mode="promise_in_bounds")
        high = jnp.take_along_axis(odd, place, axis=1, mode="promise_in_bounds")
        usable.append(jnp.where((row & 8) == 0, low, high).astype(jnp.float32))

    def fir(begin, size, out):
        for part_index in range(lines // 8):
            rows = pl.ds(8 * part_index, 8)
            taps = [taps_ref[j, rows, :] for j in range(TAPS)]

            def some(g, carry):
                for p in range(2):
                    sums = [None] * 4
                    for i in range(TAPS + 3):
                        sample = ext[p, begin + EDGE + 4 * g + i, rows, :]
                        for f in range(4):
                            if 0 <= i - f < TAPS:
                                term = taps[i - f] * sample
                                sums[f] = term if sums[f] is None else sums[f] + term
                    for f in range(4):
                        start = pl.multiple_of((p * size + 4 * g + f) * PITCH, 8) + 8 * part_index
                        out[pl.ds(start, 8), :] = sums[f]
                return carry

            lax.fori_loop(0, size // 4, some, 0)

    def rest(w0, low, high):
        for part_index in range(lines // 8):
            rows = pl.ds(8 * part_index, 8)
            for p in range(2):
                sums = {}
                for row in range(low, high):
                    sample = ext[p, row, rows, :]
                    for f in range(EDGE):
                        j = row - EDGE - w0 - f
                        if 0 <= j < TAPS:
                            term = taps_ref[j, rows, :] * sample
                            sums[f] = term if f not in sums else sums[f] + term
                for f, value in sums.items():
                    start = (p * EDGE + f) * PITCH + 8 * part_index
                    held[start:start + 8, :] = held[start:start + 8, :] + value

    def transform(size, out, begin, scale, weighted):
        group = 8
        rows_half = 2 * size
        for g in range(rows_half // group):
            p, f = divmod(g * group, size)
            first = (p * size + f) * PITCH
            items = []
            for m in range(RADIX):
                re = weighted[pl.ds(first + 2 * m, group, stride=PITCH), :]
                im = weighted[pl.ds(first + 2 * m + 1, group, stride=PITCH), :]
                items.append((re, im))
            for k1, (re, im) in enumerate(butterflies(items)):
                if k1:
                    c, s = twid_ref[0, k1:k1 + 1, :], twid_ref[1, k1:k1 + 1, :]
                    re, im = re * c - im * s, re * s + im * c
                place = k1 * rows_half + g * group
                sections[place:place + group, :LANES] = re
                sections[place:place + group, LANES:] = im
        both = sections[0:RADIX * rows_half, :]
        high = both.astype(jnp.bfloat16)
        low = (both - high.astype(jnp.float32)).astype(jnp.bfloat16)
        dot = functools.partial(jnp.dot, preferred_element_type=jnp.float32)
        spec = dot(high, table_ref[0]) + (dot(high, table_ref[1]) + dot(low, table_ref[0]))
        spec = spec * spec
        both_pols = (spec[:, :LANES] + spec[:, LANES:]).reshape(RADIX, 2, size, LANES)
        energy = both_pols[:, 0] + both_pols[:, 1]
        chunk = lax.broadcasted_iota(jnp.int32, (size, LANES), 1) >> 4
        for h in range(2):
            parts = [energy[8 * h + i] for i in range(8)]
            for bit in (4, 2, 1):
                kept = (chunk & bit) == 0
                for i in range(8):
                    if i & bit == 0:
                        low_part, high_part = parts[i], parts[i | bit]
                        parts[i] = jnp.where(kept, low_part, pltpu.roll(high_part, bit * RADIX, 1))
                        parts[i | bit] = jnp.where(kept, pltpu.roll(low_part, LANES - bit * RADIX, 1), high_part)
            for b in range(blocks):
                out[b, pl.ds(begin, size), h * LANES:(h + 1) * LANES] = parts[b] * (usable[h][b:b + 1] * scale)

    def swap():
        rows = pl.ds(first, share)
        return pltpu.make_async_remote_copy(
            src_ref=tally.at[rows], dst_ref=tally.at[rows],
            send_sem=swap_sem.at[0], recv_sem=swap_sem.at[1],
            device_id={"tm": me + 1 - 2 * core}, device_id_type=MESH,
        )

    def admit(from_before):
        @pl.when(from_before & (me > 0))
        def _():
            forward().wait_recv()
            for p in range(2):
                ext[p, EDGE:own, 0:lines] = before[p].astype(jnp.float32)

        @pl.when(jnp.logical_not(from_before) & (me < count - 1))
        def _():
            backward().wait_recv()
            for p in range(2):
                ext[p, own + frames:own + frames + EDGE, 0:lines] = after[p].astype(jnp.float32)

    inner = frames - 2 * EDGE
    fir(EDGE, inner, weighted)
    level = lax.broadcasted_iota(jnp.int32, (8, LANES), 1)

    def look(table, place):
        return jnp.take_along_axis(table, place, axis=1, mode="promise_in_bounds")

    tables = NCHAN // LANES
    groups = range(share // 8)
    each = (level & (LANES // tables - 1)) * tables + (tables - 1)

    def table(g, b):
        return delay_ref[8 * g:8 * g + 8, b * LANES:(b + 1) * LANES]

    seldom = []
    for g in groups:
        kept = jnp.zeros((8, LANES), jnp.int32)
        for b in range(tables):
            kept = jnp.where((level >> 3) == b, look(table(g, b), each), kept)
        seldom.append(kept)
    coarse = [jnp.zeros((8, LANES), jnp.int32) for g in groups]
    for step in (64, 32, 16, 8, 4, 2, 1):
        for g in groups:
            seen = look(seldom[g], coarse[g] + (step - 1))
            coarse[g] = jnp.where(seen >= level, coarse[g] + step, coarse[g])
    fine = [jnp.zeros((8, LANES), jnp.int32) for g in groups]
    for step in (8, 4, 2, 1):
        for g in groups:
            place = (coarse[g] & 7) * tables + fine[g] + (step - 1)
            which = coarse[g] >> 3
            seen = jnp.full((8, LANES), -1, jnp.int32)
            for b in range(tables):
                seen = jnp.where(which == b, look(table(g, b), place), seen)
            fine[g] = jnp.where(seen >= level, fine[g] + step, fine[g])
    tally[pl.ds(first, share), :] = jnp.concatenate(
        [jnp.where(level == 0, NCHAN, coarse[g] * tables + fine[g]).astype(jnp.float32) for g in groups], axis=0)

    transform(inner, spread_out, EDGE, 1.0, weighted)
    swap().start()
    close_round(0)
    open_round(1)
    late_begin = pl.multiple_of(core * (frames - EDGE), EDGE)
    fir(late_begin, EDGE, held)
    admit(core == 1)
    begin = pl.multiple_of((1 - core) * (frames - EDGE), EDGE)
    fir(begin, EDGE, weighted)
    transform(EDGE, spread_out, begin, 1.0, weighted)
    acc[...] = jnp.zeros_like(acc)

    swap().wait_recv()
    total = tally[...]
    turned = jnp.concatenate([total, jnp.zeros((LANES - trials, LANES), jnp.float32)], axis=0).T
    rows_kept = blockno.shape[0]
    near_side = lax.broadcasted_iota(jnp.int32, (rows_kept, LANES), 1) < trials
    total = jnp.where(
        near_side, turned[0:rows_kept], pltpu.roll(turned[HALF:HALF + rows_kept], trials, 1)
    ).astype(jnp.int32)
    blockno[...] = total >> 8
    within[...] = (total & (wide - 1)).astype(jnp.float32)
    order = lax.broadcasted_iota(jnp.int32, (wide, LANES), 0)
    order = ((order & (RADIX - 1)) * RADIX + (order >> 4)).astype(jnp.float32)

    order = order.astype(jnp.bfloat16)

    def pick(j):
        end = jnp.broadcast_to(within[j:j + 1, :], (wide, LANES)).astype(jnp.bfloat16)
        return jnp.minimum(jnp.maximum(end - order, jnp.zeros_like(end)), jnp.ones_like(end))

    def dedisperse(source, size, offset):
        values = jnp.concatenate([source[b] for b in range(blocks)], axis=0).astype(jnp.bfloat16)
        dot = functools.partial(jnp.dot, preferred_element_type=jnp.float32)
        sums = dot(values, jnp.ones((wide, LANES), jnp.bfloat16))
        column = lax.broadcasted_iota(jnp.int32, (size, LANES), 1)
        prefix = jnp.zeros((size, LANES), jnp.float32)
        for b in range(blocks):
            prefix = prefix + jnp.where(column > b, sums[b * size:(b + 1) * size], 0.0)
        last = None
        for i in range(steps // 2):
            found = dot(values, jnp.concatenate([pick(2 * i), pick(2 * i + 1)], axis=1))
            for side in range(2):
                j = 2 * i + side
                which = jnp.broadcast_to(blockno[j:j + 1, :], (size, LANES))
                inner = jnp.zeros((size, LANES), jnp.float32)
                for b in range(blocks):
                    inner = jnp.where(which == b, found[b * size:(b + 1) * size, side * LANES:(side + 1) * LANES], inner)
                now = inner + jnp.take_along_axis(prefix, which, axis=1, mode="promise_in_bounds")
                if j:
                    change = last - now
                    if j - 1 == HALF:
                        change = jnp.where(column < trials, 0.0, change)
                    a, m = divmod(j - 1, 8)
                    place = HALF + EDGE + offset - 8 * a
                    acc[m, place:place + size] += change
                last = now

    @pl.when(me == 0)
    def _():
        fir(-EDGE, EDGE, weighted)
        transform(EDGE, early, 0, 1.0, weighted)
        dedisperse(early, EDGE, -EDGE)

    admit(core == 0)

    @pl.when(core == 0)
    def _():
        rest(0, EDGE, own)

    @pl.when(core == 1)
    def _():
        rest(frames - EDGE, own + frames, own + frames + EDGE)

    transform(EDGE, spread_out, late_begin, jnp.where(me == count - 1, 0.0, 1.0), held)
    close_round(1)
    open_round(2)
    dedisperse(spread_out, frames, 0)
    height = HALF + frames + EDGE
    total = acc[0, 0:height]
    for m in range(1, 8):
        total = total + acc[m, m:m + height]
    side = lax.broadcasted_iota(jnp.int32, (8, LANES), 1) < trials
    empty = jnp.zeros((8, LANES), jnp.float32)

    def joined(r):
        first = total[r - HALF:r - HALF + 8] if HALF <= r < HALF + height else empty
        other = total[r:r + 8] if r < height else empty
        mixed = jnp.where(side, first, other)
        return mixed + pltpu.roll(mixed, trials, 1)

    half = frames // 2
    for q in range(reach + 1):
        for r in range(0, half, 8):
            top = joined(q * frames + r)
            low = joined(q * frames + half + r)
            part[q * half + r:q * half + r + 8, :] = jnp.where(side, top, low)
    rise = (reach + 1) * frames
    part[(reach + 1) * half:(reach + 1) * half + EDGE, :] = jnp.where(side, joined(rise), 0.0)

    def near(k):
        return pltpu.make_async_remote_copy(
            src_ref=part.at[pl.ds((reach - k) * half, half)], dst_ref=landed.at[k - 1],
            send_sem=near_send.at[k - 1], recv_sem=near_recv.at[k - 1],
            device_id={"tm": me - k}, device_id_type=MESH,
        )

    def up():
        return pltpu.make_async_remote_copy(
            src_ref=part.at[pl.ds((reach + 1) * half, EDGE)], dst_ref=risen,
            send_sem=near_send.at[reach], recv_sem=near_recv.at[reach],
            device_id={"tm": me + 1}, device_id_type=MESH,
        )

    for k in range(reach, 0, -1):
        @pl.when(me >= k)
        def _():
            near(k).start()

    @pl.when(me < count - 1)
    def _():
        up().start()

    close_round(2)
    open_round(3)

    @pl.when(me == 0)
    def _():
        risen[...] = jnp.zeros_like(risen)

    @pl.when(me > 0)
    def _():
        up().wait_recv()

    for k in range(1, reach + 1):
        @pl.when(me + k >= count)
        def _():
            landed[k - 1] = jnp.zeros((half, LANES), jnp.float32)

        @pl.when(me + k < count)
        def _():
            near(k).wait_recv()

    series = part[reach * half:(reach + 1) * half, :]
    for k in range(1, reach + 1):
        series = series + landed[k - 1]
    series = series + jnp.concatenate([risen[...], jnp.zeros((half - EDGE, LANES), jnp.float32)], axis=0)
    turned = pltpu.roll(series, trials, 1)

    def fold(value, op):
        return op(value, pltpu.roll(value, trials, 1))

    piece = jnp.sum(series, axis=0, keepdims=True) * (1.0 / half)
    away = series - piece
    opposite = pltpu.roll(piece, trials, 1)
    mean = (piece + opposite) * 0.5
    gap = piece - opposite
    spread = fold(jnp.sum(away * away, axis=0, keepdims=True), jnp.add) + (0.5 * half) * (gap * gap)
    peak = fold(jnp.max(series, axis=0, keepdims=True), jnp.maximum)
    mine[...] = jnp.concatenate([mean, spread, peak, peak], axis=0)

    def flipped(k):
        place = me
        for bit, step in enumerate(steps_of):
            if k >> bit & 1:
                place = place + step
        return place

    def far(k):
        return pltpu.make_async_remote_copy(
            src_ref=mine, dst_ref=gathered.at[k - 1],
            send_sem=far_send.at[k - 1], recv_sem=far_recv.at[k - 1],
            device_id={"tm": flipped(k)}, device_id_type=MESH,
        )

    for i in range(3, len(rounds)):
        close_round(i)
        open_round(i + 1)
    for k in range(count - 1, 0, -1):
        far(k).start()
    live = jnp.maximum(jnp.sum(mask_ref[...].astype(jnp.float32)), 1.0)
    for k in range(1, count):
        far(k).wait_recv()
    means, spreads, peaks = gathered[:, 0, :], gathered[:, 1, :], gathered[:, 2, :]
    average = (mean + jnp.sum(means, axis=0, keepdims=True)) * (1.0 / count)
    offset = means - average
    squares = spread + jnp.sum(spreads, axis=0, keepdims=True)
    between = (mean - average) * (mean - average) + jnp.sum(offset * offset, axis=0, keepdims=True)
    variance = (squares + frames * between) * (1.0 / (frames * count))
    top = jnp.maximum(peak, jnp.max(peaks, axis=0, keepdims=True))
    deviation = jnp.sqrt(variance + 1e-05)
    z_ref[0:half, :] = ((series - average) / deviation)[:, :trials]
    z_ref[half:frames, :] = ((turned - average) / deviation)[:, :trials]
    stats_ref[...] = jnp.concatenate(
        [average / live, deviation / live, (top - average) / deviation], axis=0
    )[:, :trials]

    @pl.when(me < count - 1)
    def _():
        forward().wait_send()
        up().wait_send()

    @pl.when(me > 0)
    def _():
        backward().wait_send()

    swap().wait_send()
    for k in range(1, reach + 1):
        @pl.when(me >= k)
        def _():
            near(k).wait_send()
    for k in range(1, count):
        far(k).wait_send()


def finish_kernel(z_ref, stats_ref, z_out, stats_out, sem):
    first = pltpu.make_async_copy(z_ref, z_out, sem.at[0])
    second = pltpu.make_async_copy(stats_ref, stats_out, sem.at[1])
    first.start()
    second.start()
    first.wait()
    second.wait()


def per_device(voltage, delays, chan_mask):
    frames = voltage.shape[2] // NCHAN
    trials = delays.shape[0]
    count = lax.axis_size("tm")
    lines = 2 * RADIX
    half = frames // 2
    blocks = LANES // RADIX
    wide = NCHAN // blocks
    reach = MAXD // frames
    steps = HALF + 2
    past = TAPS - 1
    vmem = pl.BlockSpec(memory_space=pltpu.VMEM)
    hbm = pl.BlockSpec(memory_space=pltpu.HBM)
    framed = voltage.reshape(2, 2, frames * RADIX, LANES).transpose(0, 2, 1, 3).reshape(2, frames, lines, LANES)
    operands = (framed, jnp.asarray(prototype()), jnp.asarray(twiddles()), jnp.asarray(transform_table()), delays,
                chan_mask.reshape(RADIX, LANES))
    dma = pltpu.SemaphoreType.DMA
    outputs = (
        jax.ShapeDtypeStruct((frames, trials), jnp.float32),
        jax.ShapeDtypeStruct((3, trials), jnp.float32),
    )
    results = pl.pallas_call(
        functools.partial(beam_kernel, count, frames, trials),
        out_shape=outputs,
        in_specs=[hbm] * 6,
        out_specs=(vmem,) * 2,
        scratch_shapes=[
            pltpu.VMEM((2, frames, lines, LANES), jnp.bfloat16),
            pltpu.VMEM((TAPS, PITCH, LANES), jnp.float32),
            pltpu.VMEM((2, RADIX, LANES), jnp.float32),
            pltpu.VMEM((2, 2 * LANES, 2 * LANES), jnp.bfloat16),
            pltpu.VMEM((trials // 2, NCHAN), jnp.int32),
            pltpu.VMEM((RADIX, LANES), jnp.int32),
            pltpu.VMEM((2, past - EDGE, lines, LANES), jnp.bfloat16),
            pltpu.VMEM((2, EDGE, lines, LANES), jnp.bfloat16),
            pltpu.VMEM((2, frames + past + EDGE, PITCH, LANES), jnp.float32),
            pltpu.VMEM((2 * frames * PITCH, LANES), jnp.float32),
            pltpu.VMEM((2 * EDGE * PITCH, LANES), jnp.float32),
            pltpu.VMEM((2 * RADIX * frames, 2 * LANES), jnp.float32),
            pltpu.VMEM((blocks, frames, 2 * LANES), jnp.float32),
            pltpu.VMEM((blocks, EDGE, 2 * LANES), jnp.float32),
            pltpu.VMEM((trials, LANES), jnp.float32),
            pltpu.VMEM((steps + 6, LANES), jnp.int32),
            pltpu.VMEM((steps + 6, LANES), jnp.float32),
            pltpu.VMEM((8, HALF + frames + 2 * EDGE, LANES), jnp.float32),
            pltpu.VMEM(((reach + 1) * half + EDGE, LANES), jnp.float32),
            pltpu.VMEM((reach, half, LANES), jnp.float32),
            pltpu.VMEM((EDGE, LANES), jnp.float32),
            pltpu.VMEM((4, LANES), jnp.float32),
            pltpu.VMEM((count - 1, 4, LANES), jnp.float32),
            dma((6,)),
            dma((2,)),
            dma((2,)),
            dma((reach + 1,)),
            dma((reach + 1,)),
            dma((count - 1,)),
            dma((count - 1,)),
            dma((2,)),
            pltpu.SemaphoreType.REGULAR((8,)),
        ],
        compiler_params=pltpu.CompilerParams(collective_id=1, vmem_limit_bytes=GRANT, has_side_effects=True),
        name="beam",
    )(*[pltpu.with_memory_space_constraint(v, pltpu.HBM) for v in operands])
    zscore, trial_stats = pl.pallas_call(
        finish_kernel,
        out_shape=outputs,
        in_specs=[vmem] * 2,
        out_specs=(hbm,) * 2,
        scratch_shapes=[dma((2,))],
        compiler_params=pltpu.CompilerParams(vmem_limit_bytes=GRANT),
        name="finish",
    )(*results)
    return (zscore.T, trial_stats)


def solution(mesh):
    in_specs = (P(None, None, ("beam", "tm")), P(), P("beam"))
    out_specs = (P(None, ("beam", "tm")), P(None, "beam"))
    return jax.shard_map(
        per_device, mesh=mesh, in_specs=in_specs, out_specs=out_specs, check_vma=False
    )
```

```python
import functools
import math

import jax
import jax.numpy as jnp
import numpy as np
from jax import lax
from jax.experimental import pallas as pl
from jax.experimental.pallas import tpu as pltpu
from jax.sharding import PartitionSpec as P

NCHAN = 2048
TAPS = 16
LANES = 128
RADIX = NCHAN // LANES
MAXD = 96
EDGE = 8
HALF = MAXD // 2
PITCH = 40
GRANT = 32 * 1024 * 1024
MESH = pl.DeviceIdType.MESH


def prototype():
    length = TAPS * NCHAN
    position = np.arange(length, dtype=np.float64)
    window = 0.54 - 0.46 * np.cos(2.0 * np.pi * position / (length - 1))
    shaped = np.sinc((position - (length - 1) / 2.0) / NCHAN) * window
    shaped = shaped * np.sqrt(NCHAN / np.sum(shaped * shaped))
    taps = shaped.reshape(TAPS, RADIX, 1, LANES)
    taps = np.broadcast_to(taps, (TAPS, RADIX, 2, LANES))
    return taps.reshape(TAPS, 2 * RADIX, LANES).astype(np.float32)


def twiddles():
    angle = -2.0 * np.pi * np.outer(np.arange(RADIX), np.arange(LANES)) / NCHAN
    return np.stack([np.cos(angle), np.sin(angle)]).astype(np.float32)


def transform_table():
    angle = -2.0 * np.pi * (np.outer(np.arange(LANES), np.arange(LANES)) % LANES) / LANES
    scale = 1.0 / math.sqrt(NCHAN)
    cos, sin = np.cos(angle) * scale, np.sin(angle) * scale
    full = np.block([[cos, sin], [-sin, cos]]).astype(np.float32)
    high = full.astype(jnp.bfloat16)
    low = (full - high.astype(np.float32)).astype(jnp.bfloat16)
    return np.stack([high, low])


def butterflies(items):
    count = len(items)
    if count == 1:
        return items
    even = butterflies(items[0::2])
    odd = butterflies(items[1::2])
    half = count // 2
    out = [None] * count
    for k in range(half):
        re, im = odd[k]
        if k == 0:
            tr, ti = re, im
        elif 4 * k == count:
            tr, ti = im, -re
        elif 8 * k == count:
            r = math.sqrt(0.5)
            tr, ti = (re + im) * r, (im - re) * r
        elif 8 * k == 3 * count:
            r = math.sqrt(0.5)
            tr, ti = (im - re) * r, (re + im) * (-r)
        else:
            c, s = math.cos(2 * math.pi * k / count), -math.sin(2 * math.pi * k / count)
            tr, ti = re * c - im * s, re * s + im * c
        er, ei = even[k]
        out[k] = (er + tr, ei + ti)
        out[k + half] = (er - tr, ei - ti)
    return out


def wait_some(sem, amount):
    @pl.when(amount > 0)
    def _():
        pl.semaphore_wait(sem, amount)


def beam_kernel(count, frames, trials, volt_hbm, taps_hbm, twid_hbm, table_hbm, delay_hbm, mask_hbm, z_ref, stats_ref,
                volt_ref, taps_ref, twid_ref, table_ref, delay_ref, mask_ref, before, after, ext, weighted, held, sections,
                spread_out, early, tally, blockno, within, acc, part, landed, risen, mine, gathered,
                load_sem, halo_send, halo_recv, near_send, near_recv, far_send, far_recv, swap_sem, know):
    me = lax.axis_index("tm")
    past = TAPS - 1
    lead = past - EDGE
    lines = 2 * RADIX
    own = EDGE + lead
    blocks = LANES // RADIX
    wide = NCHAN // blocks
    reach = MAXD // frames
    steps_of = [
        (1 << bit) * (1 - 2 * lax.rem(lax.div(me, 1 << bit), 2)) for bit in range((count - 1).bit_length())
    ]
    share = trials // 2
    core = lax.rem(me, 2)
    first = pl.multiple_of(core * share, share)
    barrier = pltpu.get_barrier_semaphore()

    def here(k):
        return (me + k >= 0) & (me + k < count)

    def tell(sem, k):
        @pl.when(here(k))
        def _():
            pl.semaphore_signal(sem, inc=1, device_id={"tm": me + k}, device_id_type=MESH)

    def number(distances):
        return sum(jnp.where(here(k), 1, 0) for k in distances)

    close = (-1, 1)
    for k in close:
        tell(barrier, k)
    pairs = ((volt_hbm, volt_ref), (taps_hbm, taps_ref.at[:, pl.ds(0, lines)]), (delay_hbm.at[pl.ds(first, share)], delay_ref), (twid_hbm, twid_ref),
             (table_hbm, table_ref), (mask_hbm, mask_ref))
    loads = [pltpu.make_async_copy(a, b, load_sem.at[i]) for i, (a, b) in enumerate(pairs)]
    for load in loads:
        load.start()

    def forward():
        return pltpu.make_async_remote_copy(
            src_ref=volt_ref.at[:, pl.ds(frames - lead, lead)], dst_ref=before,
            send_sem=halo_send.at[0], recv_sem=halo_recv.at[0], device_id={"tm": me + 1}, device_id_type=MESH,
        )

    def backward():
        return pltpu.make_async_remote_copy(
            src_ref=volt_ref.at[:, pl.ds(0, EDGE)], dst_ref=after,
            send_sem=halo_send.at[1], recv_sem=halo_recv.at[1], device_id={"tm": me - 1}, device_id_type=MESH,
        )

    @pl.when(core == 0)
    def _():
        for p in range(2):
            ext[p, 0:own, 0:lines] = jnp.zeros((own, lines, LANES), jnp.float32)

    @pl.when(core == 1)
    def _():
        for p in range(2):
            ext[p, own + frames:own + frames + EDGE, 0:lines] = jnp.zeros((EDGE, lines, LANES), jnp.float32)

    loads[0].wait()
    wait_some(barrier, number(close))

    @pl.when((core == 1) & (me < count - 1))
    def _():
        forward().start()

    @pl.when(me > 0)
    def _():
        backward().start()

    @pl.when((core == 0) & (me < count - 1))
    def _():
        forward().start()

    for p in range(2):
        ext[p, own:own + frames, 0:lines] = volt_ref[p].astype(jnp.float32)
    rounds = []
    known = 1
    while known < count - 1:
        rounds.append(known)
        known *= 2

    def open_round(i):
        if i < len(rounds):
            for k in (-rounds[i], rounds[i]):
                tell(know.at[i], k)

    def close_round(i):
        if i < len(rounds):
            wait_some(know.at[i], number((-rounds[i], rounds[i])))

    open_round(0)
    loads[1].wait()

    def fir(begin, size, out):
        for part_index in range(lines // 8):
            rows = pl.ds(8 * part_index, 8)
            taps = [taps_ref[j, rows, :] for j in range(TAPS)]

            def some(g, carry):
                for p in range(2):
                    sums = [None] * 4
                    for i in range(TAPS + 3):
                        sample = ext[p, begin + EDGE + 4 * g + i, rows, :]
                        for f in range(4):
                            if 0 <= i - f < TAPS:
                                term = taps[i - f] * sample
                                sums[f] = term if sums[f] is None else sums[f] + term
                    for f in range(4):
                        start = pl.multiple_of((p * size + 4 * g + f) * PITCH, 8) + 8 * part_index
                        out[pl.ds(start, 8), :] = sums[f]
                return carry

            lax.fori_loop(0, size // 4, some, 0, unroll=2)

    def rest(w0, low, high):
        for part_index in range(lines // 8):
            rows = pl.ds(8 * part_index, 8)
            for p in range(2):
                sums = {}
                for row in range(low, high):
                    sample = ext[p, row, rows, :]
                    for f in range(EDGE):
                        j = row - EDGE - w0 - f
                        if 0 <= j < TAPS:
                            term = taps_ref[j, rows, :] * sample
                            sums[f] = term if f not in sums else sums[f] + term
                for f, value in sums.items():
                    start = (p * EDGE + f) * PITCH + 8 * part_index
                    held[start:start + 8, :] = held[start:start + 8, :] + value

    def transform(size, out, begin, scale, weighted):
        group = 8
        rows_half = 2 * size
        for g in range(rows_half // group):
            p, f = divmod(g * group, size)
            first = (p * size + f) * PITCH
            items = []
            for m in range(RADIX):
                re = weighted[pl.ds(first + 2 * m, group, stride=PITCH), :]
                im = weighted[pl.ds(first + 2 * m + 1, group, stride=PITCH), :]
                items.append((re, im))
            for k1, (re, im) in enumerate(butterflies(items)):
                if k1:
                    c, s = twid_ref[0, k1:k1 + 1, :], twid_ref[1, k1:k1 + 1, :]
                    re, im = re * c - im * s, re * s + im * c
                place = k1 * rows_half + g * group
                sections[place:place + group, :LANES] = re
                sections[place:place + group, LANES:] = im
        both = sections[0:RADIX * rows_half, :]
        high = both.astype(jnp.bfloat16)
        low = (both - high.astype(jnp.float32)).astype(jnp.bfloat16)
        dot = functools.partial(jnp.dot, preferred_element_type=jnp.float32)
        spec = dot(high, table_ref[0]) + (dot(high, table_ref[1]) + dot(low, table_ref[0]))
        spec = spec * spec
        both_pols = (spec[:, :LANES] + spec[:, LANES:]).reshape(RADIX, 2, size, LANES)
        energy = both_pols[:, 0] + both_pols[:, 1]
        chunk = lax.broadcasted_iota(jnp.int32, (size, LANES), 1) >> 4
        for h in range(2):
            parts = [energy[8 * h + i] for i in range(8)]
            if size > EDGE:
                for bit in (4, 2, 1):
                    kept = (chunk & bit) == 0
                    for i in range(8):
                        if i & bit == 0:
                            low_part, high_part = parts[i], parts[i | bit]
                            parts[i] = jnp.where(kept, low_part, pltpu.roll(high_part, bit * RADIX, 1))
                            parts[i | bit] = jnp.where(kept, pltpu.roll(low_part, LANES - bit * RADIX, 1), high_part)
            else:
                moved = []
                for b in range(blocks):
                    mixed = parts[b]
                    for i in range(blocks):
                        if i != b:
                            turned = pltpu.roll(parts[i], (i - b) % blocks * RADIX, 1)
                            mixed = jnp.where(chunk == i, turned, mixed)
                    moved.append(mixed)
                parts = moved
            for b in range(blocks):
                out[b, pl.ds(begin, size), h * LANES:(h + 1) * LANES] = parts[b] * (usable[h][b:b + 1] * scale)

    def swap():
        rows = pl.ds(first, share)
        return pltpu.make_async_remote_copy(
            src_ref=tally.at[rows], dst_ref=tally.at[rows],
            send_sem=swap_sem.at[0], recv_sem=swap_sem.at[1],
            device_id={"tm": me + 1 - 2 * core}, device_id_type=MESH,
        )

    def admit(from_before):
        @pl.when(from_before & (me > 0))
        def _():
            forward().wait_recv()
            for p in range(2):
                ext[p, EDGE:own, 0:lines] = before[p].astype(jnp.float32)

        @pl.when(jnp.logical_not(from_before) & (me < count - 1))
        def _():
            backward().wait_recv()
            for p in range(2):
                ext[p, own + frames:own + frames + EDGE, 0:lines] = after[p].astype(jnp.float32)

    inner = frames - 2 * EDGE
    fir(EDGE, inner, weighted)
    for load in loads[2:]:
        load.wait()
    row = lax.broadcasted_iota(jnp.int32, (blocks, LANES), 1)
    even = mask_ref[pl.ds(0, blocks, stride=2), :]
    odd = mask_ref[pl.ds(1, blocks, stride=2), :]
    usable = []
    for h in range(2):
        place = (row & 7) * RADIX + 8 * h + (row >> 4)
        low = jnp.take_along_axis(even, place, axis=1, mode="promise_in_bounds")
        high = jnp.take_along_axis(odd, place, axis=1, mode="promise_in_bounds")
        usable.append(jnp.where((row & 8) == 0, low, high).astype(jnp.float32))

    level = lax.broadcasted_iota(jnp.int32, (8, LANES), 1)

    def look(table, place):
        return jnp.take_along_axis(table, place, axis=1, mode="promise_in_bounds")

    tables = NCHAN // LANES
    groups = range(share // 8)
    each = (level & (LANES // tables - 1)) * tables + (tables - 1)

    def table(g, b):
        return delay_ref[8 * g:8 * g + 8, b * LANES:(b + 1) * LANES]

    seldom = []
    for g in groups:
        kept = jnp.zeros((8, LANES), jnp.int32)
        for b in range(tables):
            kept = jnp.where((level >> 3) == b, look(table(g, b), each), kept)
        seldom.append(kept)
    coarse = [jnp.zeros((8, LANES), jnp.int32) for g in groups]
    for step in (64, 32, 16, 8, 4, 2, 1):
        for g in groups:
            seen = look(seldom[g], coarse[g] + (step - 1))
            coarse[g] = jnp.where(seen >= level, coarse[g] + step, coarse[g])
    fine = [jnp.zeros((8, LANES), jnp.int32) for g in groups]
    for step in (8, 4, 2, 1):
        for g in groups:
            place = (coarse[g] & 7) * tables + fine[g] + (step - 1)
            which = coarse[g] >> 3
            seen = jnp.full((8, LANES), -1, jnp.int32)
            for b in range(tables):
                seen = jnp.where(which == b, look(table(g, b), place), seen)
            fine[g] = jnp.where(seen >= level, fine[g] + step, fine[g])
    tally[pl.ds(first, share), :] = jnp.concatenate(
        [jnp.where(level == 0, NCHAN, coarse[g] * tables + fine[g]).astype(jnp.float32) for g in groups], axis=0)

    transform(inner, spread_out, EDGE, 1.0, weighted)
    swap().start()
    close_round(0)
    open_round(1)
    late_begin = pl.multiple_of(core * (frames - EDGE), EDGE)
    fir(late_begin, EDGE, held)
    admit(core == 1)
    begin = pl.multiple_of((1 - core) * (frames - EDGE), EDGE)
    fir(begin, EDGE, weighted)
    transform(EDGE, spread_out, begin, 1.0, weighted)
    acc[...] = jnp.zeros_like(acc)

    swap().wait_recv()
    total = tally[...]
    turned = jnp.concatenate([total, total], axis=0).T
    rows_kept = blockno.shape[0]
    near_side = lax.broadcasted_iota(jnp.int32, (rows_kept, LANES), 1) < trials
    total = jnp.where(near_side, turned[0:rows_kept], turned[HALF:HALF + rows_kept]).astype(jnp.int32)
    blockno[...] = total >> 8
    within[...] = (total & (wide - 1)).astype(jnp.float32)
    order = lax.broadcasted_iota(jnp.int32, (wide, LANES), 0)
    order = ((order & (RADIX - 1)) * RADIX + (order >> 4)).astype(jnp.float32)

    order = order.astype(jnp.bfloat16)

    def pick(j):
        end = jnp.broadcast_to(within[j:j + 1, :], (wide, LANES)).astype(jnp.bfloat16)
        return jnp.minimum(jnp.maximum(end - order, jnp.zeros_like(end)), jnp.ones_like(end))

    def dedisperse(source, size, offset):
        values = jnp.concatenate([source[b] for b in range(blocks)], axis=0).astype(jnp.bfloat16)
        dot = functools.partial(jnp.dot, preferred_element_type=jnp.float32)
        sums = dot(values, jnp.ones((wide, LANES), jnp.bfloat16))
        column = lax.broadcasted_iota(jnp.int32, (size, LANES), 1)
        prefix = jnp.zeros((size, LANES), jnp.float32)
        for b in range(blocks):
            prefix = prefix + jnp.where(column > b, sums[b * size:(b + 1) * size], 0.0)
        near_side = column < trials

        def add(j, change):
            a, m = divmod(j, 8)
            place = HALF + EDGE + offset - 8 * a
            acc[m, place:place + size] += change

        last = None
        for i in range(HALF // 2):
            found = dot(values, jnp.concatenate([pick(2 * i + 1), pick(2 * i + 2)], axis=1))
            for side in range(2):
                j = 2 * i + side + 1
                which = jnp.broadcast_to(blockno[j:j + 1, :], (size, LANES))
                inner = jnp.zeros((size, LANES), jnp.float32)
                for b in range(blocks):
                    inner = jnp.where(which == b, found[b * size:(b + 1) * size, side * LANES:(side + 1) * LANES], inner)
                now = inner + jnp.take_along_axis(prefix, which, axis=1, mode="promise_in_bounds")
                if j == 1:
                    whole = sums[0:size]
                    for b in range(1, blocks):
                        whole = whole + sums[b * size:(b + 1) * size]
                    add(0, jnp.where(near_side, whole - now, 0.0))
                    after_half = jnp.where(near_side, pltpu.roll(now, trials, 1), 0.0)
                else:
                    add(j - 1, last - now)
                last = now
        add(HALF, last - after_half)

    @pl.when(me == 0)
    def _():
        fir(-EDGE, EDGE, weighted)
        transform(EDGE, early, 0, 1.0, weighted)
        dedisperse(early, EDGE, -EDGE)

    admit(core == 0)

    @pl.when(core == 0)
    def _():
        rest(0, EDGE, own)

    @pl.when(core == 1)
    def _():
        rest(frames - EDGE, own + frames, own + frames + EDGE)

    transform(EDGE, spread_out, late_begin, jnp.where(me == count - 1, 0.0, 1.0), held)
    close_round(1)
    open_round(2)
    dedisperse(spread_out, frames, 0)
    height = HALF + frames + EDGE
    total = acc[0, 0:height]
    for m in range(1, 8):
        total = total + acc[m, m:m + height]
    side = lax.broadcasted_iota(jnp.int32, (8, LANES), 1) < trials
    empty = jnp.zeros((8, LANES), jnp.float32)

    def joined(r):
        first = total[r - HALF:r - HALF + 8] if HALF <= r < HALF + height else empty
        other = total[r:r + 8] if r < height else empty
        mixed = jnp.where(side, first, other)
        return mixed + pltpu.roll(mixed, trials, 1)

    half = frames // 2
    for q in range(reach + 1):
        for r in range(0, half, 8):
            top = joined(q * frames + r)
            low = joined(q * frames + half + r)
            part[q * half + r:q * half + r + 8, :] = jnp.where(side, top, low)
    rise = (reach + 1) * frames
    part[(reach + 1) * half:(reach + 1) * half + EDGE, :] = jnp.where(side, joined(rise), 0.0)

    def near(k):
        return pltpu.make_async_remote_copy(
            src_ref=part.at[pl.ds((reach - k) * half, half)], dst_ref=landed.at[k - 1],
            send_sem=near_send.at[k - 1], recv_sem=near_recv.at[k - 1],
            device_id={"tm": me - k}, device_id_type=MESH,
        )

    def up():
        return pltpu.make_async_remote_copy(
            src_ref=part.at[pl.ds((reach + 1) * half, EDGE)], dst_ref=risen,
            send_sem=near_send.at[reach], recv_sem=near_recv.at[reach],
            device_id={"tm": me + 1}, device_id_type=MESH,
        )

    for k in range(reach, 0, -1):
        @pl.when(me >= k)
        def _():
            near(k).start()

    @pl.when(me < count - 1)
    def _():
        up().start()

    close_round(2)
    open_round(3)

    @pl.when(me == 0)
    def _():
        risen[...] = jnp.zeros_like(risen)

    @pl.when(me > 0)
    def _():
        up().wait_recv()

    for k in range(1, reach + 1):
        @pl.when(me + k >= count)
        def _():
            landed[k - 1] = jnp.zeros((half, LANES), jnp.float32)

        @pl.when(me + k < count)
        def _():
            near(k).wait_recv()

    series = part[reach * half:(reach + 1) * half, :]
    for k in range(1, reach + 1):
        series = series + landed[k - 1]
    series = series + jnp.concatenate([risen[...], jnp.zeros((half - EDGE, LANES), jnp.float32)], axis=0)
    turned = pltpu.roll(series, trials, 1)

    def fold(value, op):
        return op(value, pltpu.roll(value, trials, 1))

    piece = jnp.sum(series, axis=0, keepdims=True) * (1.0 / half)
    away = series - piece
    opposite = pltpu.roll(piece, trials, 1)
    mean = (piece + opposite) * 0.5
    gap = piece - opposite
    spread = fold(jnp.sum(away * away, axis=0, keepdims=True), jnp.add) + (0.5 * half) * (gap * gap)
    peak = fold(jnp.max(series, axis=0, keepdims=True), jnp.maximum)
    mine[...] = jnp.concatenate([mean, spread, peak, peak], axis=0)

    def flipped(k):
        place = me
        for bit, step in enumerate(steps_of):
            if k >> bit & 1:
                place = place + step
        return place

    def far(k):
        return pltpu.make_async_remote_copy(
            src_ref=mine, dst_ref=gathered.at[k - 1],
            send_sem=far_send.at[k - 1], recv_sem=far_recv.at[k - 1],
            device_id={"tm": flipped(k)}, device_id_type=MESH,
        )

    for i in range(3, len(rounds)):
        close_round(i)
        open_round(i + 1)
    for k in range(count - 1, 0, -1):
        far(k).start()
    live = jnp.maximum(jnp.sum(mask_ref[...].astype(jnp.float32)), 1.0)
    for k in range(1, count):
        far(k).wait_recv()
    means, spreads, peaks = gathered[:, 0, :], gathered[:, 1, :], gathered[:, 2, :]
    average = (mean + jnp.sum(means, axis=0, keepdims=True)) * (1.0 / count)
    offset = means - average
    squares = spread + jnp.sum(spreads, axis=0, keepdims=True)
    between = (mean - average) * (mean - average) + jnp.sum(offset * offset, axis=0, keepdims=True)
    variance = (squares + frames * between) * (1.0 / (frames * count))
    top = jnp.maximum(peak, jnp.max(peaks, axis=0, keepdims=True))
    deviation = jnp.sqrt(variance + 1e-05)
    z_ref[0:half, :] = ((series - average) / deviation)[:, :trials]
    z_ref[half:frames, :] = ((turned - average) / deviation)[:, :trials]
    stats_ref[...] = jnp.concatenate(
        [average / live, deviation / live, (top - average) / deviation], axis=0
    )[:, :trials]

    @pl.when(me < count - 1)
    def _():
        forward().wait_send()
        up().wait_send()

    @pl.when(me > 0)
    def _():
        backward().wait_send()

    swap().wait_send()
    for k in range(1, reach + 1):
        @pl.when(me >= k)
        def _():
            near(k).wait_send()
    for k in range(1, count):
        far(k).wait_send()


def finish_kernel(z_ref, stats_ref, z_out, stats_out, sem):
    first = pltpu.make_async_copy(z_ref, z_out, sem.at[0])
    second = pltpu.make_async_copy(stats_ref, stats_out, sem.at[1])
    first.start()
    second.start()
    first.wait()
    second.wait()


def per_device(voltage, delays, chan_mask):
    frames = voltage.shape[2] // NCHAN
    trials = delays.shape[0]
    count = lax.axis_size("tm")
    lines = 2 * RADIX
    half = frames // 2
    blocks = LANES // RADIX
    wide = NCHAN // blocks
    reach = MAXD // frames
    past = TAPS - 1
    vmem = pl.BlockSpec(memory_space=pltpu.VMEM)
    hbm = pl.BlockSpec(memory_space=pltpu.HBM)
    framed = voltage.reshape(2, 2, frames * RADIX, LANES).transpose(0, 2, 1, 3).reshape(2, frames, lines, LANES)
    operands = (framed, jnp.asarray(prototype()), jnp.asarray(twiddles()), jnp.asarray(transform_table()), delays,
                chan_mask.reshape(RADIX, LANES))
    dma = pltpu.SemaphoreType.DMA
    outputs = (
        jax.ShapeDtypeStruct((frames, trials), jnp.float32),
        jax.ShapeDtypeStruct((3, trials), jnp.float32),
    )
    results = pl.pallas_call(
        functools.partial(beam_kernel, count, frames, trials),
        out_shape=outputs,
        in_specs=[hbm] * 6,
        out_specs=(vmem,) * 2,
        scratch_shapes=[
            pltpu.VMEM((2, frames, lines, LANES), jnp.bfloat16),
            pltpu.VMEM((TAPS, PITCH, LANES), jnp.float32),
            pltpu.VMEM((2, RADIX, LANES), jnp.float32),
            pltpu.VMEM((2, 2 * LANES, 2 * LANES), jnp.bfloat16),
            pltpu.VMEM((trials // 2, NCHAN), jnp.int32),
            pltpu.VMEM((RADIX, LANES), jnp.int32),
            pltpu.VMEM((2, past - EDGE, lines, LANES), jnp.bfloat16),
            pltpu.VMEM((2, EDGE, lines, LANES), jnp.bfloat16),
            pltpu.VMEM((2, frames + past + EDGE, PITCH, LANES), jnp.float32),
            pltpu.VMEM((2 * frames * PITCH, LANES), jnp.float32),
            pltpu.VMEM((2 * EDGE * PITCH, LANES), jnp.float32),
            pltpu.VMEM((2 * RADIX * frames, 2 * LANES), jnp.float32),
            pltpu.VMEM((blocks, frames, 2 * LANES), jnp.float32),
            pltpu.VMEM((blocks, EDGE, 2 * LANES), jnp.float32),
            pltpu.VMEM((trials, LANES), jnp.float32),
            pltpu.VMEM((HALF + 8, LANES), jnp.int32),
            pltpu.VMEM((HALF + 8, LANES), jnp.float32),
            pltpu.VMEM((8, HALF + frames + 2 * EDGE, LANES), jnp.float32),
            pltpu.VMEM(((reach + 1) * half + EDGE, LANES), jnp.float32),
            pltpu.VMEM((reach, half, LANES), jnp.float32),
            pltpu.VMEM((EDGE, LANES), jnp.float32),
            pltpu.VMEM((4, LANES), jnp.float32),
            pltpu.VMEM((count - 1, 4, LANES), jnp.float32),
            dma((6,)),
            dma((2,)),
            dma((2,)),
            dma((reach + 1,)),
            dma((reach + 1,)),
            dma((count - 1,)),
            dma((count - 1,)),
            dma((2,)),
            pltpu.SemaphoreType.REGULAR((8,)),
        ],
        compiler_params=pltpu.CompilerParams(collective_id=1, vmem_limit_bytes=GRANT, has_side_effects=True),
        name="beam",
    )(*[pltpu.with_memory_space_constraint(v, pltpu.HBM) for v in operands])
    zscore, trial_stats = pl.pallas_call(
        finish_kernel,
        out_shape=outputs,
        in_specs=[vmem] * 2,
        out_specs=(hbm,) * 2,
        scratch_shapes=[dma((2,))],
        compiler_params=pltpu.CompilerParams(vmem_limit_bytes=GRANT),
        name="finish",
    )(*results)
    return (zscore.T, trial_stats)


def solution(mesh):
    in_specs = (P(None, None, ("beam", "tm")), P(), P("beam"))
    out_specs = (P(None, ("beam", "tm")), P(None, "beam"))
    return jax.shard_map(
        per_device, mesh=mesh, in_specs=in_specs, out_specs=out_specs, check_vma=False
    )
```

```python
import functools
import math

import jax
import jax.numpy as jnp
import numpy as np
from jax import lax
from jax.experimental import pallas as pl
from jax.experimental.pallas import tpu as pltpu
from jax.sharding import PartitionSpec as P

NCHAN = 2048
TAPS = 16
LANES = 128
RADIX = NCHAN // LANES
MAXD = 96
EDGE = 8
HALF = MAXD // 2
PITCH = 40
GRANT = 32 * 1024 * 1024
MESH = pl.DeviceIdType.MESH


def prototype():
    length = TAPS * NCHAN
    position = np.arange(length, dtype=np.float64)
    window = 0.54 - 0.46 * np.cos(2.0 * np.pi * position / (length - 1))
    shaped = np.sinc((position - (length - 1) / 2.0) / NCHAN) * window
    shaped = shaped * np.sqrt(NCHAN / np.sum(shaped * shaped))
    taps = shaped.reshape(TAPS, RADIX, 1, LANES)
    taps = np.broadcast_to(taps, (TAPS, RADIX, 2, LANES))
    return taps.reshape(TAPS, 2 * RADIX, LANES).astype(np.float32)


def twiddles():
    angle = -2.0 * np.pi * np.outer(np.arange(RADIX), np.arange(LANES)) / NCHAN
    return np.stack([np.cos(angle), np.sin(angle)]).astype(np.float32)


def transform_table():
    angle = -2.0 * np.pi * (np.outer(np.arange(LANES), np.arange(LANES)) % LANES) / LANES
    scale = 1.0 / math.sqrt(NCHAN)
    cos, sin = np.cos(angle) * scale, np.sin(angle) * scale
    full = np.block([[cos, sin], [-sin, cos]]).astype(np.float32)
    high = full.astype(jnp.bfloat16)
    low = (full - high.astype(np.float32)).astype(jnp.bfloat16)
    return np.stack([high, low])


def butterflies(items):
    count = len(items)
    if count == 1:
        return items
    even = butterflies(items[0::2])
    odd = butterflies(items[1::2])
    half = count // 2
    out = [None] * count
    for k in range(half):
        re, im = odd[k]
        if k == 0:
            tr, ti = re, im
        elif 4 * k == count:
            tr, ti = im, -re
        elif 8 * k == count:
            r = math.sqrt(0.5)
            tr, ti = (re + im) * r, (im - re) * r
        elif 8 * k == 3 * count:
            r = math.sqrt(0.5)
            tr, ti = (im - re) * r, (re + im) * (-r)
        else:
            c, s = math.cos(2 * math.pi * k / count), -math.sin(2 * math.pi * k / count)
            tr, ti = re * c - im * s, re * s + im * c
        er, ei = even[k]
        out[k] = (er + tr, ei + ti)
        out[k + half] = (er - tr, ei - ti)
    return out


def wait_some(sem, amount):
    @pl.when(amount > 0)
    def _():
        pl.semaphore_wait(sem, amount)


def beam_kernel(count, frames, trials, volt_hbm, taps_hbm, twid_hbm, table_hbm, delay_hbm, mask_hbm, z_ref, stats_ref,
                volt_ref, taps_ref, twid_ref, table_ref, delay_ref, mask_ref, before, after, ext, weighted, held, sections,
                spread_out, early, tally, blockno, within, acc, part, landed, risen, mine, gathered,
                load_sem, halo_send, halo_recv, near_send, near_recv, far_send, far_recv, swap_sem, know):
    me = lax.axis_index("tm")
    past = TAPS - 1
    lead = past - EDGE
    lines = 2 * RADIX
    own = EDGE + lead
    blocks = LANES // RADIX
    wide = NCHAN // blocks
    reach = MAXD // frames
    steps_of = [
        (1 << bit) * (1 - 2 * lax.rem(lax.div(me, 1 << bit), 2)) for bit in range((count - 1).bit_length())
    ]
    share = trials // 2
    core = lax.rem(me, 2)
    first = pl.multiple_of(core * share, share)
    barrier = pltpu.get_barrier_semaphore()

    def here(k):
        return (me + k >= 0) & (me + k < count)

    def tell(sem, k):
        @pl.when(here(k))
        def _():
            pl.semaphore_signal(sem, inc=1, device_id={"tm": me + k}, device_id_type=MESH)

    def number(distances):
        return sum(jnp.where(here(k), 1, 0) for k in distances)

    close = (-1, 1)
    for k in close:
        tell(barrier, k)
    pairs = ((volt_hbm, volt_ref), (taps_hbm, taps_ref.at[:, pl.ds(0, lines)]), (delay_hbm.at[pl.ds(first, share)], delay_ref), (twid_hbm, twid_ref),
             (table_hbm, table_ref), (mask_hbm, mask_ref))
    loads = [pltpu.make_async_copy(a, b, load_sem.at[i]) for i, (a, b) in enumerate(pairs)]
    for load in loads:
        load.start()

    def forward():
        return pltpu.make_async_remote_copy(
            src_ref=volt_ref.at[:, pl.ds(frames - lead, lead)], dst_ref=before,
            send_sem=halo_send.at[0], recv_sem=halo_recv.at[0], device_id={"tm": me + 1}, device_id_type=MESH,
        )

    def backward():
        return pltpu.make_async_remote_copy(
            src_ref=volt_ref.at[:, pl.ds(0, EDGE)], dst_ref=after,
            send_sem=halo_send.at[1], recv_sem=halo_recv.at[1], device_id={"tm": me - 1}, device_id_type=MESH,
        )

    @pl.when(core == 0)
    def _():
        for p in range(2):
            ext[p, 0:own, 0:lines] = jnp.zeros((own, lines, LANES), jnp.float32)

    @pl.when(core == 1)
    def _():
        for p in range(2):
            ext[p, own + frames:own + frames + EDGE, 0:lines] = jnp.zeros((EDGE, lines, LANES), jnp.float32)

    loads[0].wait()
    wait_some(barrier, number(close))

    @pl.when((core == 1) & (me < count - 1))
    def _():
        forward().start()

    @pl.when(me > 0)
    def _():
        backward().start()

    @pl.when((core == 0) & (me < count - 1))
    def _():
        forward().start()

    for p in range(2):
        ext[p, own:own + frames, 0:lines] = volt_ref[p].astype(jnp.float32)
    rounds = []
    known = 1
    while known < count - 1:
        rounds.append(known)
        known *= 2

    def open_round(i):
        if i < len(rounds):
            for k in (-rounds[i], rounds[i]):
                tell(know.at[i], k)

    def close_round(i):
        if i < len(rounds):
            wait_some(know.at[i], number((-rounds[i], rounds[i])))

    open_round(0)
    loads[1].wait()

    def fir(begin, size, out):
        for part_index in range(lines // 8):
            rows = pl.ds(8 * part_index, 8)
            taps = [taps_ref[j, rows, :] for j in range(TAPS)]

            def some(g, carry):
                for p in range(2):
                    sums = [None] * 4
                    for i in range(TAPS + 3):
                        sample = ext[p, begin + EDGE + 4 * g + i, rows, :]
                        for f in range(4):
                            if 0 <= i - f < TAPS:
                                term = taps[i - f] * sample
                                sums[f] = term if sums[f] is None else sums[f] + term
                    for f in range(4):
                        start = pl.multiple_of((p * size + 4 * g + f) * PITCH, 8) + 8 * part_index
                        out[pl.ds(start, 8), :] = sums[f]
                return carry

            lax.fori_loop(0, size // 4, some, 0, unroll=2)

    def rest(w0, low, high):
        for part_index in range(lines // 8):
            rows = pl.ds(8 * part_index, 8)
            for p in range(2):
                sums = {}
                for row in range(low, high):
                    sample = ext[p, row, rows, :]
                    for f in range(EDGE):
                        j = row - EDGE - w0 - f
                        if 0 <= j < TAPS:
                            term = taps_ref[j, rows, :] * sample
                            sums[f] = term if f not in sums else sums[f] + term
                for f, value in sums.items():
                    start = (p * EDGE + f) * PITCH + 8 * part_index
                    held[start:start + 8, :] = held[start:start + 8, :] + value

    def transform(size, out, begin, scale, weighted):
        group = 8
        rows_half = 2 * size
        for g in range(rows_half // group):
            p, f = divmod(g * group, size)
            first = (p * size + f) * PITCH
            items = []
            for m in range(RADIX):
                re = weighted[pl.ds(first + 2 * m, group, stride=PITCH), :]
                im = weighted[pl.ds(first + 2 * m + 1, group, stride=PITCH), :]
                items.append((re, im))
            for k1, (re, im) in enumerate(butterflies(items)):
                if k1:
                    c, s = twid_ref[0, k1:k1 + 1, :], twid_ref[1, k1:k1 + 1, :]
                    re, im = re * c - im * s, re * s + im * c
                place = k1 * rows_half + g * group
                sections[place:place + group, :LANES] = re
                sections[place:place + group, LANES:] = im
        both = sections[0:RADIX * rows_half, :]
        high = both.astype(jnp.bfloat16)
        low = (both - high.astype(jnp.float32)).astype(jnp.bfloat16)
        dot = functools.partial(jnp.dot, preferred_element_type=jnp.float32)
        spec = dot(high, table_ref[0]) + (dot(high, table_ref[1]) + dot(low, table_ref[0]))
        spec = spec * spec
        both_pols = (spec[:, :LANES] + spec[:, LANES:]).reshape(RADIX, 2, size, LANES)
        energy = both_pols[:, 0] + both_pols[:, 1]
        chunk = lax.broadcasted_iota(jnp.int32, (size, LANES), 1) >> 4
        for h in range(2):
            parts = [energy[8 * h + i] for i in range(8)]
            if size > EDGE:
                for bit in (4, 2, 1):
                    kept = (chunk & bit) == 0
                    for i in range(8):
                        if i & bit == 0:
                            low_part, high_part = parts[i], parts[i | bit]
                            parts[i] = jnp.where(kept, low_part, pltpu.roll(high_part, bit * RADIX, 1))
                            parts[i | bit] = jnp.where(kept, pltpu.roll(low_part, LANES - bit * RADIX, 1), high_part)
            else:
                moved = []
                for b in range(blocks):
                    mixed = parts[b]
                    for i in range(blocks):
                        if i != b:
                            turned = pltpu.roll(parts[i], (i - b) % blocks * RADIX, 1)
                            mixed = jnp.where(chunk == i, turned, mixed)
                    moved.append(mixed)
                parts = moved
            for b in range(blocks):
                out[b, pl.ds(begin, size), h * LANES:(h + 1) * LANES] = parts[b] * (usable[h][b:b + 1] * scale)

    def swap():
        rows = pl.ds(first, share)
        return pltpu.make_async_remote_copy(
            src_ref=tally.at[rows], dst_ref=tally.at[rows],
            send_sem=swap_sem.at[0], recv_sem=swap_sem.at[1],
            device_id={"tm": me + 1 - 2 * core}, device_id_type=MESH,
        )

    def admit(from_before):
        @pl.when(from_before & (me > 0))
        def _():
            forward().wait_recv()
            for p in range(2):
                ext[p, EDGE:own, 0:lines] = before[p].astype(jnp.float32)

        @pl.when(jnp.logical_not(from_before) & (me < count - 1))
        def _():
            backward().wait_recv()
            for p in range(2):
                ext[p, own + frames:own + frames + EDGE, 0:lines] = after[p].astype(jnp.float32)

    inner = frames - 2 * EDGE
    fir(EDGE, inner, weighted)
    for load in loads[2:]:
        load.wait()
    row = lax.broadcasted_iota(jnp.int32, (blocks, LANES), 1)
    even = mask_ref[pl.ds(0, blocks, stride=2), :]
    odd = mask_ref[pl.ds(1, blocks, stride=2), :]
    usable = []
    for h in range(2):
        place = (row & 7) * RADIX + 8 * h + (row >> 4)
        low = jnp.take_along_axis(even, place, axis=1, mode="promise_in_bounds")
        high = jnp.take_along_axis(odd, place, axis=1, mode="promise_in_bounds")
        usable.append(jnp.where((row & 8) == 0, low, high).astype(jnp.float32))

    level = lax.broadcasted_iota(jnp.int32, (8, LANES), 1)

    def look(table, place):
        return jnp.take_along_axis(table, place, axis=1, mode="promise_in_bounds")

    tables = NCHAN // LANES
    groups = range(share // 8)
    each = (level & (LANES // tables - 1)) * tables + (tables - 1)

    def table(g, b):
        return delay_ref[8 * g:8 * g + 8, b * LANES:(b + 1) * LANES]

    seldom = []
    for g in groups:
        kept = jnp.zeros((8, LANES), jnp.int32)
        for b in range(tables):
            kept = jnp.where((level >> 3) == b, look(table(g, b), each), kept)
        seldom.append(kept)
    coarse = [jnp.zeros((8, LANES), jnp.int32) for g in groups]
    for step in (64, 32, 16, 8, 4, 2, 1):
        for g in groups:
            seen = look(seldom[g], coarse[g] + (step - 1))
            coarse[g] = jnp.where(seen >= level, coarse[g] + step, coarse[g])
    fine = [jnp.zeros((8, LANES), jnp.int32) for g in groups]
    for step in (8, 4, 2, 1):
        for g in groups:
            place = (coarse[g] & 7) * tables + fine[g] + (step - 1)
            which = coarse[g] >> 3
            seen = jnp.full((8, LANES), -1, jnp.int32)
            for b in range(tables):
                seen = jnp.where(which == b, look(table(g, b), place), seen)
            fine[g] = jnp.where(seen >= level, fine[g] + step, fine[g])
    tally[pl.ds(first, share), :] = jnp.concatenate(
        [jnp.where(level == 0, NCHAN, coarse[g] * tables + fine[g]).astype(jnp.float32) for g in groups], axis=0)

    transform(inner, spread_out, EDGE, 1.0, weighted)
    swap().start()
    close_round(0)
    open_round(1)
    late_begin = pl.multiple_of(core * (frames - EDGE), EDGE)
    fir(late_begin, EDGE, held)
    admit(core == 1)
    begin = pl.multiple_of((1 - core) * (frames - EDGE), EDGE)
    fir(begin, EDGE, weighted)
    transform(EDGE, spread_out, begin, 1.0, weighted)
    acc[...] = jnp.zeros_like(acc)

    swap().wait_recv()
    total = tally[...]
    turned = jnp.concatenate([total, total], axis=0).T
    rows_kept = blockno.shape[0]
    near_side = lax.broadcasted_iota(jnp.int32, (rows_kept, LANES), 1) < trials
    total = jnp.where(near_side, turned[0:rows_kept], turned[HALF:HALF + rows_kept]).astype(jnp.int32)
    blockno[...] = total >> 8
    within[...] = (total & (wide - 1)).astype(jnp.float32)
    order = lax.broadcasted_iota(jnp.int32, (wide, LANES), 0)
    order = ((order & (RADIX - 1)) * RADIX + (order >> 4)).astype(jnp.float32)

    order = order.astype(jnp.bfloat16)

    def pick(j):
        end = jnp.broadcast_to(within[j:j + 1, :], (wide, LANES)).astype(jnp.bfloat16)
        return jnp.minimum(jnp.maximum(end - order, jnp.zeros_like(end)), jnp.ones_like(end))

    def dedisperse(source, begin, size, offset):
        values = jnp.concatenate([source[b, begin:begin + size] for b in range(blocks)], axis=0).astype(jnp.bfloat16)
        dot = functools.partial(jnp.dot, preferred_element_type=jnp.float32)
        sums = dot(values, jnp.ones((wide, LANES), jnp.bfloat16))
        column = lax.broadcasted_iota(jnp.int32, (size, LANES), 1)
        prefix = jnp.zeros((size, LANES), jnp.float32)
        for b in range(blocks):
            prefix = prefix + jnp.where(column > b, sums[b * size:(b + 1) * size], 0.0)
        near_side = column < trials

        def add(j, change):
            a, m = divmod(j, 8)
            place = HALF + EDGE + offset - 8 * a
            acc[m, place:place + size] += change

        last = None
        for i in range(HALF // 2):
            found = dot(values, jnp.concatenate([pick(2 * i + 1), pick(2 * i + 2)], axis=1))
            for side in range(2):
                j = 2 * i + side + 1
                which = jnp.broadcast_to(blockno[j:j + 1, :], (size, LANES))
                inner = jnp.zeros((size, LANES), jnp.float32)
                for b in range(blocks):
                    inner = jnp.where(which == b, found[b * size:(b + 1) * size, side * LANES:(side + 1) * LANES], inner)
                now = inner + jnp.take_along_axis(prefix, which, axis=1, mode="promise_in_bounds")
                if j == 1:
                    whole = sums[0:size]
                    for b in range(1, blocks):
                        whole = whole + sums[b * size:(b + 1) * size]
                    add(0, jnp.where(near_side, whole - now, 0.0))
                    after_half = jnp.where(near_side, pltpu.roll(now, trials, 1), 0.0)
                else:
                    add(j - 1, last - now)
                last = now
        add(HALF, last - after_half)

    @pl.when(me == 0)
    def _():
        fir(-EDGE, EDGE, weighted)
        transform(EDGE, early, 0, 1.0, weighted)
        dedisperse(early, 0, EDGE, -EDGE)

    @pl.when(core == 1)
    def _():
        dedisperse(spread_out, 0, frames - EDGE, 0)

    admit(core == 0)

    @pl.when(core == 0)
    def _():
        rest(0, EDGE, own)

    @pl.when(core == 1)
    def _():
        rest(frames - EDGE, own + frames, own + frames + EDGE)

    transform(EDGE, spread_out, late_begin, jnp.where(me == count - 1, 0.0, 1.0), held)
    close_round(1)
    open_round(2)
    @pl.when(core == 0)
    def _():
        dedisperse(spread_out, 0, frames, 0)

    @pl.when(core == 1)
    def _():
        dedisperse(spread_out, frames - EDGE, EDGE, frames - EDGE)

    height = HALF + frames + EDGE
    total = acc[0, 0:height]
    for m in range(1, 8):
        total = total + acc[m, m:m + height]
    side = lax.broadcasted_iota(jnp.int32, (8, LANES), 1) < trials
    empty = jnp.zeros((8, LANES), jnp.float32)

    def joined(r):
        first = total[r - HALF:r - HALF + 8] if HALF <= r < HALF + height else empty
        other = total[r:r + 8] if r < height else empty
        mixed = jnp.where(side, first, other)
        return mixed + pltpu.roll(mixed, trials, 1)

    half = frames // 2
    for q in range(reach + 1):
        for r in range(0, half, 8):
            top = joined(q * frames + r)
            low = joined(q * frames + half + r)
            part[q * half + r:q * half + r + 8, :] = jnp.where(side, top, low)
    rise = (reach + 1) * frames
    part[(reach + 1) * half:(reach + 1) * half + EDGE, :] = jnp.where(side, joined(rise), 0.0)

    def near(k):
        return pltpu.make_async_remote_copy(
            src_ref=part.at[pl.ds((reach - k) * half, half)], dst_ref=landed.at[k - 1],
            send_sem=near_send.at[k - 1], recv_sem=near_recv.at[k - 1],
            device_id={"tm": me - k}, device_id_type=MESH,
        )

    def up():
        return pltpu.make_async_remote_copy(
            src_ref=part.at[pl.ds((reach + 1) * half, EDGE)], dst_ref=risen,
            send_sem=near_send.at[reach], recv_sem=near_recv.at[reach],
            device_id={"tm": me + 1}, device_id_type=MESH,
        )

    for k in range(reach, 0, -1):
        @pl.when(me >= k)
        def _():
            near(k).start()

    @pl.when(me < count - 1)
    def _():
        up().start()

    close_round(2)
    open_round(3)

    @pl.when(me == 0)
    def _():
        risen[...] = jnp.zeros_like(risen)

    @pl.when(me > 0)
    def _():
        up().wait_recv()

    for k in range(1, reach + 1):
        @pl.when(me + k >= count)
        def _():
            landed[k - 1] = jnp.zeros((half, LANES), jnp.float32)

        @pl.when(me + k < count)
        def _():
            near(k).wait_recv()

    series = part[reach * half:(reach + 1) * half, :]
    for k in range(1, reach + 1):
        series = series + landed[k - 1]
    series = series + jnp.concatenate([risen[...], jnp.zeros((half - EDGE, LANES), jnp.float32)], axis=0)
    turned = pltpu.roll(series, trials, 1)

    def fold(value, op):
        return op(value, pltpu.roll(value, trials, 1))

    piece = jnp.sum(series, axis=0, keepdims=True) * (1.0 / half)
    away = series - piece
    opposite = pltpu.roll(piece, trials, 1)
    mean = (piece + opposite) * 0.5
    gap = piece - opposite
    spread = fold(jnp.sum(away * away, axis=0, keepdims=True), jnp.add) + (0.5 * half) * (gap * gap)
    peak = fold(jnp.max(series, axis=0, keepdims=True), jnp.maximum)
    mine[...] = jnp.concatenate([mean, spread, peak, peak], axis=0)

    def flipped(k):
        place = me
        for bit, step in enumerate(steps_of):
            if k >> bit & 1:
                place = place + step
        return place

    def far(k):
        return pltpu.make_async_remote_copy(
            src_ref=mine, dst_ref=gathered.at[k - 1],
            send_sem=far_send.at[k - 1], recv_sem=far_recv.at[k - 1],
            device_id={"tm": flipped(k)}, device_id_type=MESH,
        )

    for i in range(3, len(rounds)):
        close_round(i)
        open_round(i + 1)
    for k in range(count - 1, 0, -1):
        far(k).start()
    live = jnp.maximum(jnp.sum(mask_ref[...].astype(jnp.float32)), 1.0)
    for k in range(1, count):
        far(k).wait_recv()
    means, spreads, peaks = gathered[:, 0, :], gathered[:, 1, :], gathered[:, 2, :]
    average = (mean + jnp.sum(means, axis=0, keepdims=True)) * (1.0 / count)
    offset = means - average
    squares = spread + jnp.sum(spreads, axis=0, keepdims=True)
    between = (mean - average) * (mean - average) + jnp.sum(offset * offset, axis=0, keepdims=True)
    variance = (squares + frames * between) * (1.0 / (frames * count))
    top = jnp.maximum(peak, jnp.max(peaks, axis=0, keepdims=True))
    deviation = jnp.sqrt(variance + 1e-05)
    z_ref[0:half, :] = ((series - average) / deviation)[:, :trials]
    z_ref[half:frames, :] = ((turned - average) / deviation)[:, :trials]
    stats_ref[...] = jnp.concatenate(
        [average / live, deviation / live, (top - average) / deviation], axis=0
    )[:, :trials]

    @pl.when(me < count - 1)
    def _():
        forward().wait_send()
        up().wait_send()

    @pl.when(me > 0)
    def _():
        backward().wait_send()

    swap().wait_send()
    for k in range(1, reach + 1):
        @pl.when(me >= k)
        def _():
            near(k).wait_send()
    for k in range(1, count):
        far(k).wait_send()


def finish_kernel(z_ref, stats_ref, z_out, stats_out, sem):
    first = pltpu.make_async_copy(z_ref, z_out, sem.at[0])
    second = pltpu.make_async_copy(stats_ref, stats_out, sem.at[1])
    first.start()
    second.start()
    first.wait()
    second.wait()


def per_device(voltage, delays, chan_mask):
    frames = voltage.shape[2] // NCHAN
    trials = delays.shape[0]
    count = lax.axis_size("tm")
    lines = 2 * RADIX
    half = frames // 2
    blocks = LANES // RADIX
    wide = NCHAN // blocks
    reach = MAXD // frames
    past = TAPS - 1
    vmem = pl.BlockSpec(memory_space=pltpu.VMEM)
    hbm = pl.BlockSpec(memory_space=pltpu.HBM)
    framed = voltage.reshape(2, 2, frames * RADIX, LANES).transpose(0, 2, 1, 3).reshape(2, frames, lines, LANES)
    operands = (framed, jnp.asarray(prototype()), jnp.asarray(twiddles()), jnp.asarray(transform_table()), delays,
                chan_mask.reshape(RADIX, LANES))
    dma = pltpu.SemaphoreType.DMA
    outputs = (
        jax.ShapeDtypeStruct((frames, trials), jnp.float32),
        jax.ShapeDtypeStruct((3, trials), jnp.float32),
    )
    results = pl.pallas_call(
        functools.partial(beam_kernel, count, frames, trials),
        out_shape=outputs,
        in_specs=[hbm] * 6,
        out_specs=(vmem,) * 2,
        scratch_shapes=[
            pltpu.VMEM((2, frames, lines, LANES), jnp.bfloat16),
            pltpu.VMEM((TAPS, PITCH, LANES), jnp.float32),
            pltpu.VMEM((2, RADIX, LANES), jnp.float32),
            pltpu.VMEM((2, 2 * LANES, 2 * LANES), jnp.bfloat16),
            pltpu.VMEM((trials // 2, NCHAN), jnp.int32),
            pltpu.VMEM((RADIX, LANES), jnp.int32),
            pltpu.VMEM((2, past - EDGE, lines, LANES), jnp.bfloat16),
            pltpu.VMEM((2, EDGE, lines, LANES), jnp.bfloat16),
            pltpu.VMEM((2, frames + past + EDGE, PITCH, LANES), jnp.float32),
            pltpu.VMEM((2 * frames * PITCH, LANES), jnp.float32),
            pltpu.VMEM((2 * EDGE * PITCH, LANES), jnp.float32),
            pltpu.VMEM((2 * RADIX * frames, 2 * LANES), jnp.float32),
            pltpu.VMEM((blocks, frames, 2 * LANES), jnp.float32),
            pltpu.VMEM((blocks, EDGE, 2 * LANES), jnp.float32),
            pltpu.VMEM((trials, LANES), jnp.float32),
            pltpu.VMEM((HALF + 8, LANES), jnp.int32),
            pltpu.VMEM((HALF + 8, LANES), jnp.float32),
            pltpu.VMEM((8, HALF + frames + 2 * EDGE, LANES), jnp.float32),
            pltpu.VMEM(((reach + 1) * half + EDGE, LANES), jnp.float32),
            pltpu.VMEM((reach, half, LANES), jnp.float32),
            pltpu.VMEM((EDGE, LANES), jnp.float32),
            pltpu.VMEM((4, LANES), jnp.float32),
            pltpu.VMEM((count - 1, 4, LANES), jnp.float32),
            dma((6,)),
            dma((2,)),
            dma((2,)),
            dma((reach + 1,)),
            dma((reach + 1,)),
            dma((count - 1,)),
            dma((count - 1,)),
            dma((2,)),
            pltpu.SemaphoreType.REGULAR((8,)),
        ],
        compiler_params=pltpu.CompilerParams(collective_id=1, vmem_limit_bytes=GRANT, has_side_effects=True),
        name="beam",
    )(*[pltpu.with_memory_space_constraint(v, pltpu.HBM) for v in operands])
    zscore, trial_stats = pl.pallas_call(
        finish_kernel,
        out_shape=outputs,
        in_specs=[vmem] * 2,
        out_specs=(hbm,) * 2,
        scratch_shapes=[dma((2,))],
        compiler_params=pltpu.CompilerParams(vmem_limit_bytes=GRANT),
        name="finish",
    )(*results)
    return (zscore.T, trial_stats)


def solution(mesh):
    in_specs = (P(None, None, ("beam", "tm")), P(), P("beam"))
    out_specs = (P(None, ("beam", "tm")), P(None, "beam"))
    return jax.shard_map(
        per_device, mesh=mesh, in_specs=in_specs, out_specs=out_specs, check_vma=False
    )
```

```python
import functools
import math

import jax
import jax.numpy as jnp
import numpy as np
from jax import lax
from jax.experimental import pallas as pl
from jax.experimental.pallas import tpu as pltpu
from jax.sharding import PartitionSpec as P

NCHAN = 2048
TAPS = 16
LANES = 128
RADIX = NCHAN // LANES
MAXD = 96
EDGE = 8
HALF = MAXD // 2
PITCH = 40
GRANT = 32 * 1024 * 1024
MESH = pl.DeviceIdType.MESH


def prototype():
    length = TAPS * NCHAN
    position = np.arange(length, dtype=np.float64)
    window = 0.54 - 0.46 * np.cos(2.0 * np.pi * position / (length - 1))
    shaped = np.sinc((position - (length - 1) / 2.0) / NCHAN) * window
    shaped = shaped * np.sqrt(NCHAN / np.sum(shaped * shaped))
    taps = shaped.reshape(TAPS, RADIX, 1, LANES)
    taps = np.broadcast_to(taps, (TAPS, RADIX, 2, LANES))
    return taps.reshape(TAPS, 2 * RADIX, LANES).astype(np.float32)


def twiddles():
    angle = -2.0 * np.pi * np.outer(np.arange(RADIX), np.arange(LANES)) / NCHAN
    return np.stack([np.cos(angle), np.sin(angle)]).astype(np.float32)


def transform_table():
    angle = -2.0 * np.pi * (np.outer(np.arange(LANES), np.arange(LANES)) % LANES) / LANES
    scale = 1.0 / math.sqrt(NCHAN)
    cos, sin = np.cos(angle) * scale, np.sin(angle) * scale
    full = np.block([[cos, sin], [-sin, cos]]).astype(np.float32)
    high = full.astype(jnp.bfloat16)
    low = (full - high.astype(np.float32)).astype(jnp.bfloat16)
    return np.stack([high, low])


def butterflies(items):
    count = len(items)
    if count == 1:
        return items
    even = butterflies(items[0::2])
    odd = butterflies(items[1::2])
    half = count // 2
    out = [None] * count
    for k in range(half):
        re, im = odd[k]
        if k == 0:
            tr, ti = re, im
        elif 4 * k == count:
            tr, ti = im, -re
        elif 8 * k == count:
            r = math.sqrt(0.5)
            tr, ti = (re + im) * r, (im - re) * r
        elif 8 * k == 3 * count:
            r = math.sqrt(0.5)
            tr, ti = (im - re) * r, (re + im) * (-r)
        else:
            c, s = math.cos(2 * math.pi * k / count), -math.sin(2 * math.pi * k / count)
            tr, ti = re * c - im * s, re * s + im * c
        er, ei = even[k]
        out[k] = (er + tr, ei + ti)
        out[k + half] = (er - tr, ei - ti)
    return out


def wait_some(sem, amount):
    @pl.when(amount > 0)
    def _():
        pl.semaphore_wait(sem, amount)


def beam_kernel(count, frames, trials, volt_hbm, taps_hbm, twid_hbm, table_hbm, delay_hbm, mask_hbm, z_ref, stats_ref,
                volt_ref, taps_ref, twid_ref, table_ref, delay_ref, mask_ref, before, after, ext, weighted, held, sections,
                spread_out, early, tally, blockno, within, acc, part, landed, risen, mine, gathered,
                load_sem, halo_send, halo_recv, near_send, near_recv, far_send, far_recv, swap_sem, know):
    me = lax.axis_index("tm")
    past = TAPS - 1
    lead = past - EDGE
    lines = 2 * RADIX
    own = EDGE + lead
    blocks = LANES // RADIX
    wide = NCHAN // blocks
    reach = MAXD // frames
    steps_of = [
        (1 << bit) * (1 - 2 * lax.rem(lax.div(me, 1 << bit), 2)) for bit in range((count - 1).bit_length())
    ]
    share = trials // 2
    core = lax.rem(me, 2)
    first = pl.multiple_of(core * share, share)
    barrier = pltpu.get_barrier_semaphore()

    def here(k):
        return (me + k >= 0) & (me + k < count)

    def tell(sem, k):
        @pl.when(here(k))
        def _():
            pl.semaphore_signal(sem, inc=1, device_id={"tm": me + k}, device_id_type=MESH)

    def number(distances):
        return sum(jnp.where(here(k), 1, 0) for k in distances)

    close = (-1, 1)
    pairs = ((volt_hbm, volt_ref), (taps_hbm, taps_ref.at[:, pl.ds(0, lines)]), (delay_hbm.at[pl.ds(first, share)], delay_ref), (twid_hbm, twid_ref),
             (table_hbm, table_ref), (mask_hbm, mask_ref))
    loads = [pltpu.make_async_copy(a, b, load_sem.at[i]) for i, (a, b) in enumerate(pairs)]
    loads[0].start()
    for k in close:
        tell(barrier, k)
    for load in loads[1:]:
        load.start()

    def forward():
        return pltpu.make_async_remote_copy(
            src_ref=volt_ref.at[:, pl.ds(frames - lead, lead)], dst_ref=before,
            send_sem=halo_send.at[0], recv_sem=halo_recv.at[0], device_id={"tm": me + 1}, device_id_type=MESH,
        )

    def backward():
        return pltpu.make_async_remote_copy(
            src_ref=volt_ref.at[:, pl.ds(0, EDGE)], dst_ref=after,
            send_sem=halo_send.at[1], recv_sem=halo_recv.at[1], device_id={"tm": me - 1}, device_id_type=MESH,
        )

    @pl.when(core == 0)
    def _():
        for p in range(2):
            ext[p, 0:own, 0:lines] = jnp.zeros((own, lines, LANES), jnp.float32)

    @pl.when(core == 1)
    def _():
        for p in range(2):
            ext[p, own + frames:own + frames + EDGE, 0:lines] = jnp.zeros((EDGE, lines, LANES), jnp.float32)

    loads[0].wait()
    wait_some(barrier, number(close))

    @pl.when((core == 1) & (me < count - 1))
    def _():
        forward().start()

    @pl.when(me > 0)
    def _():
        backward().start()

    @pl.when((core == 0) & (me < count - 1))
    def _():
        forward().start()

    for p in range(2):
        ext[p, own:own + frames, 0:lines] = volt_ref[p].astype(jnp.float32)
    rounds = []
    known = 1
    while known < count - 1:
        rounds.append(known)
        known *= 2

    def open_round(i):
        if i < len(rounds):
            for k in (-rounds[i], rounds[i]):
                tell(know.at[i], k)

    def close_round(i):
        if i < len(rounds):
            wait_some(know.at[i], number((-rounds[i], rounds[i])))

    open_round(0)
    loads[1].wait()

    def fir(begin, size, out):
        for part_index in range(lines // 8):
            rows = pl.ds(8 * part_index, 8)
            taps = [taps_ref[j, rows, :] for j in range(TAPS)]

            def some(g, carry):
                for p in range(2):
                    sums = [None] * 4
                    for i in range(TAPS + 3):
                        sample = ext[p, begin + EDGE + 4 * g + i, rows, :]
                        for f in range(4):
                            if 0 <= i - f < TAPS:
                                term = taps[i - f] * sample
                                sums[f] = term if sums[f] is None else sums[f] + term
                    for f in range(4):
                        start = pl.multiple_of((p * size + 4 * g + f) * PITCH, 8) + 8 * part_index
                        out[pl.ds(start, 8), :] = sums[f]
                return carry

            lax.fori_loop(0, size // 4, some, 0, unroll=2)

    def rest(w0, low, high):
        for part_index in range(lines // 8):
            rows = pl.ds(8 * part_index, 8)
            for p in range(2):
                sums = {}
                for row in range(low, high):
                    sample = ext[p, row, rows, :]
                    for f in range(EDGE):
                        j = row - EDGE - w0 - f
                        if 0 <= j < TAPS:
                            term = taps_ref[j, rows, :] * sample
                            sums[f] = term if f not in sums else sums[f] + term
                for f, value in sums.items():
                    start = (p * EDGE + f) * PITCH + 8 * part_index
                    held[start:start + 8, :] = held[start:start + 8, :] + value

    def transform(size, out, begin, scale, weighted):
        group = 8
        rows_half = 2 * size
        for g in range(rows_half // group):
            p, f = divmod(g * group, size)
            first = (p * size + f) * PITCH
            items = []
            for m in range(RADIX):
                re = weighted[pl.ds(first + 2 * m, group, stride=PITCH), :]
                im = weighted[pl.ds(first + 2 * m + 1, group, stride=PITCH), :]
                items.append((re, im))
            for k1, (re, im) in enumerate(butterflies(items)):
                if k1:
                    c, s = twid_ref[0, k1:k1 + 1, :], twid_ref[1, k1:k1 + 1, :]
                    re, im = re * c - im * s, re * s + im * c
                place = k1 * rows_half + g * group
                sections[place:place + group, :LANES] = re
                sections[place:place + group, LANES:] = im
        both = sections[0:RADIX * rows_half, :]
        high = both.astype(jnp.bfloat16)
        low = (both - high.astype(jnp.float32)).astype(jnp.bfloat16)
        dot = functools.partial(jnp.dot, preferred_element_type=jnp.float32)
        spec = dot(high, table_ref[0]) + (dot(high, table_ref[1]) + dot(low, table_ref[0]))
        spec = spec * spec
        both_pols = (spec[:, :LANES] + spec[:, LANES:]).reshape(RADIX, 2, size, LANES)
        energy = both_pols[:, 0] + both_pols[:, 1]
        chunk = lax.broadcasted_iota(jnp.int32, (size, LANES), 1) >> 4
        for h in range(2):
            parts = [energy[8 * h + i] for i in range(8)]
            if size > EDGE:
                for bit in (4, 2, 1):
                    kept = (chunk & bit) == 0
                    for i in range(8):
                        if i & bit == 0:
                            low_part, high_part = parts[i], parts[i | bit]
                            parts[i] = jnp.where(kept, low_part, pltpu.roll(high_part, bit * RADIX, 1))
                            parts[i | bit] = jnp.where(kept, pltpu.roll(low_part, LANES - bit * RADIX, 1), high_part)
            else:
                moved = []
                for b in range(blocks):
                    mixed = parts[b]
                    for i in range(blocks):
                        if i != b:
                            turned = pltpu.roll(parts[i], (i - b) % blocks * RADIX, 1)
                            mixed = jnp.where(chunk == i, turned, mixed)
                    moved.append(mixed)
                parts = moved
            for b in range(blocks):
                out[b, pl.ds(begin, size), h * LANES:(h + 1) * LANES] = parts[b] * (usable[h][b:b + 1] * scale)

    def swap():
        rows = pl.ds(first, share)
        return pltpu.make_async_remote_copy(
            src_ref=tally.at[rows], dst_ref=tally.at[rows],
            send_sem=swap_sem.at[0], recv_sem=swap_sem.at[1],
            device_id={"tm": me + 1 - 2 * core}, device_id_type=MESH,
        )

    def admit(from_before):
        @pl.when(from_before & (me > 0))
        def _():
            forward().wait_recv()
            for p in range(2):
                ext[p, EDGE:own, 0:lines] = before[p].astype(jnp.float32)

        @pl.when(jnp.logical_not(from_before) & (me < count - 1))
        def _():
            backward().wait_recv()
            for p in range(2):
                ext[p, own + frames:own + frames + EDGE, 0:lines] = after[p].astype(jnp.float32)

    inner = frames - 2 * EDGE
    fir(EDGE, inner, weighted)
    for load in loads[2:]:
        load.wait()
    row = lax.broadcasted_iota(jnp.int32, (blocks, LANES), 1)
    even = mask_ref[pl.ds(0, blocks, stride=2), :]
    odd = mask_ref[pl.ds(1, blocks, stride=2), :]
    usable = []
    for h in range(2):
        place = (row & 7) * RADIX + 8 * h + (row >> 4)
        low = jnp.take_along_axis(even, place, axis=1, mode="promise_in_bounds")
        high = jnp.take_along_axis(odd, place, axis=1, mode="promise_in_bounds")
        usable.append(jnp.where((row & 8) == 0, low, high).astype(jnp.float32))

    level = lax.broadcasted_iota(jnp.int32, (8, LANES), 1)

    def look(table, place):
        return jnp.take_along_axis(table, place, axis=1, mode="promise_in_bounds")

    tables = NCHAN // LANES
    groups = range(share // 8)
    each = (level & (LANES // tables - 1)) * tables + (tables - 1)

    def table(g, b):
        return delay_ref[8 * g:8 * g + 8, b * LANES:(b + 1) * LANES]

    seldom = []
    for g in groups:
        kept = jnp.zeros((8, LANES), jnp.int32)
        for b in range(tables):
            kept = jnp.where((level >> 3) == b, look(table(g, b), each), kept)
        seldom.append(kept)
    coarse = [jnp.zeros((8, LANES), jnp.int32) for g in groups]
    for step in (64, 32, 16, 8, 4, 2, 1):
        for g in groups:
            seen = look(seldom[g], coarse[g] + (step - 1))
            coarse[g] = jnp.where(seen >= level, coarse[g] + step, coarse[g])
    fine = [jnp.zeros((8, LANES), jnp.int32) for g in groups]
    for step in (8, 4, 2, 1):
        for g in groups:
            place = (coarse[g] & 7) * tables + fine[g] + (step - 1)
            which = coarse[g] >> 3
            seen = jnp.full((8, LANES), -1, jnp.int32)
            for b in range(tables):
                seen = jnp.where(which == b, look(table(g, b), place), seen)
            fine[g] = jnp.where(seen >= level, fine[g] + step, fine[g])
    tally[pl.ds(first, share), :] = jnp.concatenate(
        [jnp.where(level == 0, NCHAN, coarse[g] * tables + fine[g]).astype(jnp.float32) for g in groups], axis=0)

    transform(inner, spread_out, EDGE, 1.0, weighted)
    swap().start()
    close_round(0)
    open_round(1)
    late_begin = pl.multiple_of(core * (frames - EDGE), EDGE)
    fir(late_begin, EDGE, held)
    admit(core == 1)
    begin = pl.multiple_of((1 - core) * (frames - EDGE), EDGE)
    fir(begin, EDGE, weighted)
    transform(EDGE, spread_out, begin, 1.0, weighted)
    acc[...] = jnp.zeros_like(acc)

    swap().wait_recv()
    total = tally[...]
    turned = jnp.concatenate([total, total], axis=0).T
    rows_kept = blockno.shape[0]
    near_side = lax.broadcasted_iota(jnp.int32, (rows_kept, LANES), 1) < trials
    total = jnp.where(near_side, turned[0:rows_kept], turned[HALF:HALF + rows_kept]).astype(jnp.int32)
    blockno[...] = total >> 8
    within[...] = (total & (wide - 1)).astype(jnp.float32)
    order = lax.broadcasted_iota(jnp.int32, (wide, LANES), 0)
    order = ((order & (RADIX - 1)) * RADIX + (order >> 4)).astype(jnp.float32)

    order = order.astype(jnp.bfloat16)

    def pick(j):
        end = jnp.broadcast_to(within[j:j + 1, :], (wide, LANES)).astype(jnp.bfloat16)
        return jnp.minimum(jnp.maximum(end - order, jnp.zeros_like(end)), jnp.ones_like(end))

    def dedisperse(source, begin, size, offset):
        values = jnp.concatenate([source[b, begin:begin + size] for b in range(blocks)], axis=0).astype(jnp.bfloat16)
        dot = functools.partial(jnp.dot, preferred_element_type=jnp.float32)
        sums = dot(values, jnp.ones((wide, LANES), jnp.bfloat16))
        column = lax.broadcasted_iota(jnp.int32, (size, LANES), 1)
        prefix = jnp.zeros((size, LANES), jnp.float32)
        for b in range(blocks):
            prefix = prefix + jnp.where(column > b, sums[b * size:(b + 1) * size], 0.0)
        near_side = column < trials

        def add(j, change):
            a, m = divmod(j, 8)
            place = HALF + EDGE + offset - 8 * a
            acc[m, place:place + size] += change

        last = None
        for i in range(HALF // 2):
            found = dot(values, jnp.concatenate([pick(2 * i + 1), pick(2 * i + 2)], axis=1))
            for side in range(2):
                j = 2 * i + side + 1
                which = jnp.broadcast_to(blockno[j:j + 1, :], (size, LANES))
                inner = jnp.zeros((size, LANES), jnp.float32)
                for b in range(blocks):
                    inner = jnp.where(which == b, found[b * size:(b + 1) * size, side * LANES:(side + 1) * LANES], inner)
                now = inner + jnp.take_along_axis(prefix, which, axis=1, mode="promise_in_bounds")
                if j == 1:
                    whole = sums[0:size]
                    for b in range(1, blocks):
                        whole = whole + sums[b * size:(b + 1) * size]
                    add(0, jnp.where(near_side, whole - now, 0.0))
                    after_half = jnp.where(near_side, pltpu.roll(now, trials, 1), 0.0)
                else:
                    add(j - 1, last - now)
                last = now
        add(HALF, last - after_half)

    @pl.when(me == 0)
    def _():
        fir(-EDGE, EDGE, weighted)
        transform(EDGE, early, 0, 1.0, weighted)
        dedisperse(early, 0, EDGE, -EDGE)

    @pl.when(core == 1)
    def _():
        dedisperse(spread_out, 0, frames - EDGE, 0)

    admit(core == 0)

    @pl.when(core == 0)
    def _():
        rest(0, EDGE, own)

    @pl.when(core == 1)
    def _():
        rest(frames - EDGE, own + frames, own + frames + EDGE)

    transform(EDGE, spread_out, late_begin, jnp.where(me == count - 1, 0.0, 1.0), held)
    close_round(1)
    open_round(2)
    @pl.when(core == 0)
    def _():
        dedisperse(spread_out, 0, frames, 0)

    @pl.when(core == 1)
    def _():
        dedisperse(spread_out, frames - EDGE, EDGE, frames - EDGE)

    height = HALF + frames + EDGE
    total = acc[0, 0:height]
    for m in range(1, 8):
        total = total + acc[m, m:m + height]
    side = lax.broadcasted_iota(jnp.int32, (8, LANES), 1) < trials
    empty = jnp.zeros((8, LANES), jnp.float32)

    def joined(r):
        first = total[r - HALF:r - HALF + 8] if HALF <= r < HALF + height else empty
        other = total[r:r + 8] if r < height else empty
        mixed = jnp.where(side, first, other)
        return mixed + pltpu.roll(mixed, trials, 1)

    half = frames // 2
    for q in range(reach + 1):
        for r in range(0, half, 8):
            top = joined(q * frames + r)
            low = joined(q * frames + half + r)
            part[q * half + r:q * half + r + 8, :] = jnp.where(side, top, low)
    rise = (reach + 1) * frames
    part[(reach + 1) * half:(reach + 1) * half + EDGE, :] = jnp.where(side, joined(rise), 0.0)

    def near(k):
        return pltpu.make_async_remote_copy(
            src_ref=part.at[pl.ds((reach - k) * half, half)], dst_ref=landed.at[k - 1],
            send_sem=near_send.at[k - 1], recv_sem=near_recv.at[k - 1],
            device_id={"tm": me - k}, device_id_type=MESH,
        )

    def up():
        return pltpu.make_async_remote_copy(
            src_ref=part.at[pl.ds((reach + 1) * half, EDGE)], dst_ref=risen,
            send_sem=near_send.at[reach], recv_sem=near_recv.at[reach],
            device_id={"tm": me + 1}, device_id_type=MESH,
        )

    for k in range(reach, 0, -1):
        @pl.when(me >= k)
        def _():
            near(k).start()

    @pl.when(me < count - 1)
    def _():
        up().start()

    close_round(2)
    open_round(3)

    @pl.when(me == 0)
    def _():
        risen[...] = jnp.zeros_like(risen)

    @pl.when(me > 0)
    def _():
        up().wait_recv()

    for k in range(1, reach + 1):
        @pl.when(me + k >= count)
        def _():
            landed[k - 1] = jnp.zeros((half, LANES), jnp.float32)

        @pl.when(me + k < count)
        def _():
            near(k).wait_recv()

    series = part[reach * half:(reach + 1) * half, :]
    for k in range(1, reach + 1):
        series = series + landed[k - 1]
    series = series + jnp.concatenate([risen[...], jnp.zeros((half - EDGE, LANES), jnp.float32)], axis=0)
    turned = pltpu.roll(series, trials, 1)

    def fold(value, op):
        return op(value, pltpu.roll(value, trials, 1))

    piece = jnp.sum(series, axis=0, keepdims=True) * (1.0 / half)
    away = series - piece
    opposite = pltpu.roll(piece, trials, 1)
    mean = (piece + opposite) * 0.5
    gap = piece - opposite
    spread = fold(jnp.sum(away * away, axis=0, keepdims=True), jnp.add) + (0.5 * half) * (gap * gap)
    peak = fold(jnp.max(series, axis=0, keepdims=True), jnp.maximum)
    mine[...] = jnp.concatenate([mean, spread, peak, peak], axis=0)

    def flipped(k):
        place = me
        for bit, step in enumerate(steps_of):
            if k >> bit & 1:
                place = place + step
        return place

    def far(k):
        return pltpu.make_async_remote_copy(
            src_ref=mine, dst_ref=gathered.at[k - 1],
            send_sem=far_send.at[k - 1], recv_sem=far_recv.at[k - 1],
            device_id={"tm": flipped(k)}, device_id_type=MESH,
        )

    for i in range(3, len(rounds)):
        close_round(i)
        open_round(i + 1)
    for k in range(count - 1, 0, -1):
        far(k).start()
    live = jnp.maximum(jnp.sum(mask_ref[...].astype(jnp.float32)), 1.0)
    for k in range(1, count):
        far(k).wait_recv()
    means, spreads, peaks = gathered[:, 0, :], gathered[:, 1, :], gathered[:, 2, :]
    average = (mean + jnp.sum(means, axis=0, keepdims=True)) * (1.0 / count)
    offset = means - average
    squares = spread + jnp.sum(spreads, axis=0, keepdims=True)
    between = (mean - average) * (mean - average) + jnp.sum(offset * offset, axis=0, keepdims=True)
    variance = (squares + frames * between) * (1.0 / (frames * count))
    top = jnp.maximum(peak, jnp.max(peaks, axis=0, keepdims=True))
    deviation = jnp.sqrt(variance + 1e-05)
    z_ref[0:half, :] = ((series - average) / deviation)[:, :trials]
    z_ref[half:frames, :] = ((turned - average) / deviation)[:, :trials]
    stats_ref[...] = jnp.concatenate(
        [average / live, deviation / live, (top - average) / deviation], axis=0
    )[:, :trials]

    @pl.when(me < count - 1)
    def _():
        forward().wait_send()
        up().wait_send()

    @pl.when(me > 0)
    def _():
        backward().wait_send()

    swap().wait_send()
    for k in range(1, reach + 1):
        @pl.when(me >= k)
        def _():
            near(k).wait_send()
    for k in range(1, count):
        far(k).wait_send()


def finish_kernel(z_ref, stats_ref, z_out, stats_out, sem):
    first = pltpu.make_async_copy(z_ref, z_out, sem.at[0])
    second = pltpu.make_async_copy(stats_ref, stats_out, sem.at[1])
    first.start()
    second.start()
    first.wait()
    second.wait()


def per_device(voltage, delays, chan_mask):
    frames = voltage.shape[2] // NCHAN
    trials = delays.shape[0]
    count = lax.axis_size("tm")
    lines = 2 * RADIX
    half = frames // 2
    blocks = LANES // RADIX
    wide = NCHAN // blocks
    reach = MAXD // frames
    past = TAPS - 1
    vmem = pl.BlockSpec(memory_space=pltpu.VMEM)
    hbm = pl.BlockSpec(memory_space=pltpu.HBM)
    framed = voltage.reshape(2, 2, frames * RADIX, LANES).transpose(0, 2, 1, 3).reshape(2, frames, lines, LANES)
    operands = (framed, jnp.asarray(prototype()), jnp.asarray(twiddles()), jnp.asarray(transform_table()), delays,
                chan_mask.reshape(RADIX, LANES))
    dma = pltpu.SemaphoreType.DMA
    outputs = (
        jax.ShapeDtypeStruct((frames, trials), jnp.float32),
        jax.ShapeDtypeStruct((3, trials), jnp.float32),
    )
    results = pl.pallas_call(
        functools.partial(beam_kernel, count, frames, trials),
        out_shape=outputs,
        in_specs=[hbm] * 6,
        out_specs=(vmem,) * 2,
        scratch_shapes=[
            pltpu.VMEM((2, frames, lines, LANES), jnp.bfloat16),
            pltpu.VMEM((TAPS, PITCH, LANES), jnp.float32),
            pltpu.VMEM((2, RADIX, LANES), jnp.float32),
            pltpu.VMEM((2, 2 * LANES, 2 * LANES), jnp.bfloat16),
            pltpu.VMEM((trials // 2, NCHAN), jnp.int32),
            pltpu.VMEM((RADIX, LANES), jnp.int32),
            pltpu.VMEM((2, past - EDGE, lines, LANES), jnp.bfloat16),
            pltpu.VMEM((2, EDGE, lines, LANES), jnp.bfloat16),
            pltpu.VMEM((2, frames + past + EDGE, PITCH, LANES), jnp.float32),
            pltpu.VMEM((2 * frames * PITCH, LANES), jnp.float32),
            pltpu.VMEM((2 * EDGE * PITCH, LANES), jnp.float32),
            pltpu.VMEM((2 * RADIX * frames, 2 * LANES), jnp.float32),
            pltpu.VMEM((blocks, frames, 2 * LANES), jnp.float32),
            pltpu.VMEM((blocks, EDGE, 2 * LANES), jnp.float32),
            pltpu.VMEM((trials, LANES), jnp.float32),
            pltpu.VMEM((HALF + 8, LANES), jnp.int32),
            pltpu.VMEM((HALF + 8, LANES), jnp.float32),
            pltpu.VMEM((8, HALF + frames + 2 * EDGE, LANES), jnp.float32),
            pltpu.VMEM(((reach + 1) * half + EDGE, LANES), jnp.float32),
            pltpu.VMEM((reach, half, LANES), jnp.float32),
            pltpu.VMEM((EDGE, LANES), jnp.float32),
            pltpu.VMEM((4, LANES), jnp.float32),
            pltpu.VMEM((count - 1, 4, LANES), jnp.float32),
            dma((6,)),
            dma((2,)),
            dma((2,)),
            dma((reach + 1,)),
            dma((reach + 1,)),
            dma((count - 1,)),
            dma((count - 1,)),
            dma((2,)),
            pltpu.SemaphoreType.REGULAR((8,)),
        ],
        compiler_params=pltpu.CompilerParams(collective_id=1, vmem_limit_bytes=GRANT, has_side_effects=True),
        name="beam",
    )(*[pltpu.with_memory_space_constraint(v, pltpu.HBM) for v in operands])
    zscore, trial_stats = pl.pallas_call(
        finish_kernel,
        out_shape=outputs,
        in_specs=[vmem] * 2,
        out_specs=(hbm,) * 2,
        scratch_shapes=[dma((2,))],
        compiler_params=pltpu.CompilerParams(vmem_limit_bytes=GRANT),
        name="finish",
    )(*results)
    return (zscore.T, trial_stats)


def solution(mesh):
    in_specs = (P(None, None, ("beam", "tm")), P(), P("beam"))
    out_specs = (P(None, ("beam", "tm")), P(None, "beam"))
    return jax.shard_map(
        per_device, mesh=mesh, in_specs=in_specs, out_specs=out_specs, check_vma=False
    )
```

```python
import functools
import math

import jax
import jax.numpy as jnp
import numpy as np
from jax import lax
from jax.experimental import pallas as pl
from jax.experimental.pallas import tpu as pltpu
from jax.sharding import PartitionSpec as P

NCHAN = 2048
TAPS = 16
LANES = 128
RADIX = NCHAN // LANES
MAXD = 96
EDGE = 8
HALF = MAXD // 2
PITCH = 40
GRANT = 32 * 1024 * 1024
MESH = pl.DeviceIdType.MESH


def prototype():
    length = TAPS * NCHAN
    position = np.arange(length, dtype=np.float64)
    window = 0.54 - 0.46 * np.cos(2.0 * np.pi * position / (length - 1))
    shaped = np.sinc((position - (length - 1) / 2.0) / NCHAN) * window
    shaped = shaped * np.sqrt(NCHAN / np.sum(shaped * shaped))
    taps = shaped.reshape(TAPS, RADIX, 1, LANES)
    taps = np.broadcast_to(taps, (TAPS, RADIX, 2, LANES))
    return taps.reshape(TAPS, 2 * RADIX, LANES).astype(np.float32)


def twiddles():
    angle = -2.0 * np.pi * np.outer(np.arange(RADIX), np.arange(LANES)) / NCHAN
    return np.stack([np.cos(angle), np.sin(angle)]).astype(np.float32)


def transform_table():
    angle = -2.0 * np.pi * (np.outer(np.arange(LANES), np.arange(LANES)) % LANES) / LANES
    scale = 1.0 / math.sqrt(NCHAN)
    cos, sin = np.cos(angle) * scale, np.sin(angle) * scale
    full = np.block([[cos, sin], [-sin, cos]]).astype(np.float32)
    high = full.astype(jnp.bfloat16)
    low = (full - high.astype(np.float32)).astype(jnp.bfloat16)
    return np.stack([high, low])


def butterflies(items):
    count = len(items)
    if count == 1:
        return items
    even = butterflies(items[0::2])
    odd = butterflies(items[1::2])
    half = count // 2
    out = [None] * count
    for k in range(half):
        re, im = odd[k]
        if k == 0:
            tr, ti = re, im
        elif 4 * k == count:
            tr, ti = im, -re
        elif 8 * k == count:
            r = math.sqrt(0.5)
            tr, ti = (re + im) * r, (im - re) * r
        elif 8 * k == 3 * count:
            r = math.sqrt(0.5)
            tr, ti = (im - re) * r, (re + im) * (-r)
        else:
            c, s = math.cos(2 * math.pi * k / count), -math.sin(2 * math.pi * k / count)
            tr, ti = re * c - im * s, re * s + im * c
        er, ei = even[k]
        out[k] = (er + tr, ei + ti)
        out[k + half] = (er - tr, ei - ti)
    return out


def wait_some(sem, amount):
    @pl.when(amount > 0)
    def _():
        pl.semaphore_wait(sem, amount)


def beam_kernel(count, frames, trials, volt_hbm, taps_hbm, twid_hbm, table_hbm, delay_hbm, mask_hbm, z_ref, stats_ref,
                volt_ref, taps_ref, twid_ref, table_ref, delay_ref, mask_ref, before, after, ext, weighted, held, sections,
                spread_out, early, tally, blockno, within, acc, part, landed, risen, mine, gathered,
                load_sem, halo_send, halo_recv, near_send, near_recv, far_send, far_recv, swap_sem, know):
    me = lax.axis_index("tm")
    past = TAPS - 1
    lead = past - EDGE
    lines = 2 * RADIX
    own = EDGE + lead
    blocks = LANES // RADIX
    wide = NCHAN // blocks
    reach = MAXD // frames
    steps_of = [
        (1 << bit) * (1 - 2 * lax.rem(lax.div(me, 1 << bit), 2)) for bit in range((count - 1).bit_length())
    ]
    share = trials // 2
    core = lax.rem(me, 2)
    first = pl.multiple_of(core * share, share)
    barrier = pltpu.get_barrier_semaphore()

    def here(k):
        return (me + k >= 0) & (me + k < count)

    def tell(sem, k):
        @pl.when(here(k))
        def _():
            pl.semaphore_signal(sem, inc=1, device_id={"tm": me + k}, device_id_type=MESH)

    def number(distances):
        return sum(jnp.where(here(k), 1, 0) for k in distances)

    close = (-1, 1)
    pairs = ((volt_hbm, volt_ref), (taps_hbm, taps_ref.at[:, pl.ds(0, lines)]), (delay_hbm.at[pl.ds(first, share)], delay_ref), (twid_hbm, twid_ref),
             (table_hbm, table_ref), (mask_hbm, mask_ref))
    loads = [pltpu.make_async_copy(a, b, load_sem.at[i]) for i, (a, b) in enumerate(pairs)]
    loads[0].start()
    for k in close:
        tell(barrier, k)
    for load in loads[1:]:
        load.start()

    def forward():
        return pltpu.make_async_remote_copy(
            src_ref=volt_ref.at[:, pl.ds(frames - lead, lead)], dst_ref=before,
            send_sem=halo_send.at[0], recv_sem=halo_recv.at[0], device_id={"tm": me + 1}, device_id_type=MESH,
        )

    def backward():
        return pltpu.make_async_remote_copy(
            src_ref=volt_hbm.at[:, pl.ds(0, EDGE)], dst_ref=after,
            send_sem=halo_send.at[1], recv_sem=halo_recv.at[1], device_id={"tm": me - 1}, device_id_type=MESH,
        )

    @pl.when(core == 0)
    def _():
        for p in range(2):
            ext[p, 0:own, 0:lines] = jnp.zeros((own, lines, LANES), jnp.float32)

    @pl.when(core == 1)
    def _():
        for p in range(2):
            ext[p, own + frames:own + frames + EDGE, 0:lines] = jnp.zeros((EDGE, lines, LANES), jnp.float32)

    wait_some(barrier, number(close))

    @pl.when(me > 0)
    def _():
        backward().start()

    loads[0].wait()

    @pl.when((core == 1) & (me < count - 1))
    def _():
        forward().start()


    @pl.when((core == 0) & (me < count - 1))
    def _():
        forward().start()

    for p in range(2):
        ext[p, own:own + frames, 0:lines] = volt_ref[p].astype(jnp.float32)
    rounds = []
    known = 1
    while known < count - 1:
        rounds.append(known)
        known *= 2

    def open_round(i):
        if i < len(rounds):
            for k in (-rounds[i], rounds[i]):
                tell(know.at[i], k)

    def close_round(i):
        if i < len(rounds):
            wait_some(know.at[i], number((-rounds[i], rounds[i])))

    open_round(0)
    loads[1].wait()

    def fir(begin, size, out):
        for part_index in range(lines // 8):
            rows = pl.ds(8 * part_index, 8)
            taps = [taps_ref[j, rows, :] for j in range(TAPS)]

            def some(g, carry):
                for p in range(2):
                    sums = [None] * 4
                    for i in range(TAPS + 3):
                        sample = ext[p, begin + EDGE + 4 * g + i, rows, :]
                        for f in range(4):
                            if 0 <= i - f < TAPS:
                                term = taps[i - f] * sample
                                sums[f] = term if sums[f] is None else sums[f] + term
                    for f in range(4):
                        start = pl.multiple_of((p * size + 4 * g + f) * PITCH, 8) + 8 * part_index
                        out[pl.ds(start, 8), :] = sums[f]
                return carry

            lax.fori_loop(0, size // 4, some, 0, unroll=2)

    def rest(w0, low, high):
        for part_index in range(lines // 8):
            rows = pl.ds(8 * part_index, 8)
            for p in range(2):
                sums = {}
                for row in range(low, high):
                    sample = ext[p, row, rows, :]
                    for f in range(EDGE):
                        j = row - EDGE - w0 - f
                        if 0 <= j < TAPS:
                            term = taps_ref[j, rows, :] * sample
                            sums[f] = term if f not in sums else sums[f] + term
                for f, value in sums.items():
                    start = (p * EDGE + f) * PITCH + 8 * part_index
                    held[start:start + 8, :] = held[start:start + 8, :] + value

    def transform(size, out, begin, scale, weighted):
        group = 8
        rows_half = 2 * size
        for g in range(rows_half // group):
            p, f = divmod(g * group, size)
            first = (p * size + f) * PITCH
            items = []
            for m in range(RADIX):
                re = weighted[pl.ds(first + 2 * m, group, stride=PITCH), :]
                im = weighted[pl.ds(first + 2 * m + 1, group, stride=PITCH), :]
                items.append((re, im))
            for k1, (re, im) in enumerate(butterflies(items)):
                if k1:
                    c, s = twid_ref[0, k1:k1 + 1, :], twid_ref[1, k1:k1 + 1, :]
                    re, im = re * c - im * s, re * s + im * c
                place = k1 * rows_half + g * group
                sections[place:place + group, :LANES] = re
                sections[place:place + group, LANES:] = im
        both = sections[0:RADIX * rows_half, :]
        high = both.astype(jnp.bfloat16)
        low = (both - high.astype(jnp.float32)).astype(jnp.bfloat16)
        dot = functools.partial(jnp.dot, preferred_element_type=jnp.float32)
        spec = dot(high, table_ref[0]) + (dot(high, table_ref[1]) + dot(low, table_ref[0]))
        spec = spec * spec
        both_pols = (spec[:, :LANES] + spec[:, LANES:]).reshape(RADIX, 2, size, LANES)
        energy = both_pols[:, 0] + both_pols[:, 1]
        chunk = lax.broadcasted_iota(jnp.int32, (size, LANES), 1) >> 4
        for h in range(2):
            parts = [energy[8 * h + i] for i in range(8)]
            if size > EDGE:
                for bit in (4, 2, 1):
                    kept = (chunk & bit) == 0
                    for i in range(8):
                        if i & bit == 0:
                            low_part, high_part = parts[i], parts[i | bit]
                            parts[i] = jnp.where(kept, low_part, pltpu.roll(high_part, bit * RADIX, 1))
                            parts[i | bit] = jnp.where(kept, pltpu.roll(low_part, LANES - bit * RADIX, 1), high_part)
            else:
                moved = []
                for b in range(blocks):
                    mixed = parts[b]
                    for i in range(blocks):
                        if i != b:
                            turned = pltpu.roll(parts[i], (i - b) % blocks * RADIX, 1)
                            mixed = jnp.where(chunk == i, turned, mixed)
                    moved.append(mixed)
                parts = moved
            for b in range(blocks):
                out[b, pl.ds(begin, size), h * LANES:(h + 1) * LANES] = parts[b] * (usable[h][b:b + 1] * scale)

    def swap():
        rows = pl.ds(first, share)
        return pltpu.make_async_remote_copy(
            src_ref=tally.at[rows], dst_ref=tally.at[rows],
            send_sem=swap_sem.at[0], recv_sem=swap_sem.at[1],
            device_id={"tm": me + 1 - 2 * core}, device_id_type=MESH,
        )

    def admit(from_before):
        @pl.when(from_before & (me > 0))
        def _():
            forward().wait_recv()
            for p in range(2):
                ext[p, EDGE:own, 0:lines] = before[p].astype(jnp.float32)

        @pl.when(jnp.logical_not(from_before) & (me < count - 1))
        def _():
            backward().wait_recv()
            for p in range(2):
                ext[p, own + frames:own + frames + EDGE, 0:lines] = after[p].astype(jnp.float32)

    inner = frames - 2 * EDGE
    fir(EDGE, inner, weighted)
    for load in loads[2:]:
        load.wait()
    row = lax.broadcasted_iota(jnp.int32, (blocks, LANES), 1)
    even = mask_ref[pl.ds(0, blocks, stride=2), :]
    odd = mask_ref[pl.ds(1, blocks, stride=2), :]
    usable = []
    for h in range(2):
        place = (row & 7) * RADIX + 8 * h + (row >> 4)
        low = jnp.take_along_axis(even, place, axis=1, mode="promise_in_bounds")
        high = jnp.take_along_axis(odd, place, axis=1, mode="promise_in_bounds")
        usable.append(jnp.where((row & 8) == 0, low, high).astype(jnp.float32))

    level = lax.broadcasted_iota(jnp.int32, (8, LANES), 1)

    def look(table, place):
        return jnp.take_along_axis(table, place, axis=1, mode="promise_in_bounds")

    tables = NCHAN // LANES
    groups = range(share // 8)
    each = (level & (LANES // tables - 1)) * tables + (tables - 1)

    def table(g, b):
        return delay_ref[8 * g:8 * g + 8, b * LANES:(b + 1) * LANES]

    seldom = []
    for g in groups:
        kept = jnp.zeros((8, LANES), jnp.int32)
        for b in range(tables):
            kept = jnp.where((level >> 3) == b, look(table(g, b), each), kept)
        seldom.append(kept)
    coarse = [jnp.zeros((8, LANES), jnp.int32) for g in groups]
    for step in (64, 32, 16, 8, 4, 2, 1):
        for g in groups:
            seen = look(seldom[g], coarse[g] + (step - 1))
            coarse[g] = jnp.where(seen >= level, coarse[g] + step, coarse[g])
    fine = [jnp.zeros((8, LANES), jnp.int32) for g in groups]
    for step in (8, 4, 2, 1):
        for g in groups:
            place = (coarse[g] & 7) * tables + fine[g] + (step - 1)
            which = coarse[g] >> 3
            seen = jnp.full((8, LANES), -1, jnp.int32)
            for b in range(tables):
                seen = jnp.where(which == b, look(table(g, b), place), seen)
            fine[g] = jnp.where(seen >= level, fine[g] + step, fine[g])
    tally[pl.ds(first, share), :] = jnp.concatenate(
        [jnp.where(level == 0, NCHAN, coarse[g] * tables + fine[g]).astype(jnp.float32) for g in groups], axis=0)

    transform(inner, spread_out, EDGE, 1.0, weighted)
    swap().start()
    close_round(0)
    open_round(1)
    late_begin = pl.multiple_of(core * (frames - EDGE), EDGE)
    fir(late_begin, EDGE, held)
    admit(core == 1)
    begin = pl.multiple_of((1 - core) * (frames - EDGE), EDGE)
    fir(begin, EDGE, weighted)
    transform(EDGE, spread_out, begin, 1.0, weighted)
    acc[...] = jnp.zeros_like(acc)

    swap().wait_recv()
    total = tally[...]
    turned = jnp.concatenate([total, total], axis=0).T
    rows_kept = blockno.shape[0]
    near_side = lax.broadcasted_iota(jnp.int32, (rows_kept, LANES), 1) < trials
    total = jnp.where(near_side, turned[0:rows_kept], turned[HALF:HALF + rows_kept]).astype(jnp.int32)
    blockno[...] = total >> 8
    within[...] = (total & (wide - 1)).astype(jnp.float32)
    order = lax.broadcasted_iota(jnp.int32, (wide, LANES), 0)
    order = ((order & (RADIX - 1)) * RADIX + (order >> 4)).astype(jnp.float32)

    order = order.astype(jnp.bfloat16)

    def pick(j):
        end = jnp.broadcast_to(within[j:j + 1, :], (wide, LANES)).astype(jnp.bfloat16)
        return jnp.minimum(jnp.maximum(end - order, jnp.zeros_like(end)), jnp.ones_like(end))

    def dedisperse(source, begin, size, offset):
        values = jnp.concatenate([source[b, begin:begin + size] for b in range(blocks)], axis=0).astype(jnp.bfloat16)
        dot = functools.partial(jnp.dot, preferred_element_type=jnp.float32)
        sums = dot(values, jnp.ones((wide, LANES), jnp.bfloat16))
        column = lax.broadcasted_iota(jnp.int32, (size, LANES), 1)
        prefix = jnp.zeros((size, LANES), jnp.float32)
        for b in range(blocks):
            prefix = prefix + jnp.where(column > b, sums[b * size:(b + 1) * size], 0.0)
        near_side = column < trials

        def add(j, change):
            a, m = divmod(j, 8)
            place = HALF + EDGE + offset - 8 * a
            acc[m, place:place + size] += change

        last = None
        for i in range(HALF // 2):
            found = dot(values, jnp.concatenate([pick(2 * i + 1), pick(2 * i + 2)], axis=1))
            for side in range(2):
                j = 2 * i + side + 1
                which = jnp.broadcast_to(blockno[j:j + 1, :], (size, LANES))
                inner = jnp.zeros((size, LANES), jnp.float32)
                for b in range(blocks):
                    inner = jnp.where(which == b, found[b * size:(b + 1) * size, side * LANES:(side + 1) * LANES], inner)
                now = inner + jnp.take_along_axis(prefix, which, axis=1, mode="promise_in_bounds")
                if j == 1:
                    whole = sums[0:size]
                    for b in range(1, blocks):
                        whole = whole + sums[b * size:(b + 1) * size]
                    add(0, jnp.where(near_side, whole - now, 0.0))
                    after_half = jnp.where(near_side, pltpu.roll(now, trials, 1), 0.0)
                else:
                    add(j - 1, last - now)
                last = now
        add(HALF, last - after_half)

    @pl.when(me == 0)
    def _():
        fir(-EDGE, EDGE, weighted)
        transform(EDGE, early, 0, 1.0, weighted)
        dedisperse(early, 0, EDGE, -EDGE)

    @pl.when(core == 1)
    def _():
        dedisperse(spread_out, 0, frames - EDGE, 0)

    admit(core == 0)

    @pl.when(core == 0)
    def _():
        rest(0, EDGE, own)

    @pl.when(core == 1)
    def _():
        rest(frames - EDGE, own + frames, own + frames + EDGE)

    transform(EDGE, spread_out, late_begin, jnp.where(me == count - 1, 0.0, 1.0), held)
    close_round(1)
    open_round(2)
    @pl.when(core == 0)
    def _():
        dedisperse(spread_out, 0, frames, 0)

    @pl.when(core == 1)
    def _():
        dedisperse(spread_out, frames - EDGE, EDGE, frames - EDGE)

    height = HALF + frames + EDGE
    total = acc[0, 0:height]
    for m in range(1, 8):
        total = total + acc[m, m:m + height]
    side = lax.broadcasted_iota(jnp.int32, (8, LANES), 1) < trials
    empty = jnp.zeros((8, LANES), jnp.float32)

    def joined(r):
        first = total[r - HALF:r - HALF + 8] if HALF <= r < HALF + height else empty
        other = total[r:r + 8] if r < height else empty
        mixed = jnp.where(side, first, other)
        return mixed + pltpu.roll(mixed, trials, 1)

    half = frames // 2
    for q in range(reach + 1):
        for r in range(0, half, 8):
            top = joined(q * frames + r)
            low = joined(q * frames + half + r)
            part[q * half + r:q * half + r + 8, :] = jnp.where(side, top, low)
    rise = (reach + 1) * frames
    part[(reach + 1) * half:(reach + 1) * half + EDGE, :] = jnp.where(side, joined(rise), 0.0)

    def near(k):
        return pltpu.make_async_remote_copy(
            src_ref=part.at[pl.ds((reach - k) * half, half)], dst_ref=landed.at[k - 1],
            send_sem=near_send.at[k - 1], recv_sem=near_recv.at[k - 1],
            device_id={"tm": me - k}, device_id_type=MESH,
        )

    def up():
        return pltpu.make_async_remote_copy(
            src_ref=part.at[pl.ds((reach + 1) * half, EDGE)], dst_ref=risen,
            send_sem=near_send.at[reach], recv_sem=near_recv.at[reach],
            device_id={"tm": me + 1}, device_id_type=MESH,
        )

    for k in range(reach, 0, -1):
        @pl.when(me >= k)
        def _():
            near(k).start()

    @pl.when(me < count - 1)
    def _():
        up().start()

    close_round(2)
    open_round(3)

    @pl.when(me == 0)
    def _():
        risen[...] = jnp.zeros_like(risen)

    @pl.when(me > 0)
    def _():
        up().wait_recv()

    for k in range(1, reach + 1):
        @pl.when(me + k >= count)
        def _():
            landed[k - 1] = jnp.zeros((half, LANES), jnp.float32)

        @pl.when(me + k < count)
        def _():
            near(k).wait_recv()

    series = part[reach * half:(reach + 1) * half, :]
    for k in range(1, reach + 1):
        series = series + landed[k - 1]
    series = series + jnp.concatenate([risen[...], jnp.zeros((half - EDGE, LANES), jnp.float32)], axis=0)
    turned = pltpu.roll(series, trials, 1)

    def fold(value, op):
        return op(value, pltpu.roll(value, trials, 1))

    piece = jnp.sum(series, axis=0, keepdims=True) * (1.0 / half)
    away = series - piece
    opposite = pltpu.roll(piece, trials, 1)
    mean = (piece + opposite) * 0.5
    gap = piece - opposite
    spread = fold(jnp.sum(away * away, axis=0, keepdims=True), jnp.add) + (0.5 * half) * (gap * gap)
    peak = fold(jnp.max(series, axis=0, keepdims=True), jnp.maximum)
    mine[...] = jnp.concatenate([mean, spread, peak, peak], axis=0)

    def flipped(k):
        place = me
        for bit, step in enumerate(steps_of):
            if k >> bit & 1:
                place = place + step
        return place

    def far(k):
        return pltpu.make_async_remote_copy(
            src_ref=mine, dst_ref=gathered.at[k - 1],
            send_sem=far_send.at[k - 1], recv_sem=far_recv.at[k - 1],
            device_id={"tm": flipped(k)}, device_id_type=MESH,
        )

    for i in range(3, len(rounds)):
        close_round(i)
        open_round(i + 1)
    for k in range(count - 1, 0, -1):
        far(k).start()
    live = jnp.maximum(jnp.sum(mask_ref[...].astype(jnp.float32)), 1.0)
    for k in range(1, count):
        far(k).wait_recv()
    means, spreads, peaks = gathered[:, 0, :], gathered[:, 1, :], gathered[:, 2, :]
    average = (mean + jnp.sum(means, axis=0, keepdims=True)) * (1.0 / count)
    offset = means - average
    squares = spread + jnp.sum(spreads, axis=0, keepdims=True)
    between = (mean - average) * (mean - average) + jnp.sum(offset * offset, axis=0, keepdims=True)
    variance = (squares + frames * between) * (1.0 / (frames * count))
    top = jnp.maximum(peak, jnp.max(peaks, axis=0, keepdims=True))
    deviation = jnp.sqrt(variance + 1e-05)
    z_ref[0:half, :] = ((series - average) / deviation)[:, :trials]
    z_ref[half:frames, :] = ((turned - average) / deviation)[:, :trials]
    stats_ref[...] = jnp.concatenate(
        [average / live, deviation / live, (top - average) / deviation], axis=0
    )[:, :trials]

    @pl.when(me < count - 1)
    def _():
        forward().wait_send()
        up().wait_send()

    @pl.when(me > 0)
    def _():
        backward().wait_send()

    swap().wait_send()
    for k in range(1, reach + 1):
        @pl.when(me >= k)
        def _():
            near(k).wait_send()
    for k in range(1, count):
        far(k).wait_send()


def finish_kernel(z_ref, stats_ref, z_out, stats_out, sem):
    first = pltpu.make_async_copy(z_ref, z_out, sem.at[0])
    second = pltpu.make_async_copy(stats_ref, stats_out, sem.at[1])
    first.start()
    second.start()
    first.wait()
    second.wait()


def per_device(voltage, delays, chan_mask):
    frames = voltage.shape[2] // NCHAN
    trials = delays.shape[0]
    count = lax.axis_size("tm")
    lines = 2 * RADIX
    half = frames // 2
    blocks = LANES // RADIX
    wide = NCHAN // blocks
    reach = MAXD // frames
    past = TAPS - 1
    vmem = pl.BlockSpec(memory_space=pltpu.VMEM)
    hbm = pl.BlockSpec(memory_space=pltpu.HBM)
    framed = voltage.reshape(2, 2, frames * RADIX, LANES).transpose(0, 2, 1, 3).reshape(2, frames, lines, LANES)
    operands = (framed, jnp.asarray(prototype()), jnp.asarray(twiddles()), jnp.asarray(transform_table()), delays,
                chan_mask.reshape(RADIX, LANES))
    dma = pltpu.SemaphoreType.DMA
    outputs = (
        jax.ShapeDtypeStruct((frames, trials), jnp.float32),
        jax.ShapeDtypeStruct((3, trials), jnp.float32),
    )
    results = pl.pallas_call(
        functools.partial(beam_kernel, count, frames, trials),
        out_shape=outputs,
        in_specs=[hbm] * 6,
        out_specs=(vmem,) * 2,
        scratch_shapes=[
            pltpu.VMEM((2, frames, lines, LANES), jnp.bfloat16),
            pltpu.VMEM((TAPS, PITCH, LANES), jnp.float32),
            pltpu.VMEM((2, RADIX, LANES), jnp.float32),
            pltpu.VMEM((2, 2 * LANES, 2 * LANES), jnp.bfloat16),
            pltpu.VMEM((trials // 2, NCHAN), jnp.int32),
            pltpu.VMEM((RADIX, LANES), jnp.int32),
            pltpu.VMEM((2, past - EDGE, lines, LANES), jnp.bfloat16),
            pltpu.VMEM((2, EDGE, lines, LANES), jnp.bfloat16),
            pltpu.VMEM((2, frames + past + EDGE, PITCH, LANES), jnp.float32),
            pltpu.VMEM((2 * frames * PITCH, LANES), jnp.float32),
            pltpu.VMEM((2 * EDGE * PITCH, LANES), jnp.float32),
            pltpu.VMEM((2 * RADIX * frames, 2 * LANES), jnp.float32),
            pltpu.VMEM((blocks, frames, 2 * LANES), jnp.float32),
            pltpu.VMEM((blocks, EDGE, 2 * LANES), jnp.float32),
            pltpu.VMEM((trials, LANES), jnp.float32),
            pltpu.VMEM((HALF + 8, LANES), jnp.int32),
            pltpu.VMEM((HALF + 8, LANES), jnp.float32),
            pltpu.VMEM((8, HALF + frames + 2 * EDGE, LANES), jnp.float32),
            pltpu.VMEM(((reach + 1) * half + EDGE, LANES), jnp.float32),
            pltpu.VMEM((reach, half, LANES), jnp.float32),
            pltpu.VMEM((EDGE, LANES), jnp.float32),
            pltpu.VMEM((4, LANES), jnp.float32),
            pltpu.VMEM((count - 1, 4, LANES), jnp.float32),
            dma((6,)),
            dma((2,)),
            dma((2,)),
            dma((reach + 1,)),
            dma((reach + 1,)),
            dma((count - 1,)),
            dma((count - 1,)),
            dma((2,)),
            pltpu.SemaphoreType.REGULAR((8,)),
        ],
        compiler_params=pltpu.CompilerParams(collective_id=1, vmem_limit_bytes=GRANT, has_side_effects=True),
        name="beam",
    )(*[pltpu.with_memory_space_constraint(v, pltpu.HBM) for v in operands])
    zscore, trial_stats = pl.pallas_call(
        finish_kernel,
        out_shape=outputs,
        in_specs=[vmem] * 2,
        out_specs=(hbm,) * 2,
        scratch_shapes=[dma((2,))],
        compiler_params=pltpu.CompilerParams(vmem_limit_bytes=GRANT),
        name="finish",
    )(*results)
    return (zscore.T, trial_stats)


def solution(mesh):
    in_specs = (P(None, None, ("beam", "tm")), P(), P("beam"))
    out_specs = (P(None, ("beam", "tm")), P(None, "beam"))
    return jax.shard_map(
        per_device, mesh=mesh, in_specs=in_specs, out_specs=out_specs, check_vma=False
    )
```
